128 devices in a mesh: dp: 4 (over x_hi, core), seq: 32 (over y, z, x_lo).
Axes of the slice: x: 4 (x_hi: 2, x_lo: 2; x = x_hi * 2 + x_lo), y: 4, z: 4, core: 2. Of those that a mesh axis runs over, the one named last changes fastest.
Arguments:
- queries: bfloat16 [4, 8192, 1024], P('dp', 'seq'), may hold values from -6 to 6
- keys: bfloat16 [4, 8192, 1024], P('dp', 'seq'), may hold values from -6 to 6
- values: bfloat16 [4, 8192, 1024], P('dp', 'seq'), may hold values from -6 to 6
- out_weight: bfloat16 [1024, 1024], replicated, may hold values from -0.1875 to 0.1875
- cotangent: bfloat16 [4, 8192, 1024], P('dp', 'seq'), may hold values from -6 to 6
Outputs:
- mixed: bfloat16 [4, 8192, 1024], P('dp', 'seq')
- grad_out_weight: float32 [1024, 1024], P(('dp', 'seq'))
- grad_queries: bfloat16 [4, 8192, 1024], P('dp', 'seq')
- grad_keys: bfloat16 [4, 8192, 1024], P('dp', 'seq')
- grad_values: bfloat16 [4, 8192, 1024], P('dp', 'seq')
The draws below stay inside these ranges and needn't reach their ends.
All inputs are finite; a program needn't handle non-finite values.
Results may differ from the reference program's by a relative error of at most 0.02.
Values may be sent and summed in bfloat16 or wider, within the bound.
No kernel may reach another device: no remote copies, remote signals or barrier semaphores. Data moves between devices by JAX's collectives and lax.ppermute only.
A program may use at most 128 MiB of HBM per device.

```python
import math
import jax
import jax.numpy as jnp
from jax import lax

WIDTH = 1024
HEADS = 16
HEAD_DIM = 64
BLOCK = 64
TOK_DEV = 256
BATCH = 4
SEQ = 8192
GROUP_ONE = 4
GROUP_TWO = 16


def draw_queries(key, part):
    own_key = jax.random.fold_in(key, 11)
    noise = jax.random.normal(own_key, (BATCH, SEQ, HEADS * HEAD_DIM), jnp.float32)
    field = jnp.clip(1.25 * noise, -5.5, 5.5)
    return field.astype(jnp.bfloat16)


def draw_keys(key, part):
    own_key = jax.random.fold_in(key, 21)
    noise = jax.random.normal(own_key, (BATCH, SEQ, HEADS * HEAD_DIM), jnp.float32)
    field = jnp.clip(1.25 * noise, -5.5, 5.5)
    return field.astype(jnp.bfloat16)


def level_of(key, shape, pieces, smallest, top_value):
    def one(position, blocks):
        steps = jax.random.uniform(jax.random.fold_in(jax.random.fold_in(key, 6), position), (blocks,), jnp.float32, smallest / len(pieces), top_value / len(pieces))
        return jnp.repeat(jnp.exp(steps), shape[position] // blocks).reshape((-1,) + (1,) * (len(shape) - position - 1))

    factor_of = one(*pieces[0])
    for cut in pieces[1:]:
        factor_of = factor_of * one(*cut)
    return factor_of


def scatter_about(stream_key, dims, scale, bound, cuts=(), held_as=jnp.bfloat16):
    gain = level_of(stream_key, dims, cuts, -0.22, 0.18) if cuts else 1.0
    entries = jax.random.normal(stream_key, dims, jnp.float32) * scale * gain
    return jnp.minimum(jnp.maximum(entries, -bound), bound).astype(held_as)


def setup_inputs(seed: int = 0) -> dict:
    streams_of = jax.random.split(jax.random.key(seed), 6)
    return {
        "queries": draw_queries(jax.random.fold_in(streams_of[5], 71), 0),
        "keys": draw_keys(jax.random.fold_in(streams_of[5], 71), 0),
        "values": scatter_about(streams_of[2], (BATCH, SEQ, HEADS * HEAD_DIM), 1.0, 6.0, ((0, 4), (1, 32))),
        "out_weight": scatter_about(streams_of[3], (HEADS * HEAD_DIM, WIDTH), (HEADS * HEAD_DIM) ** -0.5, 0.1875),
        "cotangent": scatter_about(streams_of[4], (BATCH, SEQ, WIDTH), 1.0, 6.0, ((0, 4), (1, 32))),
    }


MASKED = -1e+30

def rounded(matrix):
    return lax.optimization_barrier(matrix.astype(jnp.bfloat16)).astype(jnp.float32)

def split_heads(matrix, head_count):
    return matrix.reshape(matrix.shape[0], head_count, matrix.shape[1] // head_count)

def pool_rows(matrix, pool_width):
    coarse_count = matrix.shape[0] // pool_width
    summed = lax.optimization_barrier(jnp.sum(matrix.reshape(coarse_count, pool_width, matrix.shape[1]), axis=1, dtype=jnp.float32))
    return (summed / math.sqrt(pool_width)).astype(jnp.bfloat16)

def stretch(matrix, pool_width):
    widened = jnp.broadcast_to(matrix[:, None], (matrix.shape[0], pool_width) + matrix.shape[1:])
    return widened.reshape((matrix.shape[0] * pool_width,) + matrix.shape[1:])

def key_usable(first_block, block_count, all_blocks, block_len, left_open, right_open):
    block_ids = first_block + jnp.arange(block_count)[:, None]
    slot_ids = jnp.arange(3 * block_len)[None, :] // block_len
    keep_left = jnp.logical_or(slot_ids > 0, jnp.logical_or(block_ids > 0, left_open))
    keep_right = jnp.logical_or(slot_ids < 2, jnp.logical_or(block_ids < all_blocks - 1, right_open))
    return jnp.logical_and(keep_left, keep_right)

def windows(extended, row_count, block_len, head_count):
    block_count = row_count // block_len
    head_size = extended.shape[1] // head_count
    slabs = [extended[shift_id * block_len:shift_id * block_len + row_count].reshape(block_count, block_len, head_count, head_size) for shift_id in range(3)]
    return jnp.concatenate(slabs, axis=1)

def unfold(window_grads, row_count, block_len):
    folded = jnp.zeros((row_count + 2 * block_len, window_grads.shape[2] * window_grads.shape[3]), jnp.float32)
    for shift_id in range(3):
        slab = window_grads[:, shift_id * block_len:(shift_id + 1) * block_len].reshape(row_count, -1)
        folded = folded + jnp.pad(slab, ((shift_id * block_len, (2 - shift_id) * block_len), (0, 0)))
    return folded

def to_rows(blocked):
    return jnp.transpose(blocked, (0, 2, 1)).reshape(-1, blocked.shape[1])

def to_blocks(per_row, block_len):
    return jnp.transpose(per_row.reshape(-1, block_len, per_row.shape[1]), (0, 2, 1))

def allowed_mask(level_id, query_ids, key_ids, per_device, span_one, span_two):
    query_dev = query_ids[:, None] // per_device
    key_dev = key_ids[None, :] // per_device
    if level_id == 0:
        return jnp.logical_and(query_dev // span_one == key_dev // span_one, jnp.abs(query_ids[:, None] - key_ids[None, :]) > 1)
    if level_id == 1:
        return jnp.logical_and(query_dev // span_two == key_dev // span_two, query_dev // span_one != key_dev // span_one)
    return query_dev // span_two != key_dev // span_two

def combine(fine_max, fine_total, fine_weighted, levels):
    row_max = fine_max
    for level_max, level_total, level_weighted, pool_width in levels:
        row_max = jnp.maximum(row_max, stretch(level_max, pool_width))
    factor = jnp.exp(fine_max - row_max)
    denominator = fine_total * factor
    numerator = fine_weighted * factor[..., None]
    for level_max, level_total, level_weighted, pool_width in levels:
        factor = jnp.exp(stretch(level_max, pool_width) - row_max)
        denominator = denominator + stretch(level_total, pool_width) * factor
        numerator = numerator + stretch(level_weighted, pool_width) * factor[..., None]
    attended = (numerator / denominator[..., None]).reshape(numerator.shape[0], -1).astype(jnp.bfloat16)
    return (attended, row_max, denominator)

def band_scores(queries, extended, usable, block_len, head_count, score_scale):
    row_count = queries.shape[0]
    key_value_win = windows(extended, row_count, block_len, 2 * head_count)
    key_win = key_value_win[:, :, :head_count]
    value_win = key_value_win[:, :, head_count:]
    query_blocks = queries.reshape(row_count // block_len, block_len, head_count, -1)
    scores = jnp.einsum('bqhe,bkhe->bhqk', query_blocks.astype(jnp.float32), key_win.astype(jnp.float32)) * score_scale
    scores = jnp.where(usable[:, None, None, :], scores, MASKED)
    return (scores, query_blocks, key_win, value_win)

def band_forward(queries, extended, usable, block_len, head_count, score_scale):
    scores, query_blocks, key_win, value_win = band_scores(queries, extended, usable, block_len, head_count, score_scale)
    maxima = lax.optimization_barrier(jnp.max(scores, axis=-1))
    exponent = jnp.exp(scores - maxima[..., None])
    totals = lax.optimization_barrier(jnp.sum(exponent, axis=-1))
    weighted = jnp.einsum('bhqk,bkhe->bqhe', rounded(exponent), value_win.astype(jnp.float32))
    return (to_rows(maxima), to_rows(totals), weighted.reshape(queries.shape[0], head_count, -1))

def band_backward(queries, extended, usable, upstream, row_delta, maxima, weight, block_len, head_count, score_scale):
    row_count = queries.shape[0]
    scores, query_blocks, key_win, value_win = band_scores(queries, extended, usable, block_len, head_count, score_scale)
    probability = jnp.exp(scores - to_blocks(maxima, block_len)[..., None]) * to_blocks(weight, block_len)[..., None]
    grad_blocks = upstream.reshape(row_count // block_len, block_len, head_count, -1).astype(jnp.float32)
    prob_grad = jnp.einsum('bqhe,bkhe->bhqk', grad_blocks, value_win.astype(jnp.float32))
    score_grad = rounded(probability * (prob_grad - to_blocks(row_delta, block_len)[..., None]))
    grad_query = jnp.einsum('bhqk,bkhe->bqhe', score_grad, key_win.astype(jnp.float32)) * score_scale
    grad_key = jnp.einsum('bhqk,bqhe->bkhe', score_grad, query_blocks.astype(jnp.float32)) * score_scale
    grad_value = jnp.einsum('bhqk,bqhe->bkhe', rounded(probability), grad_blocks)
    joined = jnp.concatenate([grad_key, grad_value], axis=2)
    return (grad_query.reshape(row_count, -1), unfold(joined, row_count, block_len))

def coarse_scores(coarse_query, coarse_key, allowed, head_count, score_scale):
    scores = jnp.einsum('qhe,khe->hqk', split_heads(coarse_query, head_count).astype(jnp.float32), split_heads(coarse_key, head_count).astype(jnp.float32)) * score_scale
    scores = jnp.where(allowed[None], scores, MASKED)
    maxima = lax.optimization_barrier(jnp.max(scores, axis=-1))
    exponent = jnp.where(allowed[None], jnp.exp(scores - maxima[..., None]), 0.0)
    return (maxima, exponent)

def coarse_forward(coarse_query, coarse_key, coarse_value, allowed, head_count, score_scale):
    maxima, exponent = coarse_scores(coarse_query, coarse_key, allowed, head_count, score_scale)
    weighted = jnp.einsum('hqk,khe->qhe', rounded(exponent), split_heads(coarse_value, head_count).astype(jnp.float32))
    return (maxima.T, lax.optimization_barrier(jnp.sum(exponent, axis=-1)).T, weighted)

def coarse_backward(coarse_query, coarse_key, coarse_value, allowed, head_count, score_scale, weight, upstream, row_delta, pool_width):
    maxima, exponent = coarse_scores(coarse_query, coarse_key, allowed, head_count, score_scale)
    coarse_count = coarse_query.shape[0]
    gathered = rounded(lax.optimization_barrier(jnp.sum((weight[..., None] * upstream).reshape(coarse_count, pool_width, head_count, -1), axis=1)))
    delta_sum = lax.optimization_barrier(jnp.sum((weight * row_delta).reshape(coarse_count, pool_width, head_count), axis=1))
    prob_grad = jnp.einsum('qhe,khe->hqk', gathered, split_heads(coarse_value, head_count).astype(jnp.float32))
    score_grad = rounded(exponent * (prob_grad - delta_sum.T[..., None]))
    grad_query = jnp.einsum('hqk,khe->qhe', score_grad, split_heads(coarse_key, head_count).astype(jnp.float32)) * score_scale
    grad_key = jnp.einsum('hqk,qhe->khe', score_grad, split_heads(coarse_query, head_count).astype(jnp.float32)) * score_scale
    grad_value = jnp.einsum('hqk,qhe->khe', rounded(exponent), gathered)
    key_count = coarse_key.shape[0]
    return (grad_query.reshape(coarse_count, -1), jnp.concatenate([grad_key.reshape(key_count, -1), grad_value.reshape(key_count, -1)], axis=1))

def one_performance(query_rows, key_rows, value_rows, grad_rows, out_weight):
    head_count = HEADS
    block_len = BLOCK
    hidden = HEADS * HEAD_DIM
    score_scale = 1.0 / math.sqrt(HEAD_DIM)
    segments = SEQ // TOK_DEV
    block_count = TOK_DEV // block_len
    widths = (block_len, 2 * block_len, 4 * block_len)
    joined = jnp.concatenate([key_rows, value_rows], axis=1)
    padded = jnp.pad(joined, ((block_len, block_len), (0, 0)))

    def segment_rows(matrix, segment):
        return lax.dynamic_slice_in_dim(matrix, segment * TOK_DEV, TOK_DEV, 0)

    def segment_inputs(segment):
        extended = lax.dynamic_slice_in_dim(padded, segment * TOK_DEV, TOK_DEV + 2 * block_len, 0)
        usable = key_usable(0, block_count, block_count, block_len, segment > 0, segment < segments - 1)
        return (segment_rows(query_rows, segment), extended, usable)

    def fine_forward(segment):
        rows_here, extended, usable = segment_inputs(segment)
        return band_forward(rows_here, extended, usable, block_len, head_count, score_scale)
    segment_ids = jnp.arange(segments, dtype=jnp.int32)
    fine_max, fine_total, fine_weighted = lax.map(fine_forward, segment_ids)
    fine_max = fine_max.reshape(SEQ, head_count)
    fine_total = fine_total.reshape(SEQ, head_count)
    fine_weighted = fine_weighted.reshape(SEQ, head_count, HEAD_DIM)
    coarse = []
    levels = []
    for level_id in range(3):
        pool_width = widths[level_id]
        coarse_query = pool_rows(query_rows, pool_width)
        coarse_kv = pool_rows(joined, pool_width)
        coarse_ids = jnp.arange(SEQ // pool_width)
        allowed = allowed_mask(level_id, coarse_ids, coarse_ids, TOK_DEV // pool_width, GROUP_ONE, GROUP_TWO)
        entry = (coarse_query, coarse_kv[:, :hidden], coarse_kv[:, hidden:], allowed)
        coarse.append(entry)
        levels.append(coarse_forward(entry[0], entry[1], entry[2], allowed, head_count, score_scale) + (pool_width,))
    attended, row_max, denominator = combine(fine_max, fine_total, fine_weighted, levels)
    mixed = jnp.dot(attended, out_weight, preferred_element_type=jnp.float32).astype(jnp.bfloat16)
    d_attended = lax.dot_general(grad_rows, out_weight, (((1,), (1,)), ((), ())), preferred_element_type=jnp.float32).astype(jnp.bfloat16)
    upstream = split_heads(d_attended, head_count).astype(jnp.float32)
    row_delta = lax.optimization_barrier(jnp.sum(upstream * split_heads(attended, head_count).astype(jnp.float32), axis=-1))
    fine_weight = jnp.exp(fine_max - row_max) / denominator

    def fine_backward(segment):
        rows_here, extended, usable = segment_inputs(segment)
        return band_backward(rows_here, extended, usable, segment_rows(d_attended, segment), segment_rows(row_delta, segment), segment_rows(fine_max, segment), segment_rows(fine_weight, segment), block_len, head_count, score_scale)
    grad_query, ext_grads = lax.map(fine_backward, segment_ids)
    middle = ext_grads[:, block_len:block_len + TOK_DEV]
    left_part = ext_grads[:, :block_len]
    right_part = ext_grads[:, TOK_DEV + block_len:]
    zero_part = jnp.zeros_like(left_part[:1])
    from_next = jnp.concatenate([left_part[1:], zero_part], axis=0)
    from_prev = jnp.concatenate([zero_part, right_part[:-1]], axis=0)
    middle = middle + jnp.pad(from_next, ((0, 0), (TOK_DEV - block_len, 0), (0, 0)))
    middle = middle + jnp.pad(from_prev, ((0, 0), (0, TOK_DEV - block_len), (0, 0)))
    kv_grad = middle.reshape(SEQ, 2 * hidden)
    query_grad = grad_query.reshape(SEQ, hidden)
    for entry, level in zip(coarse, levels):
        pool_width = level[3]
        weight = jnp.exp(stretch(level[0], pool_width) - row_max) / denominator
        coarse_q_grad, coarse_kv_grad = coarse_backward(entry[0], entry[1], entry[2], entry[3], head_count, score_scale, weight, upstream, row_delta, pool_width)
        query_grad = query_grad + stretch(coarse_q_grad, pool_width) / math.sqrt(pool_width)
        kv_grad = kv_grad + stretch(coarse_kv_grad, pool_width) / math.sqrt(pool_width)
    return (mixed, attended, query_grad.astype(jnp.bfloat16), kv_grad[:, :hidden].astype(jnp.bfloat16), kv_grad[:, hidden:].astype(jnp.bfloat16))

def reference(queries, keys, values, out_weight, cotangent):

    def run_one(inputs):
        return one_performance(inputs[0], inputs[1], inputs[2], inputs[3], out_weight)
    mixed, attended, grad_queries, grad_keys, grad_values = lax.map(run_one, (queries, keys, values, cotangent))
    hidden = HEADS * HEAD_DIM
    grad_out_weight = lax.dot_general(attended.reshape(-1, hidden), cotangent.reshape(-1, WIDTH), (((0,), (0,)), ((), ())), preferred_element_type=jnp.float32)
    return (mixed, grad_out_weight, grad_queries, grad_keys, grad_values)
```

```python
import math

import jax
import jax.numpy as jnp
from jax import lax
from jax.experimental import pallas as pl
from jax.experimental.pallas import tpu as pltpu
from jax.sharding import PartitionSpec as P

HEADS = 16
HEAD_DIM = 64
BLOCK = 64
TOKENS = 256
HIDDEN = 1024
PAIRS = HIDDEN // 128
LEVEL_ROWS = 8
MASKED = -1e30
F32 = jnp.float32
BF16 = jnp.bfloat16
SCALE = 1.0 / math.sqrt(HEAD_DIM)
ROOTS = (math.sqrt(64.0), math.sqrt(128.0), math.sqrt(256.0))


def mm(a, b, dims):
    return lax.dot_general(a, b, (dims, ((), ())), preferred_element_type=F32)


def iota(shape, dim):
    return lax.broadcasted_iota(jnp.int32, shape, dim)


def full(shape):
    return pl.BlockSpec(shape, lambda *_: (0,) * len(shape))


def pooled_levels(ref):
    one = [
        jnp.sum(ref[BLOCK * b : BLOCK * (b + 1), :].astype(F32), axis=0, keepdims=True)
        for b in range(4)
    ]
    two = [one[0] + one[1], one[2] + one[3]]
    three = [two[0] + two[1]]
    return [[x / root for x in rows] for rows, root in zip((one, two, three), ROOTS)]


def pool_kernel(q_ref, k_ref, v_ref, send_ref, cq_ref, first_ref, last_ref):
    me = lax.axis_index("seq")
    zero = jnp.zeros((1, HIDDEN), F32)
    q1, q2, q3 = pooled_levels(q_ref)
    cq_ref[...] = jnp.concatenate(q1 + q2 + q3 + [zero], axis=0).astype(BF16)
    k1, k2, k3 = pooled_levels(k_ref)
    v1, v2, v3 = pooled_levels(v_ref)
    slot1 = jnp.concatenate(k1 + v1, axis=0)
    slot2 = jnp.concatenate(k2 + [zero] * 2 + v2 + [zero] * 2, axis=0)
    slot3 = jnp.concatenate(k3 + [zero] * 3 + v3 + [zero] * 3, axis=0)
    for g in range(8):
        slot = jnp.where(me // 4 == g, slot1, jnp.where(me // 16 == g // 4, slot2, slot3))
        send_ref[32 * g : 32 * (g + 1), :] = jnp.concatenate([slot] * 4, axis=0).astype(BF16)
    first_ref[:BLOCK, :] = k_ref[:BLOCK, :]
    first_ref[BLOCK:, :] = v_ref[:BLOCK, :]
    last_ref[:BLOCK, :] = k_ref[TOKENS - BLOCK :, :]
    last_ref[BLOCK:, :] = v_ref[TOKENS - BLOCK :, :]


def pool(q, k, v):
    return pl.pallas_call(
        pool_kernel,
        out_shape=(
            jax.ShapeDtypeStruct((256, HIDDEN), BF16),
            jax.ShapeDtypeStruct((LEVEL_ROWS, HIDDEN), BF16),
            jax.ShapeDtypeStruct((2 * BLOCK, HIDDEN), BF16),
            jax.ShapeDtypeStruct((2 * BLOCK, HIDDEN), BF16),
        ),
        name="pool",
    )(q, k, v)


def window(own, left, right, half, row):
    if half == 0:
        return jnp.concatenate([left[row : row + BLOCK, :], own[: 3 * BLOCK, :]], axis=0)
    return jnp.concatenate([own[BLOCK:, :], right[row : row + BLOCK, :]], axis=0)


def band_bias(half, key_dim):
    me = lax.axis_index("seq")
    key_block = iota((256, 256), key_dim) // BLOCK
    query_block = iota((256, 256), 1 - key_dim) // BLOCK % 2
    gap = key_block - query_block
    keep = jnp.logical_and(gap >= 0, gap <= 2)
    if half == 0:
        keep = jnp.logical_and(keep, key_block >= jnp.where(me > 0, 0, 1))
    else:
        last = lax.axis_size("seq") - 1
        keep = jnp.logical_and(keep, key_block <= jnp.where(me < last, 3, 2))
    return jnp.where(keep, 0.0, MASKED).astype(F32)


def head_masks():
    lane = iota((1, 128), 1)
    low = jnp.where(lane < HEAD_DIM, 1.0, 0.0).astype(BF16)
    high = jnp.where(lane < HEAD_DIM, 0.0, 1.0).astype(BF16)
    return low, high


def two_heads(rows, masks):
    return jnp.concatenate([rows * masks[0], rows * masks[1]], axis=0)


def pick(stacked, low_lane):
    return jnp.where(low_lane, stacked[:128, :], stacked[128:, :])


def fine_forward_kernel(q_ref, k_ref, v_ref, left_ref, right_ref, n_ref, m_ref, l_ref, bias_ref):
    @pl.when(pl.program_id(0) == 0)
    def _():
        bias_ref[0] = band_bias(0, 1)
        bias_ref[1] = band_bias(1, 1)

    masks = head_masks()
    low_lane = iota((128, 128), 1) < HEAD_DIM
    ones = jnp.ones((256, 128), BF16)
    own_k, own_v = k_ref[...], v_ref[...]
    left, right = left_ref[...], right_ref[...]
    for half in range(2):
        rows = slice(128 * half, 128 * (half + 1))
        keys = window(own_k, left, right, half, 0)
        vals = window(own_v, left, right, half, BLOCK)
        query = two_heads(q_ref[rows, :], masks)
        scores = mm(query, keys, ((1,), (1,))) * SCALE + bias_ref[half]
        top = jnp.max(scores, axis=1, keepdims=True)
        weights = jnp.exp(scores - top).astype(BF16)
        both = mm(weights, jnp.concatenate([vals, ones], axis=1), ((1,), (0,)))
        n_ref[rows, :] = pick(both[:, :128], low_lane)
        l_ref[rows, :] = pick(both[:, 128:], low_lane)
        m_ref[rows, :] = pick(jnp.broadcast_to(top, (256, 128)), low_lane)


def pair_spec(rows):
    return pl.BlockSpec((rows, 128), lambda p: (0, p))


def fine_forward(q, k, v, left, right):
    tok = pair_spec(TOKENS)
    edge = pair_spec(2 * BLOCK)
    out = jax.ShapeDtypeStruct((TOKENS, HIDDEN), F32)
    return pl.pallas_call(
        fine_forward_kernel,
        grid=(PAIRS,),
        in_specs=[tok, tok, tok, edge, edge],
        out_specs=[tok, tok, tok],
        out_shape=(out, out, out),
        scratch_shapes=[pltpu.VMEM((2, 256, 256), F32)],
        cost_estimate=pl.CostEstimate(
            flops=3 * 16 * 2 * 256 * 256 * 128, transcendentals=16 * 256 * 256, bytes_accessed=6 << 20
        ),
        name="fine_forward",
    )(q, k, v, left, right)


def coarse_keep():
    me = lax.axis_index("seq")
    row = iota((128, 256), 0) % LEVEL_ROWS
    col = iota((128, 256), 1)
    dev = col // 8
    term = col % 8
    near = dev // 4 == me // 4
    mid = jnp.logical_and(dev // 16 == me // 16, jnp.logical_not(near))
    far = dev // 16 != me // 16
    apart = jnp.abs(4 * me + row - (4 * dev + term)) > 1
    one = jnp.logical_and(jnp.logical_and(row < 4, term < 4), jnp.logical_and(near, apart))
    two = jnp.logical_and(jnp.logical_and(row // 2 == 2, term < 2), mid)
    three = jnp.logical_and(jnp.logical_and(row == 6, term == 0), far)
    return jnp.logical_or(one, jnp.logical_or(two, three))


def by_head(rows, own):
    return jnp.concatenate([rows] * HEADS, axis=0) * own


def over_heads(stacked, own):
    return jnp.sum((stacked * own).reshape(HEADS, LEVEL_ROWS, HIDDEN), axis=0)


def join_kernel(
    cq_ref,
    kv_ref,
    n_ref,
    m_ref,
    l_ref,
    da_ref,
    att_ref,
    lse_ref,
    delta_ref,
    dq_ref,
    dkv_ref,
    mc_ref,
    lc_ref,
    nc_ref,
    g_ref,
    h_ref,
):
    own = jnp.where(
        iota((128, HIDDEN), 0) // LEVEL_ROWS == iota((128, HIDDEN), 1) // HEAD_DIM, 1.0, 0.0
    ).astype(F32)
    keep = coarse_keep()
    kv = kv_ref[...]
    query = by_head(cq_ref[...].astype(F32), own).astype(BF16)
    scores = jnp.where(keep, mm(query, kv, ((1,), (1,))) * SCALE, MASKED)
    top = jnp.max(scores, axis=1, keepdims=True)
    weights = jnp.where(keep, jnp.exp(scores - top), 0.0)
    total = jnp.sum(weights, axis=1, keepdims=True)
    on_values = pltpu.roll(weights, 4, 1).astype(BF16)
    nc_ref[...] = over_heads(mm(on_values, kv, ((1,), (0,))), own)
    mc_ref[...] = over_heads(jnp.broadcast_to(top, (128, HIDDEN)), own)
    lc_ref[...] = over_heads(jnp.broadcast_to(total, (128, HIDDEN)), own)
    same_head = jnp.where(
        iota((128, 128), 0) // HEAD_DIM == iota((128, 128), 1) // HEAD_DIM, 1.0, 0.0
    ).astype(BF16)
    for p in range(PAIRS):
        lanes = slice(128 * p, 128 * (p + 1))
        g_two, h_two, g_three, h_three = [], [], [], []
        g_one, h_one = [], []
        for b in range(4):
            rows = slice(BLOCK * b, BLOCK * (b + 1))
            level = (b, 4 + b // 2, 6)
            m0 = m_ref[rows, lanes]
            mc = [mc_ref[c : c + 1, lanes] for c in level]
            top_all = jnp.maximum(jnp.maximum(m0, mc[0]), jnp.maximum(mc[1], mc[2]))
            f0 = jnp.exp(m0 - top_all)
            fc = [jnp.exp(x - top_all) for x in mc]
            den = l_ref[rows, lanes] * f0
            num = n_ref[rows, lanes] * f0
            for c, f in zip(level, fc):
                den = den + lc_ref[c : c + 1, lanes] * f
                num = num + nc_ref[c : c + 1, lanes] * f
            inv = 1.0 / den
            att = (num * inv).astype(BF16)
            att_ref[rows, lanes] = att
            lse_ref[rows, lanes] = top_all + jnp.log(den)
            da = da_ref[rows, lanes].astype(F32)
            product = da * att.astype(F32)
            part = product.astype(BF16)
            rest = (product - part.astype(F32)).astype(BF16)
            delta = mm(part, same_head, ((1,), (0,))) + mm(rest, same_head, ((1,), (0,)))
            delta_ref[rows, lanes] = delta
            wc = [f * inv for f in fc]
            g = [jnp.sum(w * da, axis=0, keepdims=True) for w in wc]
            h = [jnp.sum(w * delta, axis=0, keepdims=True) for w in wc]
            g_one.append(g[0])
            h_one.append(h[0])
            g_two.append(g[1])
            h_two.append(h[1])
            g_three.append(g[2])
            h_three.append(h[2])
        zero = jnp.zeros((1, 128), F32)

        def rows_of(one, two, three):
            return jnp.concatenate(
                one
                + [two[0] + two[1], two[2] + two[3]]
                + [(three[0] + three[1]) + (three[2] + three[3]), zero],
                axis=0,
            )

        g_ref[:, lanes] = rows_of(g_one, g_two, g_three)
        h_ref[:, lanes] = rows_of(h_one, h_two, h_three)
    grads = by_head(g_ref[...], own).astype(BF16)
    sums = jnp.sum(by_head(h_ref[...], own), axis=1, keepdims=True) * (1.0 / HEAD_DIM)
    on_keys = pltpu.roll(mm(grads, kv, ((1,), (1,))), 252, 1)
    score_grad = weights * (on_keys - sums)
    row = iota((LEVEL_ROWS, 1), 0)
    share = jnp.where(row < 4, 1.0 / ROOTS[0], jnp.where(row < 6, 1.0 / ROOTS[1], 1.0 / ROOTS[2]))
    dq_ref[...] = over_heads(mm(score_grad.astype(BF16), kv, ((1,), (0,))), own) * (
        share.astype(F32) * SCALE
    )
    left = jnp.concatenate([(score_grad * SCALE).astype(BF16), on_values], axis=0)
    right = jnp.concatenate([query, grads], axis=0)
    dkv_ref[...] = mm(left, right, ((0,), (0,))).astype(BF16)


def join(cq, kv, n, m, l, da):
    f_out = jax.ShapeDtypeStruct((TOKENS, HIDDEN), F32)
    small = pltpu.VMEM((LEVEL_ROWS, HIDDEN), F32)
    return pl.pallas_call(
        join_kernel,
        out_shape=(
            jax.ShapeDtypeStruct((TOKENS, HIDDEN), BF16),
            f_out,
            f_out,
            jax.ShapeDtypeStruct((LEVEL_ROWS, HIDDEN), F32),
            jax.ShapeDtypeStruct((256, HIDDEN), BF16),
        ),
        scratch_shapes=[small] * 5,
        name="join",
    )(cq, kv, n, m, l, da)


def weight_kernel(att_ref, cot_ref, keep_ref, give_ref):
    core = lax.axis_index("dp") % 2
    cot = cot_ref[...]

    def half_rows(which):
        parts = []
        for hi in range(2):
            start = pl.multiple_of((2 * hi + which) * 256, 256)
            part = mm(att_ref[:, pl.ds(start, 256)], cot, ((0,), (0,)))
            parts.append(part.reshape(32, 8, HIDDEN))
        return jnp.concatenate(parts, axis=1).reshape(512, HIDDEN).astype(BF16)

    give_ref[...] = half_rows(1 - core)
    keep_ref[...] = half_rows(core)


def weight_terms(att, cot):
    out = jax.ShapeDtypeStruct((512, HIDDEN), BF16)
    return pl.pallas_call(
        weight_kernel,
        out_shape=(out, out),
        cost_estimate=pl.CostEstimate(
            flops=2 * 256 * 1024 * 1024, transcendentals=0, bytes_accessed=3 << 20
        ),
        name="weight_terms",
    )(att, cot)


def fine_backward_kernel(
    q_ref,
    k_ref,
    v_ref,
    left_ref,
    right_ref,
    da_ref,
    lse_ref,
    delta_ref,
    cdq_ref,
    gq_ref,
    dk_ref,
    dv_ref,
    to_left_ref,
    to_right_ref,
    bias_ref,
):
    @pl.when(pl.program_id(0) == 0)
    def _():
        bias_ref[0] = band_bias(0, 0)
        bias_ref[1] = band_bias(1, 0)

    masks = head_masks()
    low_lane = iota((128, 128), 1) < HEAD_DIM
    own_k, own_v = k_ref[...], v_ref[...]
    left, right = left_ref[...], right_ref[...]

    def stat_row(ref, rows):
        turned = ref[rows, :].T
        return jnp.concatenate([turned[:1, :], turned[HEAD_DIM : HEAD_DIM + 1, :]], axis=1)

    dks, dvs = [], []
    for half in range(2):
        rows = slice(128 * half, 128 * (half + 1))
        keys = window(own_k, left, right, half, 0)
        vals = window(own_v, left, right, half, BLOCK)
        query = two_heads(q_ref[rows, :], masks)
        grad = two_heads(da_ref[rows, :], masks)
        scores = mm(keys, query, ((1,), (1,))) * SCALE + bias_ref[half]
        prob = jnp.exp(scores - stat_row(lse_ref, rows))
        prob_grad = mm(vals, grad, ((1,), (1,)))
        score_grad = (prob * (prob_grad - stat_row(delta_ref, rows))).astype(BF16)
        dks.append(mm(score_grad, query, ((1,), (0,))) * SCALE)
        dvs.append(mm(prob.astype(BF16), grad, ((1,), (0,))))
        dq = pick(mm(score_grad, keys, ((0,), (0,))), low_lane) * SCALE
        for b in range(2):
            block = 2 * half + b
            coarse = (
                cdq_ref[block : block + 1, :]
                + cdq_ref[4 + half : 5 + half, :]
                + cdq_ref[6:7, :]
            )
            gq_ref[BLOCK * block : BLOCK * (block + 1), :] = (
                dq[BLOCK * b : BLOCK * (b + 1), :] + coarse
            ).astype(BF16)
    for first, ref, at in ((dks, dk_ref, 0), (dvs, dv_ref, BLOCK)):
        low, high = first
        to_left_ref[at : at + BLOCK, :] = low[:BLOCK, :].astype(BF16)
        ref[:BLOCK, :] = low[BLOCK : 2 * BLOCK, :]
        ref[BLOCK : 3 * BLOCK, :] = low[2 * BLOCK :, :] + high[: 2 * BLOCK, :]
        ref[3 * BLOCK :, :] = high[2 * BLOCK : 3 * BLOCK, :]
        to_right_ref[at : at + BLOCK, :] = high[3 * BLOCK :, :].astype(BF16)


def fine_backward(q, k, v, left, right, da, lse, delta, cdq):
    tok = pair_spec(TOKENS)
    edge = pair_spec(2 * BLOCK)
    f_out = jax.ShapeDtypeStruct((TOKENS, HIDDEN), F32)
    e_out = jax.ShapeDtypeStruct((2 * BLOCK, HIDDEN), BF16)
    return pl.pallas_call(
        fine_backward_kernel,
        grid=(PAIRS,),
        in_specs=[tok, tok, tok, edge, edge, tok, tok, tok, pair_spec(LEVEL_ROWS)],
        out_specs=[tok, tok, tok, edge, edge],
        out_shape=(jax.ShapeDtypeStruct((TOKENS, HIDDEN), BF16), f_out, f_out, e_out, e_out),
        scratch_shapes=[pltpu.VMEM((2, 256, 256), F32)],
        cost_estimate=pl.CostEstimate(
            flops=5 * 16 * 2 * 256 * 256 * 128, transcendentals=16 * 256 * 256, bytes_accessed=8 << 20
        ),
        name="fine_backward",
    )(q, k, v, left, right, da, lse, delta, cdq)


def finish_kernel(dk_ref, dv_ref, from_left_ref, from_right_ref, coarse_ref, gk_ref, gv_ref):
    me = lax.axis_index("seq")
    row = iota((16, 256), 0)
    col = iota((16, 256), 1)
    dev = col // 8
    level_row = row % 8
    term = col % 8 - 4 * (row // 8)
    near = dev // 4 == me // 4
    mid = jnp.logical_and(dev // 16 == me // 16, jnp.logical_not(near))
    far = dev // 16 != me // 16
    one = jnp.logical_and(jnp.logical_and(level_row < 4, term == level_row), near)
    two = jnp.logical_and(jnp.logical_and(level_row // 2 == 2, term == level_row - 4), mid)
    three = jnp.logical_and(jnp.logical_and(level_row == 6, term == 0), far)
    chosen = jnp.logical_or(one, jnp.logical_or(two, three))
    sums = mm(jnp.where(chosen, 1.0, 0.0).astype(BF16), coarse_ref[...], ((1,), (0,)))
    for at, own_ref, out_ref in ((0, dk_ref, gk_ref), (8, dv_ref, gv_ref)):
        side = BLOCK * (at // 8)
        for b in range(4):
            rows = slice(BLOCK * b, BLOCK * (b + 1))
            c1, c2, c3 = at + b, at + 4 + b // 2, at + 6
            coarse = (
                sums[c1 : c1 + 1, :] * (1.0 / ROOTS[0])
                + sums[c2 : c2 + 1, :] * (1.0 / ROOTS[1])
                + sums[c3 : c3 + 1, :] * (1.0 / ROOTS[2])
            )
            value = own_ref[rows, :] + coarse
            if b == 0:
                value = value + from_left_ref[side : side + BLOCK, :].astype(F32)
            if b == 3:
                value = value + from_right_ref[side : side + BLOCK, :].astype(F32)
            out_ref[rows, :] = value.astype(BF16)


def finish(dk, dv, from_left, from_right, coarse):
    out = jax.ShapeDtypeStruct((TOKENS, HIDDEN), BF16)
    return pl.pallas_call(finish_kernel, out_shape=(out, out), name="finish")(
        dk, dv, from_left, from_right, coarse
    )


def swap(x, axis, bit):
    return lax.ppermute(x, axis, [(i, i ^ bit) for i in range(lax.axis_size(axis))])


def to_next(x):
    n = lax.axis_size("seq")
    return lax.ppermute(x, "seq", [(i, i + 1) for i in range(n - 1)])


def to_previous(x):
    n = lax.axis_size("seq")
    return lax.ppermute(x, "seq", [(i + 1, i) for i in range(n - 1)])


def exchanged(x, rows):
    parts = x.reshape(32, rows, HIDDEN)
    return lax.all_to_all(parts, "seq", split_axis=0, concat_axis=0, tiled=True)


def on_device(queries, keys, values, out_weight, cotangent):
    q, k, v, cot = queries[0], keys[0], values[0], cotangent[0]
    send, cq, first, last = pool(q, k, v)
    coarse_kv = exchanged(send, 8).reshape(256, HIDDEN)
    left = to_next(last)
    right = to_previous(first)
    d_att = lax.dot_general(
        cot, out_weight, (((1,), (1,)), ((), ())), preferred_element_type=F32
    ).astype(BF16)
    n0, m0, l0 = fine_forward(q, k, v, left, right)
    att, lse, delta, cdq, dkv = join(cq, coarse_kv, n0, m0, l0, d_att)
    kept, given = weight_terms(att, cot)
    got = swap(given, "dp", 1)
    back = exchanged(dkv, 8).reshape(256, HIDDEN)
    gq, dk, dv, to_left, to_right = fine_backward(q, k, v, left, right, d_att, lse, delta, cdq)
    from_left = to_next(to_right)
    from_right = to_previous(to_left)
    mixed = jnp.dot(att, out_weight, preferred_element_type=F32).astype(BF16)
    chip = (kept.astype(F32) + got.astype(F32)).astype(BF16)
    rows = exchanged(chip, 16).astype(F32).sum(axis=0)
    high = lax.axis_index("dp") // 2 == 1
    mine = jnp.where(high, rows[8:], rows[:8])
    other = jnp.where(high, rows[:8], rows[8:]).astype(BF16)
    grad_weight = mine + swap(other, "dp", 2).astype(F32)
    gk, gv = finish(dk, dv, from_left, from_right, back)
    return (mixed[None], grad_weight, gq[None], gk[None], gv[None])


def solution(mesh):
    tokens = P("dp", "seq", None)
    return jax.shard_map(
        on_device,
        mesh=mesh,
        in_specs=(tokens, tokens, tokens, P(), tokens),
        out_specs=(tokens, P(("dp", "seq"), None), tokens, tokens, tokens),
        check_vma=False,
    )
```

```python
import math

import jax
import jax.numpy as jnp
from jax import lax
from jax.experimental import pallas as pl
from jax.experimental.pallas import tpu as pltpu
from jax.sharding import PartitionSpec as P


HEADS = 16
HEAD_DIM = 64
BLOCK = 64
TOKENS = 256
HIDDEN = 1024
PAIRS = HIDDEN // 128
LEVEL_ROWS = 8
MASKED = -1e30
F32 = jnp.float32
BF16 = jnp.bfloat16
SCALE = 1.0 / math.sqrt(HEAD_DIM)
ROOTS = (math.sqrt(64.0), math.sqrt(128.0), math.sqrt(256.0))


def mm(a, b, dims):
    return lax.dot_general(a, b, (dims, ((), ())), preferred_element_type=F32)


def iota(shape, dim):
    return lax.broadcasted_iota(jnp.int32, shape, dim)


def local_call(kernel, outs, args, flops, scratch=(), exps=0, far_in=(), far_out=()):
    near = pl.BlockSpec(memory_space=pltpu.VMEM)
    far = pl.BlockSpec(memory_space=pltpu.HBM)
    held = [
        pltpu.with_memory_space_constraint(x, pltpu.HBM if i in far_in else pltpu.VMEM)
        for i, x in enumerate(args)
    ]
    return pl.pallas_call(
        kernel,
        in_specs=[far if i in far_in else near for i in range(len(args))],
        out_specs=tuple(far if i in far_out else near for i in range(len(outs))),
        out_shape=tuple(
            (pltpu.HBM if i in far_out else pltpu.VMEM)(*out) for i, out in enumerate(outs)
        ),
        scratch_shapes=list(scratch),
        compiler_params=pltpu.CompilerParams(vmem_limit_bytes=24 << 20),
        cost_estimate=pl.CostEstimate(flops=flops, transcendentals=exps, bytes_accessed=1 << 20),
    )(*held)


def pooled_levels(one):
    two = [one[0] + one[1], one[2] + one[3]]
    three = [two[0] + two[1]]
    return [[x / root for x in rows] for rows, root in zip((one, two, three), ROOTS)]


def pool_kernel(
    q_ref, k_ref, v_ref, send_ref, cq_ref, first_ref, last_ref, held_ref, out_ref, sems, edge_sems, out_sem
):
    me = lax.axis_index("seq")
    copies = {}
    for i, ref in ((1, k_ref), (2, v_ref), (0, q_ref)):
        for b in range(4):
            rows = pl.ds(BLOCK * b, BLOCK)
            copies[i, b] = pltpu.make_async_copy(ref.at[rows], held_ref.at[i, rows], sems.at[i, b])
            copies[i, b].start()
    edges = []
    for i, ref in enumerate((k_ref, v_ref)):
        to = pl.ds(BLOCK * i, BLOCK)
        edges.append(
            pltpu.make_async_copy(ref.at[pl.ds(0, BLOCK)], first_ref.at[to], edge_sems.at[i, 0])
        )
        edges.append(
            pltpu.make_async_copy(
                ref.at[pl.ds(TOKENS - BLOCK, BLOCK)], last_ref.at[to], edge_sems.at[i, 1]
            )
        )
    for copy in edges:
        copy.start()

    def sums(i):
        parts = []
        for b in range(4):
            copies[i, b].wait()
            rows = held_ref[i, BLOCK * b : BLOCK * (b + 1), :].astype(F32)
            parts.append(jnp.sum(rows, axis=0, keepdims=True))
        return parts

    zero = jnp.zeros((1, HIDDEN), F32)
    k1, k2, k3 = pooled_levels(sums(1))
    v1, v2, v3 = pooled_levels(sums(2))
    slot1 = jnp.concatenate(k1 + v1, axis=0)
    slot2 = jnp.concatenate(k2 + [zero] * 2 + v2 + [zero] * 2, axis=0)
    slot3 = jnp.concatenate(k3 + [zero] * 3 + v3 + [zero] * 3, axis=0)
    for g in range(8):
        slot = jnp.where(me // 4 == g, slot1, jnp.where(me // 16 == g // 4, slot2, slot3))
        out_ref[32 * g : 32 * (g + 1), :] = jnp.concatenate([slot] * 4, axis=0).astype(BF16)
    out = pltpu.make_async_copy(out_ref, send_ref, out_sem)
    out.start()
    q1, q2, q3 = pooled_levels(sums(0))
    cq_ref[...] = jnp.concatenate(q1 + q2 + q3 + [zero], axis=0).astype(BF16)
    for copy in edges:
        copy.wait()
    out.wait()


def pool(q, k, v):
    slab = ((2 * BLOCK, HIDDEN), BF16)
    return local_call(
        pool_kernel,
        [((256, HIDDEN), BF16), ((LEVEL_ROWS, HIDDEN), BF16), slab, slab],
        (q, k, v),
        3 * 256 * 1024,
        scratch=[
            pltpu.VMEM((3, TOKENS, HIDDEN), BF16),
            pltpu.VMEM((256, HIDDEN), BF16),
            pltpu.SemaphoreType.DMA((3, 4)),
            pltpu.SemaphoreType.DMA((2, 2)),
            pltpu.SemaphoreType.DMA,
        ],
        far_in=(0, 1, 2),
        far_out=(0,),
    )


def window(own, left, right, half, row):
    if half == 0:
        return jnp.concatenate([left[row : row + BLOCK, :], own[: 3 * BLOCK, :]], axis=0)
    return jnp.concatenate([own[BLOCK:, :], right[row : row + BLOCK, :]], axis=0)


def band_bias(half, key_dim):
    me = lax.axis_index("seq")
    key_block = iota((256, 256), key_dim) // BLOCK
    query_block = iota((256, 256), 1 - key_dim) // BLOCK % 2
    gap = key_block - query_block
    keep = jnp.logical_and(gap >= 0, gap <= 2)
    if half == 0:
        keep = jnp.logical_and(keep, key_block >= jnp.where(me > 0, 0, 1))
    else:
        last = lax.axis_size("seq") - 1
        keep = jnp.logical_and(keep, key_block <= jnp.where(me < last, 3, 2))
    return jnp.where(keep, 0.0, MASKED).astype(F32)


def head_masks(scale):
    lane = iota((1, 128), 1)
    low = jnp.where(lane < HEAD_DIM, scale, 0.0).astype(BF16)
    high = jnp.where(lane < HEAD_DIM, 0.0, scale).astype(BF16)
    return low, high


def two_heads(rows, masks):
    return jnp.concatenate([rows * masks[0], rows * masks[1]], axis=0)


def pick(stacked, low_lane):
    return jnp.where(low_lane, stacked[:128, :], stacked[128:, :])


def over_groups(body, count):
    width = 128 * count

    def step(g, carry):
        start = g * width
        lanes = [pl.ds(pl.multiple_of(start + 128 * p, 128), 128) for p in range(count)]
        body(g, lanes, pl.ds(pl.multiple_of(start, 128), width))
        return carry

    if count == PAIRS:
        body(0, [slice(128 * p, 128 * (p + 1)) for p in range(PAIRS)], slice(0, HIDDEN))
    else:
        lax.fori_loop(0, PAIRS // count, step, 0)


FORWARD_GROUP = 2
BACKWARD_GROUP = 2


def fine_forward_kernel(
    q_ref, k_ref, v_ref, left_ref, right_ref, a_out, lse_out, bias_ref, a_ref, lse_ref, sems, lse_sem
):
    bias_ref[0] = band_bias(0, 1)
    bias_ref[1] = band_bias(1, 1)
    masks = head_masks(SCALE)
    lane = iota((128, 128), 1)
    low_lane = lane < HEAD_DIM
    ones = jnp.ones((256, 128), BF16)
    lse_ref[...] = jnp.zeros((TOKENS, 128), F32)

    def out_copy(g, span):
        return pltpu.make_async_copy(a_ref.at[:, span], a_out.at[:, span], sems.at[g])

    def body(g, groups, span):
        units = [(p, lanes, half) for p, lanes in enumerate(groups) for half in range(2)]
        scores = []
        for p, lanes, half in units:
            rows = slice(128 * half, 128 * (half + 1))
            keys = window(k_ref.at[:, lanes], left_ref.at[:, lanes], right_ref.at[:, lanes], half, 0)
            query = two_heads(q_ref[rows, lanes], masks)
            scores.append(mm(query, keys, ((1,), (1,))) + bias_ref[half])
        tops = [jnp.max(x, axis=1, keepdims=True) for x in scores]
        weights = [jnp.exp(x - top).astype(BF16) for x, top in zip(scores, tops)]
        for (p, lanes, half), top, weight in zip(units, tops, weights):
            rows = slice(128 * half, 128 * (half + 1))
            vals = window(
                v_ref.at[:, lanes], left_ref.at[:, lanes], right_ref.at[:, lanes], half, BLOCK
            )
            both = mm(weight, jnp.concatenate([vals, ones], axis=1), ((1,), (0,)))
            total = both[:, 128:]
            a_ref[rows, lanes] = (pick(both[:, :128], low_lane) / pick(total, low_lane)).astype(BF16)
            lse = top + jnp.log(total)
            head = 2 * (g * len(groups) + p)
            lse_ref[rows, :] = jnp.where(
                lane == head, lse[:128, :], jnp.where(lane == head + 1, lse[128:, :], lse_ref[rows, :])
            )
        out_copy(g, span).start()

    over_groups(body, FORWARD_GROUP)
    lse_copy = pltpu.make_async_copy(lse_ref, lse_out, lse_sem)
    lse_copy.start()
    for g in range(PAIRS // FORWARD_GROUP):
        width = 128 * FORWARD_GROUP
        out_copy(g, pl.ds(width * g, width)).wait()
    lse_copy.wait()


def fine_forward(q, k, v, left, right):
    return local_call(
        fine_forward_kernel,
        [((TOKENS, HIDDEN), BF16), ((TOKENS, 128), F32)],
        (q, k, v, left, right),
        3 * 16 * 2 * 256 * 256 * 128,
        scratch=[
            pltpu.VMEM((2, 256, 256), F32),
            pltpu.VMEM((TOKENS, HIDDEN), BF16),
            pltpu.VMEM((TOKENS, 128), F32),
            pltpu.SemaphoreType.DMA((PAIRS // FORWARD_GROUP,)),
            pltpu.SemaphoreType.DMA,
        ],
        exps=16 * 256 * 256,
        far_out=(0, 1),
    )


def coarse_keep():
    me = lax.axis_index("seq")
    row = iota((128, 256), 0) % LEVEL_ROWS
    col = iota((128, 256), 1)
    dev = col // 8
    term = col % 8
    near = dev // 4 == me // 4
    mid = jnp.logical_and(dev // 16 == me // 16, jnp.logical_not(near))
    far = dev // 16 != me // 16
    apart = jnp.abs(4 * me + row - (4 * dev + term)) > 1
    one = jnp.logical_and(jnp.logical_and(row < 4, term < 4), jnp.logical_and(near, apart))
    two = jnp.logical_and(jnp.logical_and(row // 2 == 2, term < 2), mid)
    three = jnp.logical_and(jnp.logical_and(row == 6, term == 0), far)
    return jnp.logical_or(one, jnp.logical_or(two, three))


def by_head(rows, own):
    return jnp.concatenate([rows] * HEADS, axis=0) * own


def over_heads(stacked, own):
    return jnp.sum((stacked * own).reshape(HEADS, LEVEL_ROWS, HIDDEN), axis=0)


def three_terms(x):
    first = x.astype(BF16)
    rest = x - first.astype(F32)
    second = rest.astype(BF16)
    third = (rest - second.astype(F32)).astype(BF16)
    return jnp.concatenate([first, second, third], axis=1)


def join_kernel(
    cq_ref,
    kv_ref,
    a_hbm,
    lse0_hbm,
    da_hbm,
    att_ref,
    lse_ref,
    delta_ref,
    dq_ref,
    dkv_ref,
    give_ref,
    a_ref,
    da_ref,
    lse0_ref,
    m0_ref,
    mc_ref,
    nc_ref,
    g_ref,
    h_ref,
    sems,
):
    loads = [
        pltpu.make_async_copy(lse0_hbm, lse0_ref, sems.at[2]),
        pltpu.make_async_copy(a_hbm, a_ref, sems.at[0]),
        pltpu.make_async_copy(da_hbm, da_ref, sems.at[1]),
    ]
    for load in loads:
        load.start()
    own = jnp.where(
        iota((128, HIDDEN), 0) // LEVEL_ROWS == iota((128, HIDDEN), 1) // HEAD_DIM, 1.0, 0.0
    ).astype(F32)
    keep = coarse_keep()
    kv = kv_ref[...]
    query = by_head(cq_ref[...].astype(F32), own * SCALE).astype(BF16)
    scores = jnp.where(keep, mm(query, kv, ((1,), (1,))), MASKED)
    top = jnp.max(scores, axis=1, keepdims=True)
    weights = jnp.where(keep, jnp.exp(scores - top), 0.0)
    total = jnp.maximum(jnp.sum(weights, axis=1, keepdims=True), 1.0)
    on_values = pltpu.roll(weights, 4, 1).astype(BF16)
    inverse = 1.0 / total
    nc_ref[...] = over_heads(mm(on_values, kv, ((1,), (0,))) * inverse, own)
    mc_ref[...] = over_heads(jnp.broadcast_to(top + jnp.log(total), (128, HIDDEN)), own)
    same_head = jnp.where(
        iota((128, 128), 0) // HEAD_DIM == iota((128, 128), 1) // HEAD_DIM, 1.0, 0.0
    ).astype(BF16)
    spread = jnp.where(
        iota((384, HIDDEN), 0) % 128 == iota((384, HIDDEN), 1) // HEAD_DIM, 1.0, 0.0
    ).astype(BF16)
    for load in loads:
        load.wait()
    m0_ref[...] = mm(three_terms(lse0_ref[...]), spread, ((1,), (0,)))
    zero = jnp.zeros((1, 128), F32)

    def rows_of(parts):
        one, two, three = zip(*parts)
        return jnp.concatenate(
            list(one)
            + [two[0] + two[1], two[2] + two[3]]
            + [(three[0] + three[1]) + (three[2] + three[3]), zero],
            axis=0,
        )

    for p in range(PAIRS):
        lanes = slice(128 * p, 128 * (p + 1))
        g_parts, h_parts, lses, deltas = [], [], [], []
        for b in range(4):
            rows = slice(BLOCK * b, BLOCK * (b + 1))
            level = (b, 4 + b // 2, 6)
            m0 = m0_ref[rows, lanes]
            mc = [mc_ref[c : c + 1, lanes] for c in level]
            top_all = jnp.maximum(m0, jnp.maximum(mc[0], jnp.maximum(mc[1], mc[2])))
            f0 = jnp.exp(m0 - top_all)
            fc = [jnp.exp(x - top_all) for x in mc]
            inv = 1.0 / (f0 + fc[0] + (fc[1] + fc[2]))
            num = a_ref[rows, lanes].astype(F32) * f0
            for c, f in zip(level, fc):
                num = num + nc_ref[c : c + 1, lanes] * f
            att = (num * inv).astype(BF16)
            att_ref[rows, lanes] = att
            lses.append(top_all - jnp.log(inv))
            da = da_ref[rows, lanes].astype(F32)
            product = da * att.astype(F32)
            part = product.astype(BF16)
            rest = (product - part.astype(F32)).astype(BF16)
            delta = mm(part, same_head, ((1,), (0,))) + mm(rest, same_head, ((1,), (0,)))
            deltas.append(delta)
            wc = [f * inv for f in fc]
            g_parts.append([jnp.sum(w * da, axis=0, keepdims=True) for w in wc])
            h_parts.append([jnp.sum(w * delta, axis=0, keepdims=True) for w in wc])
        for parts, ref in ((lses, lse_ref), (deltas, delta_ref)):
            turned = jnp.concatenate(parts, axis=0).T
            for half in range(2):
                span = slice(128 * half, 128 * (half + 1))
                ref[p, half : half + 1, :] = jnp.concatenate(
                    [turned[:1, span], turned[HEAD_DIM : HEAD_DIM + 1, span]], axis=1
                )
        g_ref[:, lanes] = rows_of(g_parts)
        h_ref[:, lanes] = rows_of(h_parts)
    core = lax.axis_index("dp") % 2
    for hi in range(2):
        start = pl.multiple_of((2 * hi + 1 - core) * 256, 256)
        give_ref[:, 256 * hi : 256 * (hi + 1)] = att_ref[:, pl.ds(start, 256)]
    grads = (by_head(g_ref[...], own) * inverse).astype(BF16)
    sums = jnp.sum(by_head(h_ref[...], own), axis=1, keepdims=True) * (inverse * (1.0 / HEAD_DIM))
    on_keys = pltpu.roll(mm(grads, kv, ((1,), (1,))), 252, 1)
    score_grad = (weights * (on_keys - sums)).astype(BF16)
    row = iota((LEVEL_ROWS, 1), 0)
    share = jnp.where(row < 4, 1.0 / ROOTS[0], jnp.where(row < 6, 1.0 / ROOTS[1], 1.0 / ROOTS[2]))
    dq_ref[...] = over_heads(mm(score_grad, kv, ((1,), (0,))), own) * (share.astype(F32) * SCALE)
    left = jnp.concatenate([score_grad, on_values], axis=0)
    right = jnp.concatenate([query, grads], axis=0)
    dkv_ref[...] = mm(left, right, ((0,), (0,))).astype(BF16)


def join(cq, kv, a, lse0, da):
    stat = ((PAIRS, 2, 256), F32)
    level = pltpu.VMEM((LEVEL_ROWS, HIDDEN), F32)
    return local_call(
        join_kernel,
        [
            ((TOKENS, HIDDEN), BF16),
            stat,
            stat,
            ((LEVEL_ROWS, HIDDEN), F32),
            ((256, HIDDEN), BF16),
            ((TOKENS, 512), BF16),
        ],
        (cq, kv, a, lse0, da),
        5 * 2 * 128 * 256 * 1024,
        scratch=[
            pltpu.VMEM((TOKENS, HIDDEN), BF16),
            pltpu.VMEM((TOKENS, HIDDEN), BF16),
            pltpu.VMEM((TOKENS, 128), F32),
            pltpu.VMEM((TOKENS, HIDDEN), F32),
            level,
            level,
            level,
            level,
            pltpu.SemaphoreType.DMA((3,)),
        ],
        exps=6 * 256 * 1024,
        far_in=(2, 3, 4),
    )


SLOT = 48


def weight_kernel(
    att_ref, got_ref, cot_ref, peer_cot_ref, dkv_ref, send_out, lhs_ref, send_ref, sems
):
    core = lax.axis_index("dp") % 2
    for hi in range(2):
        start = pl.multiple_of((2 * hi + core) * 256, 256)
        rows = slice(256 * hi, 256 * (hi + 1))
        lhs_ref[rows, :TOKENS] = att_ref[:, pl.ds(start, 256)].T
        lhs_ref[rows, TOKENS:] = got_ref[:, rows].T
    width = 256
    copies = []
    for j in range(HIDDEN // width):
        cols = slice(width * j, width * (j + 1))
        cot = jnp.concatenate([cot_ref[:, cols], peer_cot_ref[:, cols]], axis=0)
        terms = mm(lhs_ref[...], cot, ((1,), (0,))).reshape(2, 16, 16, width)
        coarse = dkv_ref[:, cols].astype(F32).reshape(16, 16, width)
        slots = jnp.concatenate([coarse, terms[0], terms[1]], axis=1)
        send_ref[:, cols] = slots.reshape(16 * SLOT, width).astype(BF16)
        span = pl.ds(width * j, width)
        copies.append(
            pltpu.make_async_copy(send_ref.at[:, span], send_out.at[:, span], sems.at[j])
        )
        copies[-1].start()
    for copy in copies:
        copy.wait()


def weight_terms(att, got, cot, peer_cot, dkv):
    return local_call(
        weight_kernel,
        [((16 * SLOT, HIDDEN), BF16)],
        (att, got, cot, peer_cot, dkv),
        2 * 512 * 512 * 1024,
        scratch=[
            pltpu.VMEM((512, 512), BF16),
            pltpu.VMEM((16 * SLOT, HIDDEN), BF16),
            pltpu.SemaphoreType.DMA((4,)),
        ],
        far_out=(0,),
    )[0]


def stat_row(ref, pair, start, count):
    half, at = start // 128, start % 128
    row = ref[pair, half : half + 1, :]
    if count == 128:
        return row
    return jnp.concatenate([row[:, at : at + count], row[:, 128 + at : 128 + at + count]], axis=1)


def edge_backward_kernel(
    q_hbm,
    da_hbm,
    k_hbm,
    v_hbm,
    left_hbm,
    right_hbm,
    lse_ref,
    delta_ref,
    to_left_ref,
    to_right_ref,
    q_ref,
    da_ref,
    k_ref,
    v_ref,
    left_ref,
    right_ref,
    part_sems,
    sems,
):
    me = lax.axis_index("seq")
    now, later = [], []
    for i, (far, near) in enumerate(((left_hbm, left_ref), (right_hbm, right_ref))):
        now.append(pltpu.make_async_copy(far, near, sems.at[i]))
    for i, (far, near) in enumerate(((q_hbm, q_ref), (da_hbm, da_ref))):
        for at, (start, size) in enumerate(
            ((0, BLOCK), (TOKENS - BLOCK, BLOCK), (BLOCK, TOKENS - 2 * BLOCK))
        ):
            rows = pl.ds(start, size)
            copy = pltpu.make_async_copy(far.at[rows], near.at[rows], part_sems.at[i, at])
            (now if at < 2 else later).append(copy)
    for i, (far, near) in enumerate(((k_hbm, k_ref), (v_hbm, v_ref))):
        later.append(pltpu.make_async_copy(far, near, sems.at[2 + i]))
    for copy in now + later:
        copy.start()
    for copy in now:
        copy.wait()
    masks = head_masks(1.0)
    scaled = head_masks(SCALE)
    last = lax.axis_size("seq") - 1
    left_bias = jnp.where(me > 0, 0.0, MASKED).astype(F32)
    right_bias = jnp.where(me < last, 0.0, MASKED).astype(F32)

    def body(g, groups, span):
        units = []
        for p, lanes in enumerate(groups):
            pair = g * len(groups) + p
            units.append((pair, lanes, 0, left_ref, to_left_ref, left_bias))
            units.append((pair, lanes, TOKENS - BLOCK, right_ref, to_right_ref, right_bias))
        held = []
        for pair, lanes, start, near_ref, out_ref, bias in units:
            rows = slice(start, start + BLOCK)
            query = two_heads(q_ref[rows, lanes], scaled)
            grad = two_heads(da_ref[rows, lanes], masks)
            scores = mm(near_ref[:BLOCK, lanes], query, ((1,), (1,))) + bias
            prob_grad = mm(near_ref[BLOCK:, lanes], grad, ((1,), (1,)))
            held.append((query, grad, scores, prob_grad))
        probs = [
            jnp.exp(h[2] - stat_row(lse_ref, u[0], u[2], BLOCK)) for u, h in zip(units, held)
        ]
        for (pair, lanes, start, near_ref, out_ref, bias), (query, grad, _, prob_grad), prob in zip(
            units, held, probs
        ):
            delta = stat_row(delta_ref, pair, start, BLOCK)
            score_grad = (prob * (prob_grad - delta)).astype(BF16)
            out_ref[:BLOCK, lanes] = mm(score_grad, query, ((1,), (0,))).astype(BF16)
            out_ref[BLOCK:, lanes] = mm(prob.astype(BF16), grad, ((1,), (0,))).astype(BF16)

    over_groups(body, PAIRS)
    for copy in later:
        copy.wait()


def edge_backward(q, da, k, v, left, right, lse, delta):
    slab = ((2 * BLOCK, HIDDEN), BF16)
    tokens = ((TOKENS, HIDDEN), BF16)
    return local_call(
        edge_backward_kernel,
        [slab, slab, tokens, tokens, tokens, tokens, slab, slab],
        (q, da, k, v, left, right, lse, delta),
        4 * 16 * 2 * 64 * 128 * 128,
        scratch=[pltpu.SemaphoreType.DMA((2, 3)), pltpu.SemaphoreType.DMA((4,))],
        far_in=(0, 1, 2, 3, 4, 5),
        exps=16 * 64 * 128,
    )


def fine_backward_kernel(
    q_ref,
    k_ref,
    v_ref,
    left_ref,
    right_ref,
    da_ref,
    lse_ref,
    delta_ref,
    cdq_ref,
    gq_out,
    dk_out,
    dv_out,
    bias_ref,
    gq_ref,
    dk_ref,
    dv_ref,
    sems,
):
    bias_ref[0] = band_bias(0, 0)
    bias_ref[1] = band_bias(1, 0)
    masks = head_masks(1.0)
    scaled = head_masks(SCALE)
    low_lane = iota((128, 128), 1) < HEAD_DIM

    def copies(g, span):
        held_refs = (gq_ref, dk_ref, dv_ref)
        return [
            pltpu.make_async_copy(ref.at[:, span], out.at[:, span], sems.at[i, g])
            for i, (ref, out) in enumerate(zip(held_refs, (gq_out, dk_out, dv_out)))
        ]

    def body(g, groups, span):
        units = [
            (g * len(groups) + p, lanes, half) for p, lanes in enumerate(groups) for half in range(2)
        ]
        held = []
        for pair, lanes, half in units:
            rows = slice(128 * half, 128 * (half + 1))
            near = (left_ref.at[:, lanes], right_ref.at[:, lanes], half)
            keys = window(k_ref.at[:, lanes], *near, 0)
            vals = window(v_ref.at[:, lanes], *near, BLOCK)
            query = two_heads(q_ref[rows, lanes], scaled)
            grad = two_heads(da_ref[rows, lanes], masks)
            scores = mm(keys, query, ((1,), (1,))) + bias_ref[half]
            prob_grad = mm(vals, grad, ((1,), (1,)))
            held.append((keys, query, grad, scores, prob_grad))
        probs = [
            jnp.exp(h[3] - stat_row(lse_ref, u[0], 128 * u[2], 128)) for u, h in zip(units, held)
        ]
        parts = []
        for (pair, lanes, half), (keys, query, grad, _, prob_grad), prob in zip(
            units, held, probs
        ):
            rows = slice(128 * half, 128 * (half + 1))
            delta = stat_row(delta_ref, pair, 128 * half, 128)
            score_grad = (prob * (prob_grad - delta)).astype(BF16)
            dk = mm(score_grad, query, ((1,), (0,)))
            dv = mm(prob.astype(BF16), grad, ((1,), (0,)))
            parts.append((dk, dv))
            dq = pick(mm(score_grad, keys, ((0,), (0,))), low_lane) * SCALE
            for b in range(2):
                block = 2 * half + b
                coarse = (
                    cdq_ref[block : block + 1, lanes]
                    + cdq_ref[4 + half : 5 + half, lanes]
                    + cdq_ref[6:7, lanes]
                )
                gq_ref[BLOCK * block : BLOCK * (block + 1), lanes] = (
                    dq[BLOCK * b : BLOCK * (b + 1), :] + coarse
                ).astype(BF16)
        for p, lanes in enumerate(groups):
            for ref, low, high in zip((dk_ref, dv_ref), parts[2 * p], parts[2 * p + 1]):
                ref[:BLOCK, lanes] = low[BLOCK : 2 * BLOCK, :].astype(BF16)
                middle = low[2 * BLOCK :, :] + high[: 2 * BLOCK, :]
                ref[BLOCK : 3 * BLOCK, lanes] = middle.astype(BF16)
                ref[3 * BLOCK :, lanes] = high[2 * BLOCK : 3 * BLOCK, :].astype(BF16)
        for copy in copies(g, span):
            copy.start()

    over_groups(body, BACKWARD_GROUP)
    width = 128 * BACKWARD_GROUP
    for g in range(PAIRS // BACKWARD_GROUP):
        for copy in copies(g, pl.ds(width * g, width)):
            copy.wait()


def fine_backward(q, k, v, left, right, da, lse, delta, cdq):
    out = ((TOKENS, HIDDEN), BF16)
    return local_call(
        fine_backward_kernel,
        [out, out, out],
        (q, k, v, left, right, da, lse, delta, cdq),
        5 * 16 * 2 * 256 * 256 * 128,
        scratch=[pltpu.VMEM((2, 256, 256), F32)]
        + [pltpu.VMEM((TOKENS, HIDDEN), BF16)] * 3
        + [pltpu.SemaphoreType.DMA((3, PAIRS // BACKWARD_GROUP))],
        exps=16 * 256 * 256,
        far_out=(0, 1, 2),
    )


def sums_kernel(
    got_ref,
    dk_hbm,
    dv_hbm,
    coarse_ref,
    mine_ref,
    to_low_ref,
    to_high_ref,
    to_both_ref,
    dk_ref,
    dv_ref,
    sems,
):
    copies = [
        pltpu.make_async_copy(dk_hbm, dk_ref, sems.at[0]),
        pltpu.make_async_copy(dv_hbm, dv_ref, sems.at[1]),
    ]
    for copy in copies:
        copy.start()
    me = lax.axis_index("seq")
    low, column = me % 2, me // 2
    high = lax.axis_index("dp") // 2
    row = iota((64, 16 * SLOT), 0)
    col = iota((64, 16 * SLOT), 1)
    source = col // SLOT
    at = col % SLOT
    near = source // 2 == column // 2
    mid = jnp.logical_and(source // 8 == column // 8, jnp.logical_not(near))
    far = source // 8 != column // 8
    level_row = row % 8
    side = jnp.where(row < 16, low, 1 - low)
    term = at - 8 * side - 4 * (row // 8 % 2)
    one = jnp.logical_and(jnp.logical_and(level_row < 4, term == level_row), near)
    two = jnp.logical_and(jnp.logical_and(level_row // 2 == 2, term == level_row - 4), mid)
    three = jnp.logical_and(jnp.logical_and(level_row == 6, term == 0), far)
    coarse = jnp.logical_and(jnp.logical_or(one, jnp.logical_or(two, three)), row < 32)
    block = row // 8 - 4
    block_high = jnp.where(block < 2, high, 1 - high)
    block_low = jnp.where(block % 2 == 0, low, 1 - low)
    weight = jnp.logical_and(row >= 32, at == 16 + 16 * block_high + 8 * block_low + level_row)
    chosen = jnp.where(jnp.logical_or(coarse, weight), 1.0, 0.0).astype(BF16)
    sums = mm(chosen, got_ref[...], ((1,), (0,)))
    coarse_ref[...] = sums[:16, :]
    mine_ref[...] = sums[32:40, :]
    to_low_ref[:16, :] = sums[16:32, :].astype(BF16)
    to_low_ref[16:, :] = sums[40:48, :].astype(BF16)
    to_high_ref[...] = sums[48:56, :].astype(BF16)
    to_both_ref[...] = sums[56:, :].astype(BF16)
    for copy in copies:
        copy.wait()


def all_sums(got, dk, dv):
    return local_call(
        sums_kernel,
        [
            ((16, HIDDEN), F32),
            ((8, HIDDEN), F32),
            ((24, HIDDEN), BF16),
            ((8, HIDDEN), BF16),
            ((8, HIDDEN), BF16),
            ((TOKENS, HIDDEN), BF16),
            ((TOKENS, HIDDEN), BF16),
        ],
        (got, dk, dv),
        2 * 64 * 768 * 1024,
        scratch=[pltpu.SemaphoreType.DMA((2,))],
        far_in=(1, 2),
    )


def finish_kernel(
    dk_ref,
    dv_ref,
    from_left_ref,
    from_right_ref,
    sums_ref,
    low_ref,
    gk_out,
    gv_out,
    gk_ref,
    gv_ref,
    sems,
):
    copies = []
    sums = sums_ref[...] + low_ref[:16, :].astype(F32)
    for at, own_ref, out_ref, out in ((0, dk_ref, gk_ref, gk_out), (8, dv_ref, gv_ref, gv_out)):
        side = BLOCK * (at // 8)
        for b in range(4):
            rows = slice(BLOCK * b, BLOCK * (b + 1))
            c1, c2, c3 = at + b, at + 4 + b // 2, at + 6
            coarse = (
                sums[c1 : c1 + 1, :] * (1.0 / ROOTS[0])
                + sums[c2 : c2 + 1, :] * (1.0 / ROOTS[1])
                + sums[c3 : c3 + 1, :] * (1.0 / ROOTS[2])
            )
            value = own_ref[rows, :].astype(F32) + coarse
            if b == 0:
                value = value + from_left_ref[side : side + BLOCK, :].astype(F32)
            if b == 3:
                value = value + from_right_ref[side : side + BLOCK, :].astype(F32)
            out_ref[rows, :] = value.astype(BF16)
            span = pl.ds(BLOCK * b, BLOCK)
            copies.append(
                pltpu.make_async_copy(out_ref.at[span], out.at[span], sems.at[at // 8, b])
            )
            copies[-1].start()
    for copy in copies:
        copy.wait()


def finish(dk, dv, from_left, from_right, sums, low):
    out = ((TOKENS, HIDDEN), BF16)
    return local_call(
        finish_kernel,
        [out, out],
        (dk, dv, from_left, from_right, sums, low),
        16 * 256 * 1024,
        scratch=[pltpu.VMEM((TOKENS, HIDDEN), BF16)] * 2 + [pltpu.SemaphoreType.DMA((2, 4))],
        far_out=(0, 1),
    )


def swap(x, axis, bit):
    return lax.ppermute(x, axis, [(i, i ^ bit) for i in range(lax.axis_size(axis))])


def to_next(x):
    n = lax.axis_size("seq")
    return lax.ppermute(x, "seq", [(i, i + 1) for i in range(n - 1)])


def to_previous(x):
    n = lax.axis_size("seq")
    return lax.ppermute(x, "seq", [(i + 1, i) for i in range(n - 1)])


def swap_both(x):
    n = lax.axis_size("seq")
    total = n * lax.axis_size("dp")
    return lax.ppermute(x, ("dp", "seq"), [(i, i ^ (2 * n + 1)) for i in range(total)])


def exchanged(x):
    parts = x.reshape(32, 8, HIDDEN)
    got = lax.all_to_all(parts, "seq", split_axis=0, concat_axis=0, tiled=True)
    return got.reshape(256, HIDDEN)


def exchanged_back(x):
    parts = x.reshape(16, SLOT, HIDDEN)
    groups = [[2 * j + low for j in range(16)] for low in range(2)]
    got = lax.all_to_all(
        parts, "seq", split_axis=0, concat_axis=0, tiled=True, axis_index_groups=groups
    )
    return got.reshape(16 * SLOT, HIDDEN)


def body(q, k, v, out_weight, cot):
    send, cq, first, last = pool(q, k, v)
    left = to_next(last)
    right = to_previous(first)
    coarse_kv = exchanged(send)
    peer_cot = swap(cot, "dp", 1)
    d_att = lax.dot_general(
        cot, out_weight, (((1,), (1,)), ((), ())), preferred_element_type=F32
    ).astype(BF16)
    a0, lse0 = fine_forward(q, k, v, left, right)
    att, lse, delta, cdq, dkv, give = join(cq, coarse_kv, a0, lse0, d_att)
    got = swap(give, "dp", 1)
    mixed = jnp.dot(att, out_weight, preferred_element_type=F32).astype(BF16)
    send_back = weight_terms(att, got, cot, peer_cot, dkv)
    back = exchanged_back(send_back)
    to_left, to_right, *near = edge_backward(q, d_att, k, v, left, right, lse, delta)
    from_left = to_next(to_right)
    from_right = to_previous(to_left)
    near_q, near_da, near_k, near_v, near_left, near_right = near
    gq, dk, dv = fine_backward(
        near_q, near_k, near_v, near_left, near_right, near_da, lse, delta, cdq
    )
    sums, mine, to_low, to_high, to_both, dk, dv = all_sums(back, dk, dv)
    low = swap(to_low, "seq", 1)
    high = swap(to_high, "dp", 2)
    both = swap_both(to_both)
    gk, gv = finish(dk, dv, from_left, from_right, sums, low)
    grad_weight = (mine + low[16:].astype(F32)) + (high.astype(F32) + both.astype(F32))
    return (mixed[None], grad_weight, gq[None], gk[None], gv[None])


def on_device(queries, keys, values, out_weight, cotangent):
    return body(queries[0], keys[0], values[0], out_weight, cotangent[0])


def solution(mesh):
    tokens = P("dp", "seq", None)
    return jax.shard_map(
        on_device,
        mesh=mesh,
        in_specs=(tokens, tokens, tokens, P(), tokens),
        out_specs=(tokens, P(("dp", "seq"), None), tokens, tokens, tokens),
        check_vma=False,
    )
```

```python
import math

import jax
import jax.numpy as jnp
from jax import lax
from jax.experimental import pallas as pl
from jax.experimental.pallas import tpu as pltpu
from jax.sharding import PartitionSpec as P


HEADS = 16
HEAD_DIM = 64
BLOCK = 64
TOKENS = 256
HIDDEN = 1024
PAIRS = HIDDEN // 128
LEVEL_ROWS = 8
MASKED = -1e30
F32 = jnp.float32
BF16 = jnp.bfloat16
SCALE = 1.0 / math.sqrt(HEAD_DIM)
ROOTS = (math.sqrt(64.0), math.sqrt(128.0), math.sqrt(256.0))


def mm(a, b, dims):
    return lax.dot_general(a, b, (dims, ((), ())), preferred_element_type=F32)


def iota(shape, dim):
    return lax.broadcasted_iota(jnp.int32, shape, dim)


def local_call(kernel, outs, args, flops, scratch=(), exps=0, far_in=(), far_out=()):
    near = pl.BlockSpec(memory_space=pltpu.VMEM)
    far = pl.BlockSpec(memory_space=pltpu.HBM)
    held = [
        pltpu.with_memory_space_constraint(x, pltpu.HBM if i in far_in else pltpu.VMEM)
        for i, x in enumerate(args)
    ]
    return pl.pallas_call(
        kernel,
        in_specs=[far if i in far_in else near for i in range(len(args))],
        out_specs=tuple(far if i in far_out else near for i in range(len(outs))),
        out_shape=tuple(
            (pltpu.HBM if i in far_out else pltpu.VMEM)(*out) for i, out in enumerate(outs)
        ),
        scratch_shapes=list(scratch),
        compiler_params=pltpu.CompilerParams(vmem_limit_bytes=24 << 20),
        cost_estimate=pl.CostEstimate(flops=flops, transcendentals=exps, bytes_accessed=1 << 20),
    )(*held)


def pooled_levels(one):
    two = [one[0] + one[1], one[2] + one[3]]
    three = [two[0] + two[1]]
    return [[x / root for x in rows] for rows, root in zip((one, two, three), ROOTS)]


def pool_kernel(
    q_ref, k_ref, v_ref, levels_ref, cq_ref, inner_ref, outer_ref, held_ref, sems, edge_sems
):
    me = lax.axis_index("seq")
    copies = {}
    for i, ref in ((1, k_ref), (2, v_ref), (0, q_ref)):
        for b in range(4):
            rows = pl.ds(BLOCK * b, BLOCK)
            copies[i, b] = pltpu.make_async_copy(ref.at[rows], held_ref.at[i, rows], sems.at[i, b])
            copies[i, b].start()
    inner = pl.multiple_of((1 - me % 2) * (TOKENS - BLOCK), BLOCK)
    outer = pl.multiple_of((me % 2) * (TOKENS - BLOCK), BLOCK)
    edges = []
    for i, ref in enumerate((k_ref, v_ref)):
        to = pl.ds(BLOCK * i, BLOCK)
        for j, (start, out) in enumerate(((inner, inner_ref), (outer, outer_ref))):
            edges.append(
                pltpu.make_async_copy(ref.at[pl.ds(start, BLOCK)], out.at[to], edge_sems.at[i, j])
            )
    for copy in edges:
        copy.start()

    def sums(i):
        parts = []
        for b in range(4):
            copies[i, b].wait()
            rows = held_ref[i, BLOCK * b : BLOCK * (b + 1), :].astype(F32)
            parts.append(jnp.sum(rows, axis=0, keepdims=True))
        return parts

    zero = jnp.zeros((1, HIDDEN), F32)
    k1, k2, k3 = pooled_levels(sums(1))
    v1, v2, v3 = pooled_levels(sums(2))
    slot1 = jnp.concatenate(k1 + v1, axis=0)
    slot2 = jnp.concatenate(k2 + [zero] * 2 + v2 + [zero] * 2, axis=0)
    slot3 = jnp.concatenate(k3 + [zero] * 3 + v3 + [zero] * 3, axis=0)
    levels_ref[...] = jnp.concatenate([slot1, slot2, slot3], axis=0).astype(BF16)
    q1, q2, q3 = pooled_levels(sums(0))
    cq_ref[...] = jnp.concatenate(q1 + q2 + q3 + [zero], axis=0).astype(BF16)
    for copy in edges:
        copy.wait()


def pool(q, k, v):
    slab = ((2 * BLOCK, HIDDEN), BF16)
    return local_call(
        pool_kernel,
        [((24, HIDDEN), BF16), ((LEVEL_ROWS, HIDDEN), BF16), slab, slab],
        (q, k, v),
        3 * 256 * 1024,
        scratch=[
            pltpu.VMEM((3, TOKENS, HIDDEN), BF16),
            pltpu.SemaphoreType.DMA((3, 4)),
            pltpu.SemaphoreType.DMA((2, 2)),
        ],
        far_in=(0, 1, 2),
    )


def slots_kernel(own_ref, peer_ref, send_out, send_ref, sem):
    column = lax.axis_index("seq") // 2
    own, peer = own_ref[...].astype(F32), peer_ref[...].astype(F32)
    one, two, three = [
        jnp.concatenate([own[8 * i : 8 * (i + 1)], peer[8 * i : 8 * (i + 1)]], axis=0).astype(BF16)
        for i in range(3)
    ]
    for j in range(16):
        slot = jnp.where(column // 2 == j // 2, one, jnp.where(column // 8 == j // 8, two, three))
        send_ref[16 * j : 16 * (j + 1), :] = slot
    copy = pltpu.make_async_copy(send_ref, send_out, sem)
    copy.start()
    copy.wait()


def slots(own, peer):
    return local_call(
        slots_kernel,
        [((256, HIDDEN), BF16)],
        (own, peer),
        256 * 1024,
        scratch=[pltpu.VMEM((256, HIDDEN), BF16), pltpu.SemaphoreType.DMA],
        far_out=(0,),
    )[0]


def window(own, left, right, half, row):
    if half == 0:
        return jnp.concatenate([left[row : row + BLOCK, :], own[: 3 * BLOCK, :]], axis=0)
    return jnp.concatenate([own[BLOCK:, :], right[row : row + BLOCK, :]], axis=0)


def band_bias(half, key_dim):
    me = lax.axis_index("seq")
    key_block = iota((256, 256), key_dim) // BLOCK
    query_block = iota((256, 256), 1 - key_dim) // BLOCK % 2
    gap = key_block - query_block
    keep = jnp.logical_and(gap >= 0, gap <= 2)
    if half == 0:
        keep = jnp.logical_and(keep, key_block >= jnp.where(me > 0, 0, 1))
    else:
        last = lax.axis_size("seq") - 1
        keep = jnp.logical_and(keep, key_block <= jnp.where(me < last, 3, 2))
    return jnp.where(keep, 0.0, MASKED).astype(F32)


def head_masks(scale):
    lane = iota((1, 128), 1)
    low = jnp.where(lane < HEAD_DIM, scale, 0.0).astype(BF16)
    high = jnp.where(lane < HEAD_DIM, 0.0, scale).astype(BF16)
    return low, high


def two_heads(rows, masks):
    return jnp.concatenate([rows * masks[0], rows * masks[1]], axis=0)


def pick(stacked, low_lane):
    return jnp.where(low_lane, stacked[:128, :], stacked[128:, :])


def over_groups(body, count):
    width = 128 * count

    def step(g, carry):
        start = g * width
        lanes = [pl.ds(pl.multiple_of(start + 128 * p, 128), 128) for p in range(count)]
        body(g, lanes, pl.ds(pl.multiple_of(start, 128), width))
        return carry

    if count == PAIRS:
        body(0, [slice(128 * p, 128 * (p + 1)) for p in range(PAIRS)], slice(0, HIDDEN))
    else:
        lax.fori_loop(0, PAIRS // count, step, 0)


def by_parity(inner, outer):
    odd = lax.axis_index("seq") % 2 == 1
    return jnp.where(odd, inner, outer), jnp.where(odd, outer, inner)


FORWARD_GROUP = 2
BACKWARD_GROUP = 2
RIM_GROUP = 4


def soft_rows(scores, vals, low_lane, rows):
    top = jnp.max(scores, axis=1, keepdims=True)
    weight = jnp.exp(scores - top).astype(BF16)
    ones = jnp.ones((vals.shape[0], 128), BF16)
    both = mm(weight, jnp.concatenate([vals, ones], axis=1), ((1,), (0,)))
    total = both[:, 128:]
    part = jnp.where(low_lane, both[:rows, :128], both[rows:, :128])
    share = jnp.where(low_lane, total[:rows], total[rows:])
    return (part / share).astype(BF16), top + jnp.log(total)


def place(ref, span, lse, lane, head, rows):
    ref[span, :] = jnp.where(
        lane == head, lse[:rows, :], jnp.where(lane == head + 1, lse[rows:, :], ref[span, :])
    )


def inside_kernel(
    q_ref,
    k_ref,
    v_ref,
    cot_ref,
    w_hbm,
    a_out,
    lse_out,
    da_out,
    a_ref,
    lse_ref,
    w_ref,
    da_ref,
    sems,
    lse_sem,
    w_sems,
    da_sems,
):
    steps = PAIRS // FORWARD_GROUP
    width = 128 * FORWARD_GROUP

    def w_copy(g):
        rows = pl.ds(pl.multiple_of(width * g, width), width)
        return pltpu.make_async_copy(w_hbm.at[rows], w_ref.at[rows], w_sems.at[g])

    def da_copy(g, span):
        return pltpu.make_async_copy(da_ref.at[:, span], da_out.at[:, span], da_sems.at[g])

    def a_copy(g, span):
        return pltpu.make_async_copy(a_ref.at[:, span], a_out.at[:, span], sems.at[g])

    for g in range(steps):
        w_copy(g).start()
    gap = iota((256, 256), 1) // BLOCK - iota((256, 256), 0) // BLOCK % 2
    bias = jnp.where(jnp.logical_and(gap >= 0, gap <= 2), 0.0, MASKED).astype(F32)
    masks = head_masks(SCALE)
    lane = iota((128, 128), 1)
    low_lane = lane < HEAD_DIM
    lse_ref[...] = jnp.zeros((128, 128), F32)

    def body(g, groups, span):
        scores = []
        for lanes in groups:
            query = two_heads(q_ref[BLOCK : 3 * BLOCK, lanes], masks)
            scores.append(mm(query, k_ref[:, lanes], ((1,), (1,))) + bias)
        for p, (lanes, score) in enumerate(zip(groups, scores)):
            a_ref[:, lanes], lse = soft_rows(score, v_ref[:, lanes], low_lane, 128)
            place(lse_ref, slice(0, 128), lse, lane, 2 * (g * len(groups) + p), 128)
        a_copy(g, span).start()
        w_copy(g).wait()
        rows = pl.ds(pl.multiple_of(width * g, width), width)
        da_ref[:, span] = mm(cot_ref[...], w_ref[rows, :], ((1,), (1,))).astype(BF16)
        da_copy(g, span).start()

    over_groups(body, FORWARD_GROUP)
    lse_copy = pltpu.make_async_copy(lse_ref, lse_out, lse_sem)
    lse_copy.start()
    for g in range(steps):
        a_copy(g, pl.ds(width * g, width)).wait()
        da_copy(g, pl.ds(width * g, width)).wait()
    lse_copy.wait()


def inside_forward(q, k, v, cot, w):
    steps = PAIRS // FORWARD_GROUP
    return local_call(
        inside_kernel,
        [((128, HIDDEN), BF16), ((128, 128), F32), ((TOKENS, HIDDEN), BF16)],
        (q, k, v, cot, w),
        3 * 16 * 2 * 128 * 256 * 128 + 2 * 256 * 1024 * 1024,
        scratch=[
            pltpu.VMEM((128, HIDDEN), BF16),
            pltpu.VMEM((128, 128), F32),
            pltpu.VMEM((HIDDEN, HIDDEN), BF16),
            pltpu.VMEM((TOKENS, HIDDEN), BF16),
            pltpu.SemaphoreType.DMA((steps,)),
            pltpu.SemaphoreType.DMA,
            pltpu.SemaphoreType.DMA((steps,)),
            pltpu.SemaphoreType.DMA((steps,)),
        ],
        exps=8 * 256 * 256,
        far_in=(4,),
        far_out=(0, 1, 2),
    )


def rim_kernel(
    q_ref, k_ref, v_ref, inner_ref, outer_ref, a_out, lse_out, left_ref, right_ref, a_ref, lse_ref, sems
):
    left_ref[...], right_ref[...] = by_parity(inner_ref[...], outer_ref[...])
    me = lax.axis_index("seq")
    last = lax.axis_size("seq") - 1
    key_lane = iota((128, 192), 1)
    starts = (
        jnp.where(jnp.logical_and(key_lane < BLOCK, me == 0), MASKED, 0.0).astype(F32),
        jnp.where(jnp.logical_and(key_lane >= 2 * BLOCK, me == last), MASKED, 0.0).astype(F32),
    )
    masks = head_masks(SCALE)
    lane = iota((BLOCK, 128), 1)
    low_lane = lane < HEAD_DIM
    lse_ref[...] = jnp.zeros((128, 128), F32)

    def body(g, groups, span):
        units = [(p, lanes, side) for p, lanes in enumerate(groups) for side in range(2)]
        scores = []
        for p, lanes, side in units:
            at = side * (TOKENS - BLOCK)
            query = two_heads(q_ref[at : at + BLOCK, lanes], masks)
            if side == 0:
                keys = jnp.concatenate([left_ref[:BLOCK, lanes], k_ref[: 2 * BLOCK, lanes]], axis=0)
            else:
                keys = jnp.concatenate([k_ref[2 * BLOCK :, lanes], right_ref[:BLOCK, lanes]], axis=0)
            scores.append(mm(query, keys, ((1,), (1,))) + starts[side])
        for (p, lanes, side), score in zip(units, scores):
            if side == 0:
                vals = jnp.concatenate([left_ref[BLOCK:, lanes], v_ref[: 2 * BLOCK, lanes]], axis=0)
            else:
                vals = jnp.concatenate([v_ref[2 * BLOCK :, lanes], right_ref[BLOCK:, lanes]], axis=0)
            rows = slice(BLOCK * side, BLOCK * (side + 1))
            a_ref[rows, lanes], lse = soft_rows(score, vals, low_lane, BLOCK)
            place(lse_ref, rows, lse, lane, 2 * (g * len(groups) + p), BLOCK)

    over_groups(body, RIM_GROUP)
    copies = [
        pltpu.make_async_copy(a_ref, a_out, sems.at[0]),
        pltpu.make_async_copy(lse_ref, lse_out, sems.at[1]),
    ]
    for copy in copies:
        copy.start()
    for copy in copies:
        copy.wait()


def rim_forward(q, k, v, inner, outer):
    return local_call(
        rim_kernel,
        [((128, HIDDEN), BF16), ((128, 128), F32)],
        (q, k, v, inner, outer),
        3 * 16 * 2 * 128 * 192 * 128,
        scratch=[
            pltpu.VMEM((2 * BLOCK, HIDDEN), BF16),
            pltpu.VMEM((2 * BLOCK, HIDDEN), BF16),
            pltpu.VMEM((128, HIDDEN), BF16),
            pltpu.VMEM((128, 128), F32),
            pltpu.SemaphoreType.DMA((2,)),
        ],
        exps=16 * 128 * 192,
        far_out=(0, 1),
    )


def coarse_keep():
    me = lax.axis_index("seq")
    row = iota((128, 256), 0) % LEVEL_ROWS
    col = iota((128, 256), 1)
    same = me % 2
    dev = 2 * (col // 16) + same + (1 - 2 * same) * (col % 16 // 8)
    term = col % 8
    near = dev // 4 == me // 4
    mid = jnp.logical_and(dev // 16 == me // 16, jnp.logical_not(near))
    far = dev // 16 != me // 16
    apart = jnp.abs(4 * me + row - (4 * dev + term)) > 1
    one = jnp.logical_and(jnp.logical_and(row < 4, term < 4), jnp.logical_and(near, apart))
    two = jnp.logical_and(jnp.logical_and(row // 2 == 2, term < 2), mid)
    three = jnp.logical_and(jnp.logical_and(row == 6, term == 0), far)
    return jnp.logical_or(one, jnp.logical_or(two, three))


def by_head(rows, own):
    return jnp.concatenate([rows] * HEADS, axis=0) * own


def over_heads(stacked, own):
    return jnp.sum((stacked * own).reshape(HEADS, LEVEL_ROWS, HIDDEN), axis=0)


def three_terms(x):
    first = x.astype(BF16)
    rest = x - first.astype(F32)
    second = rest.astype(BF16)
    third = (rest - second.astype(F32)).astype(BF16)
    return jnp.concatenate([first, second, third], axis=1)


def join_kernel(
    cq_ref,
    kv_ref,
    a_mid_hbm,
    lse_mid_hbm,
    a_rim_hbm,
    lse_rim_hbm,
    da_hbm,
    w_hbm,
    att_ref,
    lse_ref,
    delta_ref,
    dq_ref,
    packed_ref,
    own_ref,
    near_ref,
    give_ref,
    w_ref,
    a_ref,
    da_ref,
    lse0_ref,
    m0_ref,
    mc_ref,
    nc_ref,
    g_ref,
    h_ref,
    dkv_ref,
    sems,
):
    loads = [
        pltpu.make_async_copy(da_hbm, da_ref, sems.at[0]),
    ]
    mid = pl.ds(BLOCK, 2 * BLOCK)
    for i, (mid_hbm, rim_hbm, ref) in enumerate(
        ((lse_mid_hbm, lse_rim_hbm, lse0_ref), (a_mid_hbm, a_rim_hbm, a_ref))
    ):
        loads.append(pltpu.make_async_copy(mid_hbm, ref.at[mid], sems.at[2 + 3 * i]))
        for side in range(2):
            to = pl.ds(side * (TOKENS - BLOCK), BLOCK)
            rows = pl.ds(side * BLOCK, BLOCK)
            sem = sems.at[3 + 3 * i + side]
            loads.append(pltpu.make_async_copy(rim_hbm.at[rows], ref.at[to], sem))
    w_copy = pltpu.make_async_copy(w_hbm, w_ref, sems.at[1])
    for load in loads:
        load.start()
    w_copy.start()
    own = jnp.where(
        iota((128, HIDDEN), 0) // LEVEL_ROWS == iota((128, HIDDEN), 1) // HEAD_DIM, 1.0, 0.0
    ).astype(F32)
    keep = coarse_keep()
    kv = kv_ref[...]
    query = by_head(cq_ref[...].astype(F32), own * SCALE).astype(BF16)
    scores = jnp.where(keep, mm(query, kv, ((1,), (1,))), MASKED)
    top = jnp.max(scores, axis=1, keepdims=True)
    weights = jnp.where(keep, jnp.exp(scores - top), 0.0)
    total = jnp.maximum(jnp.sum(weights, axis=1, keepdims=True), 1.0)
    on_values = pltpu.roll(weights, 4, 1).astype(BF16)
    inverse = 1.0 / total
    nc_ref[...] = over_heads(mm(on_values, kv, ((1,), (0,))) * inverse, own)
    mc_ref[...] = over_heads(jnp.broadcast_to(top + jnp.log(total), (128, HIDDEN)), own)
    same_head = jnp.where(
        iota((128, 128), 0) // HEAD_DIM == iota((128, 128), 1) // HEAD_DIM, 1.0, 0.0
    ).astype(BF16)
    spread = jnp.where(
        iota((384, HIDDEN), 0) % 128 == iota((384, HIDDEN), 1) // HEAD_DIM, 1.0, 0.0
    ).astype(BF16)
    for load in loads:
        load.wait()
    m0_ref[...] = mm(three_terms(lse0_ref[...]), spread, ((1,), (0,)))
    zero = jnp.zeros((1, 128), F32)

    def rows_of(parts):
        one, two, three = zip(*parts)
        return jnp.concatenate(
            list(one)
            + [two[0] + two[1], two[2] + two[3]]
            + [(three[0] + three[1]) + (three[2] + three[3]), zero],
            axis=0,
        )

    for p in range(PAIRS):
        lanes = slice(128 * p, 128 * (p + 1))
        g_parts, h_parts, lses, deltas = [], [], [], []
        for b in range(4):
            rows = slice(BLOCK * b, BLOCK * (b + 1))
            level = (b, 4 + b // 2, 6)
            m0 = m0_ref[rows, lanes]
            mc = [mc_ref[c : c + 1, lanes] for c in level]
            top_all = jnp.maximum(m0, jnp.maximum(mc[0], jnp.maximum(mc[1], mc[2])))
            f0 = jnp.exp(m0 - top_all)
            fc = [jnp.exp(x - top_all) for x in mc]
            inv = 1.0 / (f0 + fc[0] + (fc[1] + fc[2]))
            num = a_ref[rows, lanes].astype(F32) * f0
            for c, f in zip(level, fc):
                num = num + nc_ref[c : c + 1, lanes] * f
            att = (num * inv).astype(BF16)
            att_ref[rows, lanes] = att
            lses.append(top_all - jnp.log(inv))
            da = da_ref[rows, lanes].astype(F32)
            product = da * att.astype(F32)
            part = product.astype(BF16)
            rest = (product - part.astype(F32)).astype(BF16)
            delta = mm(part, same_head, ((1,), (0,))) + mm(rest, same_head, ((1,), (0,)))
            deltas.append(delta)
            wc = [f * inv for f in fc]
            g_parts.append([jnp.sum(w * da, axis=0, keepdims=True) for w in wc])
            h_parts.append([jnp.sum(w * delta, axis=0, keepdims=True) for w in wc])
        for parts, ref in ((lses, lse_ref), (deltas, delta_ref)):
            turned = jnp.concatenate(parts, axis=0).T
            for half in range(2):
                span = slice(128 * half, 128 * (half + 1))
                ref[p, half : half + 1, :] = jnp.concatenate(
                    [turned[:1, span], turned[HEAD_DIM : HEAD_DIM + 1, span]], axis=1
                )
        g_ref[:, lanes] = rows_of(g_parts)
        h_ref[:, lanes] = rows_of(h_parts)
    core = lax.axis_index("dp") % 2
    for hi in range(2):
        start = pl.multiple_of((2 * hi + 1 - core) * 256, 256)
        give_ref[:, 256 * hi : 256 * (hi + 1)] = att_ref[:, pl.ds(start, 256)]
    grads = (by_head(g_ref[...], own) * inverse).astype(BF16)
    sums = jnp.sum(by_head(h_ref[...], own), axis=1, keepdims=True) * (inverse * (1.0 / HEAD_DIM))
    on_keys = pltpu.roll(mm(grads, kv, ((1,), (1,))), 252, 1)
    score_grad = (weights * (on_keys - sums)).astype(BF16)
    row = iota((LEVEL_ROWS, 1), 0)
    share = jnp.where(row < 4, 1.0 / ROOTS[0], jnp.where(row < 6, 1.0 / ROOTS[1], 1.0 / ROOTS[2]))
    dq_ref[...] = over_heads(mm(score_grad, kv, ((1,), (0,))), own) * (share.astype(F32) * SCALE)
    left = jnp.concatenate([score_grad, on_values], axis=0)
    right = jnp.concatenate([query, grads], axis=0)
    dkv = mm(left, right, ((0,), (0,))).astype(BF16)
    dkv_ref[...] = dkv
    row, col = iota((128, 256), 0), iota((128, 256), 1)
    taken = 16 * (row // 8) + 8 * (row % 8 // 4) + 4 * (row % 4 // 2) + row % 2
    pick_rows = jnp.where(col == taken, 1.0, 0.0).astype(BF16)
    packed_ref[...] = mm(pick_rows, dkv, ((1,), (0,))).astype(BF16)
    column = lax.axis_index("seq") // 2
    other = column + 1 - 2 * (column % 2)
    own_ref[...] = dkv_ref[pl.ds(pl.multiple_of(16 * column, 16), 16), :]
    near_ref[...] = dkv_ref[pl.ds(pl.multiple_of(16 * other, 16), 16), :]
    w_copy.wait()


def join(cq, kv, inside, rim, da, w):
    stat = ((PAIRS, 2, 256), F32)
    level = pltpu.VMEM((LEVEL_ROWS, HIDDEN), F32)
    return local_call(
        join_kernel,
        [
            ((TOKENS, HIDDEN), BF16),
            stat,
            stat,
            ((LEVEL_ROWS, HIDDEN), F32),
            ((128, HIDDEN), BF16),
            ((16, HIDDEN), BF16),
            ((16, HIDDEN), BF16),
            ((TOKENS, 512), BF16),
            ((HIDDEN, HIDDEN), BF16),
        ],
        (cq, kv, *inside, *rim, da, w),
        5 * 2 * 128 * 256 * 1024,
        scratch=[
            pltpu.VMEM((TOKENS, HIDDEN), BF16),
            pltpu.VMEM((TOKENS, HIDDEN), BF16),
            pltpu.VMEM((TOKENS, 128), F32),
            pltpu.VMEM((TOKENS, HIDDEN), F32),
            level,
            level,
            level,
            level,
            pltpu.VMEM((256, HIDDEN), BF16),
            pltpu.SemaphoreType.DMA((8,)),
        ],
        exps=6 * 256 * 1024,
        far_in=(2, 3, 4, 5, 6, 7),
    )


SLOT = 40


def weight_kernel(
    att_ref, got_ref, cot_ref, peer_cot_ref, packed_ref, send_ref, lhs_ref
):
    core = lax.axis_index("dp") % 2
    for hi in range(2):
        start = pl.multiple_of((2 * hi + core) * 256, 256)
        rows = slice(256 * hi, 256 * (hi + 1))
        lhs_ref[rows, :TOKENS] = att_ref[:, pl.ds(start, 256)].T
        lhs_ref[rows, TOKENS:] = got_ref[:, rows].T
    width = 256
    for j in range(HIDDEN // width):
        cols = slice(width * j, width * (j + 1))
        cot = jnp.concatenate([cot_ref[:, cols], peer_cot_ref[:, cols]], axis=0)
        terms = mm(lhs_ref[...], cot, ((1,), (0,))).reshape(2, 16, 16, width)
        coarse = packed_ref[:, cols].astype(F32).reshape(16, 8, width)
        slots = jnp.concatenate([coarse, terms[0], terms[1]], axis=1)
        send_ref[:, cols] = slots.reshape(16 * SLOT, width).astype(BF16)


def weight_terms(att, got, cot, peer_cot, packed):
    return local_call(
        weight_kernel,
        [((16 * SLOT, HIDDEN), BF16)],
        (att, got, cot, peer_cot, packed),
        2 * 512 * 512 * 1024,
        scratch=[pltpu.VMEM((512, 512), BF16)],
    )[0]


def stat_row(ref, pair, start, count):
    half, at = start // 128, start % 128
    row = ref[pair, half : half + 1, :]
    if count == 128:
        return row
    return jnp.concatenate([row[:, at : at + count], row[:, 128 + at : 128 + at + count]], axis=1)


def edge_backward_kernel(
    q_hbm,
    da_hbm,
    k_hbm,
    v_hbm,
    inner_hbm,
    outer_hbm,
    lse_ref,
    delta_ref,
    to_inner_ref,
    to_outer_ref,
    q_ref,
    da_ref,
    k_ref,
    v_ref,
    left_ref,
    right_ref,
    to_left_ref,
    to_right_ref,
    inner_ref,
    outer_ref,
    part_sems,
    sems,
):
    me = lax.axis_index("seq")
    now, later = [], []
    for i, (far, near) in enumerate(((inner_hbm, inner_ref), (outer_hbm, outer_ref))):
        now.append(pltpu.make_async_copy(far, near, sems.at[i]))
    for i, (far, near) in enumerate(((q_hbm, q_ref), (da_hbm, da_ref))):
        for at, (start, size) in enumerate(
            ((0, BLOCK), (TOKENS - BLOCK, BLOCK), (BLOCK, TOKENS - 2 * BLOCK))
        ):
            rows = pl.ds(start, size)
            copy = pltpu.make_async_copy(far.at[rows], near.at[rows], part_sems.at[i, at])
            (now if at < 2 else later).append(copy)
    for i, (far, near) in enumerate(((k_hbm, k_ref), (v_hbm, v_ref))):
        later.append(pltpu.make_async_copy(far, near, sems.at[2 + i]))
    for copy in now + later:
        copy.start()
    for copy in now:
        copy.wait()
    left_ref[...], right_ref[...] = by_parity(inner_ref[...], outer_ref[...])
    masks = head_masks(1.0)
    scaled = head_masks(SCALE)
    last = lax.axis_size("seq") - 1
    left_bias = jnp.where(me > 0, 0.0, MASKED).astype(F32)
    right_bias = jnp.where(me < last, 0.0, MASKED).astype(F32)

    def body(g, groups, span):
        units = []
        for p, lanes in enumerate(groups):
            pair = g * len(groups) + p
            units.append((pair, lanes, 0, left_ref, to_left_ref, left_bias))
            units.append((pair, lanes, TOKENS - BLOCK, right_ref, to_right_ref, right_bias))
        held = []
        for pair, lanes, start, near_ref, out_ref, bias in units:
            rows = slice(start, start + BLOCK)
            query = two_heads(q_ref[rows, lanes], scaled)
            grad = two_heads(da_ref[rows, lanes], masks)
            scores = mm(near_ref[:BLOCK, lanes], query, ((1,), (1,))) + bias
            prob_grad = mm(near_ref[BLOCK:, lanes], grad, ((1,), (1,)))
            held.append((query, grad, scores, prob_grad))
        probs = [
            jnp.exp(h[2] - stat_row(lse_ref, u[0], u[2], BLOCK)) for u, h in zip(units, held)
        ]
        for (pair, lanes, start, near_ref, out_ref, bias), (query, grad, _, prob_grad), prob in zip(
            units, held, probs
        ):
            delta = stat_row(delta_ref, pair, start, BLOCK)
            score_grad = (prob * (prob_grad - delta)).astype(BF16)
            out_ref[:BLOCK, lanes] = mm(score_grad, query, ((1,), (0,))).astype(BF16)
            out_ref[BLOCK:, lanes] = mm(prob.astype(BF16), grad, ((1,), (0,))).astype(BF16)

    over_groups(body, PAIRS)
    to_inner_ref[...], to_outer_ref[...] = by_parity(to_left_ref[...], to_right_ref[...])
    for copy in later:
        copy.wait()


def edge_backward(q, da, k, v, inner, outer, lse, delta):
    slab = ((2 * BLOCK, HIDDEN), BF16)
    tokens = ((TOKENS, HIDDEN), BF16)
    return local_call(
        edge_backward_kernel,
        [slab, slab, tokens, tokens, tokens, tokens, slab, slab],
        (q, da, k, v, inner, outer, lse, delta),
        4 * 16 * 2 * 64 * 128 * 128,
        scratch=[pltpu.VMEM((2 * BLOCK, HIDDEN), BF16)] * 4
        + [pltpu.SemaphoreType.DMA((2, 3)), pltpu.SemaphoreType.DMA((4,))],
        far_in=(0, 1, 2, 3, 4, 5),
        exps=16 * 64 * 128,
    )


def fine_backward_kernel(
    q_ref,
    k_ref,
    v_ref,
    left_ref,
    right_ref,
    da_ref,
    lse_ref,
    delta_ref,
    cdq_ref,
    gq_out,
    dk_out,
    dv_out,
    bias_ref,
    gq_ref,
    dk_ref,
    dv_ref,
    sems,
):
    bias_ref[0] = band_bias(0, 0)
    bias_ref[1] = band_bias(1, 0)
    masks = head_masks(1.0)
    scaled = head_masks(SCALE)
    low_lane = iota((128, 128), 1) < HEAD_DIM

    def copies(g, span):
        held_refs = (gq_ref, dk_ref, dv_ref)
        return [
            pltpu.make_async_copy(ref.at[:, span], out.at[:, span], sems.at[i, g])
            for i, (ref, out) in enumerate(zip(held_refs, (gq_out, dk_out, dv_out)))
        ]

    def body(g, groups, span):
        units = [
            (g * len(groups) + p, lanes, half) for p, lanes in enumerate(groups) for half in range(2)
        ]
        held = []
        for pair, lanes, half in units:
            rows = slice(128 * half, 128 * (half + 1))
            near = (left_ref.at[:, lanes], right_ref.at[:, lanes], half)
            keys = window(k_ref.at[:, lanes], *near, 0)
            vals = window(v_ref.at[:, lanes], *near, BLOCK)
            query = two_heads(q_ref[rows, lanes], scaled)
            grad = two_heads(da_ref[rows, lanes], masks)
            scores = mm(keys, query, ((1,), (1,))) + bias_ref[half]
            prob_grad = mm(vals, grad, ((1,), (1,)))
            held.append((keys, query, grad, scores, prob_grad))
        probs = [
            jnp.exp(h[3] - stat_row(lse_ref, u[0], 128 * u[2], 128)) for u, h in zip(units, held)
        ]
        parts = []
        for (pair, lanes, half), (keys, query, grad, _, prob_grad), prob in zip(
            units, held, probs
        ):
            rows = slice(128 * half, 128 * (half + 1))
            delta = stat_row(delta_ref, pair, 128 * half, 128)
            score_grad = (prob * (prob_grad - delta)).astype(BF16)
            dk = mm(score_grad, query, ((1,), (0,)))
            dv = mm(prob.astype(BF16), grad, ((1,), (0,)))
            parts.append((dk, dv))
            dq = pick(mm(score_grad, keys, ((0,), (0,))), low_lane) * SCALE
            for b in range(2):
                block = 2 * half + b
                coarse = (
                    cdq_ref[block : block + 1, lanes]
                    + cdq_ref[4 + half : 5 + half, lanes]
                    + cdq_ref[6:7, lanes]
                )
                gq_ref[BLOCK * block : BLOCK * (block + 1), lanes] = (
                    dq[BLOCK * b : BLOCK * (b + 1), :] + coarse
                ).astype(BF16)
        for p, lanes in enumerate(groups):
            for ref, low, high in zip((dk_ref, dv_ref), parts[2 * p], parts[2 * p + 1]):
                ref[:BLOCK, lanes] = low[BLOCK : 2 * BLOCK, :].astype(BF16)
                middle = low[2 * BLOCK :, :] + high[: 2 * BLOCK, :]
                ref[BLOCK : 3 * BLOCK, lanes] = middle.astype(BF16)
                ref[3 * BLOCK :, lanes] = high[2 * BLOCK : 3 * BLOCK, :].astype(BF16)
        for copy in copies(g, span):
            copy.start()

    over_groups(body, BACKWARD_GROUP)
    width = 128 * BACKWARD_GROUP
    for g in range(PAIRS // BACKWARD_GROUP):
        for copy in copies(g, pl.ds(width * g, width)):
            copy.wait()


def fine_backward(q, k, v, left, right, da, lse, delta, cdq):
    out = ((TOKENS, HIDDEN), BF16)
    return local_call(
        fine_backward_kernel,
        [out, out, out],
        (q, k, v, left, right, da, lse, delta, cdq),
        5 * 16 * 2 * 256 * 256 * 128,
        scratch=[pltpu.VMEM((2, 256, 256), F32)]
        + [pltpu.VMEM((TOKENS, HIDDEN), BF16)] * 3
        + [pltpu.SemaphoreType.DMA((3, PAIRS // BACKWARD_GROUP))],
        exps=16 * 256 * 256,
        far_out=(0, 1, 2),
    )


def sums_kernel(
    got_ref,
    near_ref,
    own_ref,
    dk_hbm,
    dv_hbm,
    coarse_ref,
    mine_ref,
    to_low_ref,
    to_high_ref,
    to_both_ref,
    dk_ref,
    dv_ref,
    sems,
):
    copies = [
        pltpu.make_async_copy(dk_hbm, dk_ref, sems.at[0]),
        pltpu.make_async_copy(dv_hbm, dv_ref, sems.at[1]),
    ]
    for copy in copies:
        copy.start()
    me = lax.axis_index("seq")
    low, column = me % 2, me // 2
    high = lax.axis_index("dp") // 2
    row = iota((64, 16 * SLOT), 0)
    col = iota((64, 16 * SLOT), 1)
    source = col // SLOT
    at = col % SLOT
    near = source // 2 == column // 2
    mid = jnp.logical_and(source // 8 == column // 8, jnp.logical_not(near))
    far = source // 8 != column // 8
    level_row = row % 8
    side = jnp.where(row < 16, 0, 1)
    term = at - 4 * side - 2 * (row // 8 % 2)
    two = jnp.logical_and(jnp.logical_and(level_row // 2 == 2, term == level_row - 4), mid)
    three = jnp.logical_and(jnp.logical_and(level_row == 6, term == 0), far)
    coarse = jnp.logical_and(jnp.logical_or(two, three), row < 32)
    block = row // 8 - 4
    block_high = jnp.where(block < 2, high, 1 - high)
    block_low = jnp.where(block % 2 == 0, low, 1 - low)
    weight = jnp.logical_and(row >= 32, at == 8 + 16 * block_high + 8 * block_low + level_row)
    chosen = jnp.where(jnp.logical_or(coarse, weight), 1.0, 0.0).astype(BF16)
    sums = mm(chosen, got_ref[...], ((1,), (0,)))
    row = iota((32, 32), 0)
    col = iota((32, 32), 1) % 16
    side = jnp.where(row < 16, 0, 1)
    first = jnp.logical_and(row % 8 < 4, col == 8 * side + 4 * (row // 8 % 2) + row % 8)
    close = jnp.concatenate([near_ref[...], own_ref[...]], axis=0)
    coarse_sums = sums[:32, :] + mm(jnp.where(first, 1.0, 0.0).astype(BF16), close, ((1,), (0,)))
    coarse_ref[...] = coarse_sums[:16, :]
    mine_ref[...] = sums[32:40, :]
    to_low_ref[:16, :] = coarse_sums[16:, :].astype(BF16)
    to_low_ref[16:, :] = sums[40:48, :].astype(BF16)
    to_high_ref[...] = sums[48:56, :].astype(BF16)
    to_both_ref[...] = sums[56:, :].astype(BF16)
    for copy in copies:
        copy.wait()


def all_sums(got, near, own, dk, dv):
    return local_call(
        sums_kernel,
        [
            ((16, HIDDEN), F32),
            ((8, HIDDEN), F32),
            ((24, HIDDEN), BF16),
            ((8, HIDDEN), BF16),
            ((8, HIDDEN), BF16),
            ((TOKENS, HIDDEN), BF16),
            ((TOKENS, HIDDEN), BF16),
        ],
        (got, near, own, dk, dv),
        2 * 64 * 640 * 1024,
        scratch=[pltpu.SemaphoreType.DMA((2,))],
        far_in=(3, 4),
    )


def finish_kernel(
    dk_ref,
    dv_ref,
    inner_ref,
    outer_ref,
    sums_ref,
    low_ref,
    gk_out,
    gv_out,
    gk_ref,
    gv_ref,
    sems,
):
    copies = []
    sums = sums_ref[...] + low_ref[:16, :].astype(F32)
    from_left, from_right = by_parity(inner_ref[...], outer_ref[...])
    for at, own_ref, out_ref, out in ((0, dk_ref, gk_ref, gk_out), (8, dv_ref, gv_ref, gv_out)):
        side = BLOCK * (at // 8)
        for b in range(4):
            rows = slice(BLOCK * b, BLOCK * (b + 1))
            c1, c2, c3 = at + b, at + 4 + b // 2, at + 6
            coarse = (
                sums[c1 : c1 + 1, :] * (1.0 / ROOTS[0])
                + sums[c2 : c2 + 1, :] * (1.0 / ROOTS[1])
                + sums[c3 : c3 + 1, :] * (1.0 / ROOTS[2])
            )
            value = own_ref[rows, :].astype(F32) + coarse
            if b == 0:
                value = value + from_left[side : side + BLOCK, :].astype(F32)
            if b == 3:
                value = value + from_right[side : side + BLOCK, :].astype(F32)
            out_ref[rows, :] = value.astype(BF16)
            span = pl.ds(BLOCK * b, BLOCK)
            copies.append(
                pltpu.make_async_copy(out_ref.at[span], out.at[span], sems.at[at // 8, b])
            )
            copies[-1].start()
    for copy in copies:
        copy.wait()


def finish(dk, dv, inner, outer, sums, low):
    out = ((TOKENS, HIDDEN), BF16)
    return local_call(
        finish_kernel,
        [out, out],
        (dk, dv, inner, outer, sums, low),
        16 * 256 * 1024,
        scratch=[pltpu.VMEM((TOKENS, HIDDEN), BF16)] * 2 + [pltpu.SemaphoreType.DMA((2, 4))],
        far_out=(0, 1),
    )


def swap(x, axis, bit):
    return lax.ppermute(x, axis, [(i, i ^ bit) for i in range(lax.axis_size(axis))])


def swap_inner(x):
    return swap(x, "seq", 1)


def swap_outer(x):
    n = lax.axis_size("seq")
    return lax.ppermute(x, "seq", [(i, i + 1 if i % 2 else i - 1) for i in range(1, n - 1)])


def swap_both(x):
    n = lax.axis_size("seq")
    total = n * lax.axis_size("dp")
    return lax.ppermute(x, ("dp", "seq"), [(i, i ^ (2 * n + 1)) for i in range(total)])


def exchanged(x, rows):
    groups = [[2 * j + low for j in range(16)] for low in range(2)]
    got = lax.all_to_all(
        x.reshape(16, rows, HIDDEN),
        "seq",
        split_axis=0,
        concat_axis=0,
        tiled=True,
        axis_index_groups=groups,
    )
    return got.reshape(16 * rows, HIDDEN)


def body(q, k, v, out_weight, cot):
    levels, cq, inner, outer = pool(q, k, v)
    peer_levels = swap(levels, "seq", 1)
    outer = swap_outer(outer)
    inner = swap_inner(inner)
    send = slots(levels, peer_levels)
    coarse_kv = exchanged(send, 16)
    peer_cot = swap(cot, "dp", 1)
    *inside, d_att = inside_forward(q, k, v, cot, out_weight)
    rim = rim_forward(q, k, v, inner, outer)
    att, lse, delta, cdq, packed, own_rows, near_rows, give, near_w = join(
        cq, coarse_kv, inside, rim, d_att, out_weight
    )
    got = swap(give, "dp", 1)
    mixed = jnp.dot(att, near_w, preferred_element_type=F32).astype(BF16)
    send_back = weight_terms(att, got, cot, peer_cot, packed)
    back = exchanged(send_back, SLOT)
    near_rows = swap(near_rows, "seq", 2)
    to_inner, to_outer, *near = edge_backward(q, d_att, k, v, inner, outer, lse, delta)
    from_outer = swap_outer(to_outer)
    from_inner = swap_inner(to_inner)
    near_q, near_da, near_k, near_v, near_left, near_right = near
    gq, dk, dv = fine_backward(
        near_q, near_k, near_v, near_left, near_right, near_da, lse, delta, cdq
    )
    sums, mine, to_low, to_high, to_both, dk, dv = all_sums(
        back, near_rows, own_rows, dk, dv
    )
    low = swap(to_low, "seq", 1)
    high = swap(to_high, "dp", 2)
    both = swap_both(to_both)
    gk, gv = finish(dk, dv, from_inner, from_outer, sums, low)
    grad_weight = (mine + low[16:].astype(F32)) + (high.astype(F32) + both.astype(F32))
    return (mixed[None], grad_weight, gq[None], gk[None], gv[None])


def on_device(queries, keys, values, out_weight, cotangent):
    return body(queries[0], keys[0], values[0], out_weight, cotangent[0])


def solution(mesh):
    tokens = P("dp", "seq", None)
    return jax.shard_map(
        on_device,
        mesh=mesh,
        in_specs=(tokens, tokens, tokens, P(), tokens),
        out_specs=(tokens, P(("dp", "seq"), None), tokens, tokens, tokens),
        check_vma=False,
    )
```

```python
import math

import jax
import jax.numpy as jnp
from jax import lax
from jax.experimental import pallas as pl
from jax.experimental.pallas import tpu as pltpu
from jax.sharding import PartitionSpec as P


HEADS = 16
HEAD_DIM = 64
BLOCK = 64
TOKENS = 256
HIDDEN = 1024
PAIRS = HIDDEN // 128
LEVEL_ROWS = 8
MASKED = -1e30
F32 = jnp.float32
BF16 = jnp.bfloat16
SCALE = 1.0 / math.sqrt(HEAD_DIM)
ROOTS = (math.sqrt(64.0), math.sqrt(128.0), math.sqrt(256.0))


def mm(a, b, dims):
    return lax.dot_general(a, b, (dims, ((), ())), preferred_element_type=F32)


def iota(shape, dim):
    return lax.broadcasted_iota(jnp.int32, shape, dim)


def local_call(kernel, outs, args, flops, scratch=(), exps=0, far_in=(), far_out=()):
    near = pl.BlockSpec(memory_space=pltpu.VMEM)
    far = pl.BlockSpec(memory_space=pltpu.HBM)
    held = [
        pltpu.with_memory_space_constraint(x, pltpu.HBM if i in far_in else pltpu.VMEM)
        for i, x in enumerate(args)
    ]
    return pl.pallas_call(
        kernel,
        in_specs=[far if i in far_in else near for i in range(len(args))],
        out_specs=tuple(far if i in far_out else near for i in range(len(outs))),
        out_shape=tuple(
            (pltpu.HBM if i in far_out else pltpu.VMEM)(*out) for i, out in enumerate(outs)
        ),
        scratch_shapes=list(scratch),
        compiler_params=pltpu.CompilerParams(vmem_limit_bytes=24 << 20),
        cost_estimate=pl.CostEstimate(flops=flops, transcendentals=exps, bytes_accessed=1 << 20),
    )(*held)


def pooled_levels(one):
    two = [one[0] + one[1], one[2] + one[3]]
    three = [two[0] + two[1]]
    return [[x / root for x in rows] for rows, root in zip((one, two, three), ROOTS)]


def pool_kernel(
    q_ref, k_ref, v_ref, levels_ref, cq_ref, inner_ref, outer_ref, held_ref, sems, edge_sems
):
    me = lax.axis_index("seq")
    copies = {}
    for i, ref in ((1, k_ref), (2, v_ref), (0, q_ref)):
        for b in range(4):
            rows = pl.ds(BLOCK * b, BLOCK)
            copies[i, b] = pltpu.make_async_copy(ref.at[rows], held_ref.at[i, rows], sems.at[i, b])
            copies[i, b].start()
    inner = pl.multiple_of((1 - me % 2) * (TOKENS - BLOCK), BLOCK)
    outer = pl.multiple_of((me % 2) * (TOKENS - BLOCK), BLOCK)
    edges = []
    for i, ref in enumerate((k_ref, v_ref)):
        to = pl.ds(BLOCK * i, BLOCK)
        for j, (start, out) in enumerate(((inner, inner_ref), (outer, outer_ref))):
            edges.append(
                pltpu.make_async_copy(ref.at[pl.ds(start, BLOCK)], out.at[to], edge_sems.at[i, j])
            )
    for copy in edges:
        copy.start()

    def sums(i):
        parts = []
        for b in range(4):
            copies[i, b].wait()
            rows = held_ref[i, BLOCK * b : BLOCK * (b + 1), :].astype(F32)
            parts.append(jnp.sum(rows, axis=0, keepdims=True))
        return parts

    zero = jnp.zeros((1, HIDDEN), F32)
    k1, k2, k3 = pooled_levels(sums(1))
    v1, v2, v3 = pooled_levels(sums(2))
    slot1 = jnp.concatenate(k1 + v1, axis=0)
    slot2 = jnp.concatenate(k2 + [zero] * 2 + v2 + [zero] * 2, axis=0)
    slot3 = jnp.concatenate(k3 + [zero] * 3 + v3 + [zero] * 3, axis=0)
    levels_ref[...] = jnp.concatenate([slot1, slot2, slot3], axis=0).astype(BF16)
    q1, q2, q3 = pooled_levels(sums(0))
    cq_ref[...] = jnp.concatenate(q1 + q2 + q3 + [zero], axis=0).astype(BF16)
    for copy in edges:
        copy.wait()


def pool(q, k, v):
    slab = ((2 * BLOCK, HIDDEN), BF16)
    return local_call(
        pool_kernel,
        [((24, HIDDEN), BF16), ((LEVEL_ROWS, HIDDEN), BF16), slab, slab],
        (q, k, v),
        3 * 256 * 1024,
        scratch=[
            pltpu.VMEM((3, TOKENS, HIDDEN), BF16),
            pltpu.SemaphoreType.DMA((3, 4)),
            pltpu.SemaphoreType.DMA((2, 2)),
        ],
        far_in=(0, 1, 2),
    )


def slots_kernel(own_ref, peer_ref, send_out, send_ref, sem):
    column = lax.axis_index("seq") // 2
    own, peer = own_ref[...].astype(F32), peer_ref[...].astype(F32)
    one, two, three = [
        jnp.concatenate([own[8 * i : 8 * (i + 1)], peer[8 * i : 8 * (i + 1)]], axis=0).astype(BF16)
        for i in range(3)
    ]
    for j in range(16):
        slot = jnp.where(column // 2 == j // 2, one, jnp.where(column // 8 == j // 8, two, three))
        send_ref[16 * j : 16 * (j + 1), :] = slot
    copy = pltpu.make_async_copy(send_ref, send_out, sem)
    copy.start()
    copy.wait()


def slots(own, peer):
    return local_call(
        slots_kernel,
        [((256, HIDDEN), BF16)],
        (own, peer),
        256 * 1024,
        scratch=[pltpu.VMEM((256, HIDDEN), BF16), pltpu.SemaphoreType.DMA],
        far_out=(0,),
    )[0]


def window(own, left, right, half, row):
    if half == 0:
        return jnp.concatenate([left[row : row + BLOCK, :], own[: 3 * BLOCK, :]], axis=0)
    return jnp.concatenate([own[BLOCK:, :], right[row : row + BLOCK, :]], axis=0)


def band_bias(half, key_dim):
    me = lax.axis_index("seq")
    key_block = iota((256, 256), key_dim) // BLOCK
    query_block = iota((256, 256), 1 - key_dim) // BLOCK % 2
    gap = key_block - query_block
    keep = jnp.logical_and(gap >= 0, gap <= 2)
    if half == 0:
        keep = jnp.logical_and(keep, key_block >= jnp.where(me > 0, 0, 1))
    else:
        last = lax.axis_size("seq") - 1
        keep = jnp.logical_and(keep, key_block <= jnp.where(me < last, 3, 2))
    return jnp.where(keep, 0.0, MASKED).astype(F32)


def head_masks(scale):
    lane = iota((1, 128), 1)
    low = jnp.where(lane < HEAD_DIM, scale, 0.0).astype(BF16)
    high = jnp.where(lane < HEAD_DIM, 0.0, scale).astype(BF16)
    return low, high


def two_heads(rows, masks):
    return jnp.concatenate([rows * masks[0], rows * masks[1]], axis=0)


def pick(stacked, low_lane):
    return jnp.where(low_lane, stacked[:128, :], stacked[128:, :])


def over_groups(body, count):
    width = 128 * count

    def step(g, carry):
        start = g * width
        lanes = [pl.ds(pl.multiple_of(start + 128 * p, 128), 128) for p in range(count)]
        body(g, lanes, pl.ds(pl.multiple_of(start, 128), width))
        return carry

    if count == PAIRS:
        body(0, [slice(128 * p, 128 * (p + 1)) for p in range(PAIRS)], slice(0, HIDDEN))
    else:
        lax.fori_loop(0, PAIRS // count, step, 0)


def by_parity(inner, outer):
    odd = lax.axis_index("seq") % 2 == 1
    return jnp.where(odd, inner, outer), jnp.where(odd, outer, inner)


FORWARD_GROUP = 2
BACKWARD_GROUP = 2
RIM_GROUP = 4


def soft_rows(scores, vals, low_lane, rows):
    top = jnp.max(scores, axis=1, keepdims=True)
    weight = jnp.exp(scores - top).astype(BF16)
    ones = jnp.ones((vals.shape[0], 128), BF16)
    both = mm(weight, jnp.concatenate([vals, ones], axis=1), ((1,), (0,)))
    total = both[:, 128:]
    part = jnp.where(low_lane, both[:rows, :128], both[rows:, :128])
    share = jnp.where(low_lane, total[:rows], total[rows:])
    return (part / share).astype(BF16), top + jnp.log(total)


def place(ref, span, lse, lane, head, rows):
    ref[span, :] = jnp.where(
        lane == head, lse[:rows, :], jnp.where(lane == head + 1, lse[rows:, :], ref[span, :])
    )


def inside_kernel(
    q_ref,
    k_ref,
    v_ref,
    cot_ref,
    w_hbm,
    a_out,
    lse_out,
    da_out,
    a_ref,
    lse_ref,
    w_ref,
    da_ref,
    sems,
    lse_sem,
    w_sems,
    da_sems,
):
    steps = PAIRS // FORWARD_GROUP
    width = 128 * FORWARD_GROUP

    def w_copy(g):
        rows = pl.ds(pl.multiple_of(width * g, width), width)
        return pltpu.make_async_copy(w_hbm.at[rows], w_ref.at[rows], w_sems.at[g])

    def da_copy(g, span):
        return pltpu.make_async_copy(da_ref.at[:, span], da_out.at[:, span], da_sems.at[g])

    def a_copy(g, span):
        return pltpu.make_async_copy(a_ref.at[:, span], a_out.at[:, span], sems.at[g])

    for g in range(steps):
        w_copy(g).start()
    gap = iota((256, 256), 1) // BLOCK - iota((256, 256), 0) // BLOCK % 2
    bias = jnp.where(jnp.logical_and(gap >= 0, gap <= 2), 0.0, MASKED).astype(F32)
    masks = head_masks(SCALE)
    lane = iota((128, 128), 1)
    low_lane = lane < HEAD_DIM
    lse_ref[...] = jnp.zeros((128, 128), F32)

    def body(g, groups, span):
        scores = []
        for lanes in groups:
            query = two_heads(q_ref[BLOCK : 3 * BLOCK, lanes], masks)
            scores.append(mm(query, k_ref[:, lanes], ((1,), (1,))) + bias)
        for p, (lanes, score) in enumerate(zip(groups, scores)):
            a_ref[:, lanes], lse = soft_rows(score, v_ref[:, lanes], low_lane, 128)
            place(lse_ref, slice(0, 128), lse, lane, 2 * (g * len(groups) + p), 128)
        a_copy(g, span).start()
        w_copy(g).wait()
        rows = pl.ds(pl.multiple_of(width * g, width), width)
        da_ref[:, span] = mm(cot_ref[...], w_ref[rows, :], ((1,), (1,))).astype(BF16)
        da_copy(g, span).start()

    over_groups(body, FORWARD_GROUP)
    lse_copy = pltpu.make_async_copy(lse_ref, lse_out, lse_sem)
    lse_copy.start()
    for g in range(steps):
        a_copy(g, pl.ds(width * g, width)).wait()
        da_copy(g, pl.ds(width * g, width)).wait()
    lse_copy.wait()


def inside_forward(q, k, v, cot, w):
    steps = PAIRS // FORWARD_GROUP
    return local_call(
        inside_kernel,
        [((128, HIDDEN), BF16), ((128, 128), F32), ((TOKENS, HIDDEN), BF16)],
        (q, k, v, cot, w),
        3 * 16 * 2 * 128 * 256 * 128 + 2 * 256 * 1024 * 1024,
        scratch=[
            pltpu.VMEM((128, HIDDEN), BF16),
            pltpu.VMEM((128, 128), F32),
            pltpu.VMEM((HIDDEN, HIDDEN), BF16),
            pltpu.VMEM((TOKENS, HIDDEN), BF16),
            pltpu.SemaphoreType.DMA((steps,)),
            pltpu.SemaphoreType.DMA,
            pltpu.SemaphoreType.DMA((steps,)),
            pltpu.SemaphoreType.DMA((steps,)),
        ],
        exps=8 * 256 * 256,
        far_in=(4,),
        far_out=(0, 1, 2),
    )


def rim_kernel(
    q_ref, k_ref, v_ref, inner_ref, outer_ref, a_out, lse_out, left_ref, right_ref, a_ref, lse_ref, sems
):
    left_ref[...], right_ref[...] = by_parity(inner_ref[...], outer_ref[...])
    me = lax.axis_index("seq")
    last = lax.axis_size("seq") - 1
    key_lane = iota((128, 192), 1)
    starts = (
        jnp.where(jnp.logical_and(key_lane < BLOCK, me == 0), MASKED, 0.0).astype(F32),
        jnp.where(jnp.logical_and(key_lane >= 2 * BLOCK, me == last), MASKED, 0.0).astype(F32),
    )
    masks = head_masks(SCALE)
    lane = iota((BLOCK, 128), 1)
    low_lane = lane < HEAD_DIM
    lse_ref[...] = jnp.zeros((128, 128), F32)

    def body(g, groups, span):
        units = [(p, lanes, side) for p, lanes in enumerate(groups) for side in range(2)]
        scores = []
        for p, lanes, side in units:
            at = side * (TOKENS - BLOCK)
            query = two_heads(q_ref[at : at + BLOCK, lanes], masks)
            if side == 0:
                keys = jnp.concatenate([left_ref[:BLOCK, lanes], k_ref[: 2 * BLOCK, lanes]], axis=0)
            else:
                keys = jnp.concatenate([k_ref[2 * BLOCK :, lanes], right_ref[:BLOCK, lanes]], axis=0)
            scores.append(mm(query, keys, ((1,), (1,))) + starts[side])
        for (p, lanes, side), score in zip(units, scores):
            if side == 0:
                vals = jnp.concatenate([left_ref[BLOCK:, lanes], v_ref[: 2 * BLOCK, lanes]], axis=0)
            else:
                vals = jnp.concatenate([v_ref[2 * BLOCK :, lanes], right_ref[BLOCK:, lanes]], axis=0)
            rows = slice(BLOCK * side, BLOCK * (side + 1))
            a_ref[rows, lanes], lse = soft_rows(score, vals, low_lane, BLOCK)
            place(lse_ref, rows, lse, lane, 2 * (g * len(groups) + p), BLOCK)

    over_groups(body, RIM_GROUP)
    copies = [
        pltpu.make_async_copy(a_ref, a_out, sems.at[0]),
        pltpu.make_async_copy(lse_ref, lse_out, sems.at[1]),
    ]
    for copy in copies:
        copy.start()
    for copy in copies:
        copy.wait()


def rim_forward(q, k, v, inner, outer):
    return local_call(
        rim_kernel,
        [((128, HIDDEN), BF16), ((128, 128), F32)],
        (q, k, v, inner, outer),
        3 * 16 * 2 * 128 * 192 * 128,
        scratch=[
            pltpu.VMEM((2 * BLOCK, HIDDEN), BF16),
            pltpu.VMEM((2 * BLOCK, HIDDEN), BF16),
            pltpu.VMEM((128, HIDDEN), BF16),
            pltpu.VMEM((128, 128), F32),
            pltpu.SemaphoreType.DMA((2,)),
        ],
        exps=16 * 128 * 192,
        far_out=(0, 1),
    )


def coarse_keep():
    me = lax.axis_index("seq")
    row = iota((128, 256), 0) % LEVEL_ROWS
    col = iota((128, 256), 1)
    same = me % 2
    dev = 2 * (col // 16) + same + (1 - 2 * same) * (col % 16 // 8)
    term = col % 8
    near = dev // 4 == me // 4
    mid = jnp.logical_and(dev // 16 == me // 16, jnp.logical_not(near))
    far = dev // 16 != me // 16
    apart = jnp.abs(4 * me + row - (4 * dev + term)) > 1
    one = jnp.logical_and(jnp.logical_and(row < 4, term < 4), jnp.logical_and(near, apart))
    two = jnp.logical_and(jnp.logical_and(row // 2 == 2, term < 2), mid)
    three = jnp.logical_and(jnp.logical_and(row == 6, term == 0), far)
    return jnp.logical_or(one, jnp.logical_or(two, three))


def by_head(rows, own):
    return jnp.concatenate([rows] * HEADS, axis=0) * own


def over_heads(stacked, own):
    return jnp.sum((stacked * own).reshape(HEADS, LEVEL_ROWS, HIDDEN), axis=0)


def three_terms(x):
    first = x.astype(BF16)
    rest = x - first.astype(F32)
    second = rest.astype(BF16)
    third = (rest - second.astype(F32)).astype(BF16)
    return jnp.concatenate([first, second, third], axis=1)


def stat_row(ref, pair, start, count):
    half, at = start // 128, start % 128
    row = ref[pair, half : half + 1, :]
    if count == 128:
        return row
    return jnp.concatenate([row[:, at : at + count], row[:, 128 + at : 128 + at + count]], axis=1)


def edge_terms(q_ref, da_ref, lse_ref, delta_ref, left_ref, right_ref, to_left_ref, to_right_ref):
    me = lax.axis_index("seq")
    masks = head_masks(1.0)
    scaled = head_masks(SCALE)
    last = lax.axis_size("seq") - 1
    left_bias = jnp.where(me > 0, 0.0, MASKED).astype(F32)
    right_bias = jnp.where(me < last, 0.0, MASKED).astype(F32)
    units = []
    for pair in range(PAIRS):
        lanes = slice(128 * pair, 128 * (pair + 1))
        units.append((pair, lanes, 0, 0, left_ref, to_left_ref, left_bias))
        units.append((pair, lanes, TOKENS - BLOCK, BLOCK, right_ref, to_right_ref, right_bias))
    held = []
    for pair, lanes, start, at, near_ref, out_ref, bias in units:
        query = two_heads(q_ref[at : at + BLOCK, lanes], scaled)
        grad = two_heads(da_ref[start : start + BLOCK, lanes], masks)
        scores = mm(near_ref[:BLOCK, lanes], query, ((1,), (1,))) + bias
        prob_grad = mm(near_ref[BLOCK:, lanes], grad, ((1,), (1,)))
        held.append((query, grad, scores, prob_grad))
    probs = [jnp.exp(h[2] - stat_row(lse_ref, u[0], u[2], BLOCK)) for u, h in zip(units, held)]
    for (pair, lanes, start, at, near_ref, out_ref, bias), (query, grad, _, prob_grad), prob in zip(
        units, held, probs
    ):
        delta = stat_row(delta_ref, pair, start, BLOCK)
        score_grad = (prob * (prob_grad - delta)).astype(BF16)
        out_ref[:BLOCK, lanes] = mm(score_grad, query, ((1,), (0,))).astype(BF16)
        out_ref[BLOCK:, lanes] = mm(prob.astype(BF16), grad, ((1,), (0,))).astype(BF16)


def join_kernel(
    cq_ref,
    kv_ref,
    a_mid_hbm,
    lse_mid_hbm,
    a_rim_hbm,
    lse_rim_hbm,
    da_hbm,
    q_hbm,
    inner_hbm,
    outer_hbm,
    att_ref,
    lse_ref,
    delta_ref,
    dq_ref,
    packed_ref,
    own_ref,
    near_ref,
    give_ref,
    to_inner_ref,
    to_outer_ref,
    a_ref,
    da_ref,
    lse0_ref,
    m0_ref,
    mc_ref,
    nc_ref,
    g_ref,
    h_ref,
    dkv_ref,
    q_ref,
    inner_ref,
    outer_ref,
    left_ref,
    right_ref,
    to_left_ref,
    to_right_ref,
    sems,
    edge_sems,
):
    loads = [
        pltpu.make_async_copy(da_hbm, da_ref, sems.at[0]),
    ]
    mid = pl.ds(BLOCK, 2 * BLOCK)
    for i, (mid_hbm, rim_hbm, ref) in enumerate(
        ((lse_mid_hbm, lse_rim_hbm, lse0_ref), (a_mid_hbm, a_rim_hbm, a_ref))
    ):
        loads.append(pltpu.make_async_copy(mid_hbm, ref.at[mid], sems.at[2 + 3 * i]))
        for side in range(2):
            to = pl.ds(side * (TOKENS - BLOCK), BLOCK)
            rows = pl.ds(side * BLOCK, BLOCK)
            sem = sems.at[3 + 3 * i + side]
            loads.append(pltpu.make_async_copy(rim_hbm.at[rows], ref.at[to], sem))
    edge_loads = [
        pltpu.make_async_copy(inner_hbm, inner_ref, edge_sems.at[0]),
        pltpu.make_async_copy(outer_hbm, outer_ref, edge_sems.at[1]),
    ]
    for side in range(2):
        rows = pl.ds(side * (TOKENS - BLOCK), BLOCK)
        to = pl.ds(side * BLOCK, BLOCK)
        edge_loads.append(
            pltpu.make_async_copy(q_hbm.at[rows], q_ref.at[to], edge_sems.at[2 + side])
        )
    for load in loads + edge_loads:
        load.start()
    own = jnp.where(
        iota((128, HIDDEN), 0) // LEVEL_ROWS == iota((128, HIDDEN), 1) // HEAD_DIM, 1.0, 0.0
    ).astype(F32)
    keep = coarse_keep()
    kv = kv_ref[...]
    query = by_head(cq_ref[...].astype(F32), own * SCALE).astype(BF16)
    scores = jnp.where(keep, mm(query, kv, ((1,), (1,))), MASKED)
    top = jnp.max(scores, axis=1, keepdims=True)
    weights = jnp.where(keep, jnp.exp(scores - top), 0.0)
    total = jnp.maximum(jnp.sum(weights, axis=1, keepdims=True), 1.0)
    on_values = pltpu.roll(weights, 4, 1).astype(BF16)
    inverse = 1.0 / total
    nc_ref[...] = over_heads(mm(on_values, kv, ((1,), (0,))) * inverse, own)
    mc_ref[...] = over_heads(jnp.broadcast_to(top + jnp.log(total), (128, HIDDEN)), own)
    same_head = jnp.where(
        iota((128, 128), 0) // HEAD_DIM == iota((128, 128), 1) // HEAD_DIM, 1.0, 0.0
    ).astype(BF16)
    spread = jnp.where(
        iota((384, HIDDEN), 0) % 128 == iota((384, HIDDEN), 1) // HEAD_DIM, 1.0, 0.0
    ).astype(BF16)
    for load in loads:
        load.wait()
    m0_ref[...] = mm(three_terms(lse0_ref[...]), spread, ((1,), (0,)))
    zero = jnp.zeros((1, 128), F32)

    def rows_of(parts):
        one, two, three = zip(*parts)
        return jnp.concatenate(
            list(one)
            + [two[0] + two[1], two[2] + two[3]]
            + [(three[0] + three[1]) + (three[2] + three[3]), zero],
            axis=0,
        )

    for p in range(PAIRS):
        lanes = slice(128 * p, 128 * (p + 1))
        g_parts, h_parts, lses, deltas = [], [], [], []
        for b in range(4):
            rows = slice(BLOCK * b, BLOCK * (b + 1))
            level = (b, 4 + b // 2, 6)
            m0 = m0_ref[rows, lanes]
            mc = [mc_ref[c : c + 1, lanes] for c in level]
            top_all = jnp.maximum(m0, jnp.maximum(mc[0], jnp.maximum(mc[1], mc[2])))
            f0 = jnp.exp(m0 - top_all)
            fc = [jnp.exp(x - top_all) for x in mc]
            inv = 1.0 / (f0 + fc[0] + (fc[1] + fc[2]))
            num = a_ref[rows, lanes].astype(F32) * f0
            for c, f in zip(level, fc):
                num = num + nc_ref[c : c + 1, lanes] * f
            att = (num * inv).astype(BF16)
            att_ref[rows, lanes] = att
            lses.append(top_all - jnp.log(inv))
            da = da_ref[rows, lanes].astype(F32)
            product = da * att.astype(F32)
            part = product.astype(BF16)
            rest = (product - part.astype(F32)).astype(BF16)
            delta = mm(part, same_head, ((1,), (0,))) + mm(rest, same_head, ((1,), (0,)))
            deltas.append(delta)
            wc = [f * inv for f in fc]
            g_parts.append([jnp.sum(w * da, axis=0, keepdims=True) for w in wc])
            h_parts.append([jnp.sum(w * delta, axis=0, keepdims=True) for w in wc])
        for parts, ref in ((lses, lse_ref), (deltas, delta_ref)):
            turned = jnp.concatenate(parts, axis=0).T
            for half in range(2):
                span = slice(128 * half, 128 * (half + 1))
                ref[p, half : half + 1, :] = jnp.concatenate(
                    [turned[:1, span], turned[HEAD_DIM : HEAD_DIM + 1, span]], axis=1
                )
        g_ref[:, lanes] = rows_of(g_parts)
        h_ref[:, lanes] = rows_of(h_parts)
    for load in edge_loads:
        load.wait()
    left_ref[...], right_ref[...] = by_parity(inner_ref[...], outer_ref[...])
    edge_terms(q_ref, da_ref, lse_ref, delta_ref, left_ref, right_ref, to_left_ref, to_right_ref)
    to_inner_ref[...], to_outer_ref[...] = by_parity(to_left_ref[...], to_right_ref[...])
    core = lax.axis_index("dp") % 2
    for hi in range(2):
        start = pl.multiple_of((2 * hi + 1 - core) * 256, 256)
        give_ref[:, 256 * hi : 256 * (hi + 1)] = att_ref[:, pl.ds(start, 256)]
    grads = (by_head(g_ref[...], own) * inverse).astype(BF16)
    sums = jnp.sum(by_head(h_ref[...], own), axis=1, keepdims=True) * (inverse * (1.0 / HEAD_DIM))
    on_keys = pltpu.roll(mm(grads, kv, ((1,), (1,))), 252, 1)
    score_grad = (weights * (on_keys - sums)).astype(BF16)
    row = iota((LEVEL_ROWS, 1), 0)
    share = jnp.where(row < 4, 1.0 / ROOTS[0], jnp.where(row < 6, 1.0 / ROOTS[1], 1.0 / ROOTS[2]))
    dq_ref[...] = over_heads(mm(score_grad, kv, ((1,), (0,))), own) * (share.astype(F32) * SCALE)
    left = jnp.concatenate([score_grad, on_values], axis=0)
    right = jnp.concatenate([query, grads], axis=0)
    dkv = mm(left, right, ((0,), (0,))).astype(BF16)
    dkv_ref[...] = dkv
    row, col = iota((128, 256), 0), iota((128, 256), 1)
    taken = 16 * (row // 8) + 8 * (row % 8 // 4) + 4 * (row % 4 // 2) + row % 2
    pick_rows = jnp.where(col == taken, 1.0, 0.0).astype(BF16)
    packed_ref[...] = mm(pick_rows, dkv, ((1,), (0,))).astype(BF16)
    column = lax.axis_index("seq") // 2
    other = column + 1 - 2 * (column % 2)
    own_ref[...] = dkv_ref[pl.ds(pl.multiple_of(16 * column, 16), 16), :]
    near_ref[...] = dkv_ref[pl.ds(pl.multiple_of(16 * other, 16), 16), :]


def join(cq, kv, inside, rim, da, q, inner, outer):
    stat = ((PAIRS, 2, 256), F32)
    level = pltpu.VMEM((LEVEL_ROWS, HIDDEN), F32)
    slab = ((2 * BLOCK, HIDDEN), BF16)
    return local_call(
        join_kernel,
        [
            ((TOKENS, HIDDEN), BF16),
            stat,
            stat,
            ((LEVEL_ROWS, HIDDEN), F32),
            ((128, HIDDEN), BF16),
            ((16, HIDDEN), BF16),
            ((16, HIDDEN), BF16),
            ((TOKENS, 512), BF16),
            slab,
            slab,
        ],
        (cq, kv, *inside, *rim, da, q, inner, outer),
        5 * 2 * 128 * 256 * 1024,
        scratch=[
            pltpu.VMEM((TOKENS, HIDDEN), BF16),
            pltpu.VMEM((TOKENS, HIDDEN), BF16),
            pltpu.VMEM((TOKENS, 128), F32),
            pltpu.VMEM((TOKENS, HIDDEN), F32),
            level,
            level,
            level,
            level,
            pltpu.VMEM((256, HIDDEN), BF16),
            *[pltpu.VMEM(*slab)] * 7,
            pltpu.SemaphoreType.DMA((8,)),
            pltpu.SemaphoreType.DMA((4,)),
        ],
        exps=6 * 256 * 1024,
        far_in=(2, 3, 4, 5, 6, 7, 8, 9),
    )


SLOT = 40


def weight_kernel(
    att_ref, got_ref, cot_ref, peer_cot_ref, packed_ref, send_ref, att_out, lhs_ref, att_sem
):
    att_copy = pltpu.make_async_copy(att_ref, att_out, att_sem)
    att_copy.start()
    core = lax.axis_index("dp") % 2
    for hi in range(2):
        start = pl.multiple_of((2 * hi + core) * 256, 256)
        rows = slice(256 * hi, 256 * (hi + 1))
        lhs_ref[rows, :TOKENS] = att_ref[:, pl.ds(start, 256)].T
        lhs_ref[rows, TOKENS:] = got_ref[:, rows].T
    width = 256
    for j in range(HIDDEN // width):
        cols = slice(width * j, width * (j + 1))
        cot = jnp.concatenate([cot_ref[:, cols], peer_cot_ref[:, cols]], axis=0)
        terms = mm(lhs_ref[...], cot, ((1,), (0,))).reshape(2, 16, 16, width)
        coarse = packed_ref[:, cols].astype(F32).reshape(16, 8, width)
        slots = jnp.concatenate([coarse, terms[0], terms[1]], axis=1)
        send_ref[:, cols] = slots.reshape(16 * SLOT, width).astype(BF16)
    att_copy.wait()


def weight_terms(att, got, cot, peer_cot, packed):
    return local_call(
        weight_kernel,
        [((16 * SLOT, HIDDEN), BF16), ((TOKENS, HIDDEN), BF16)],
        (att, got, cot, peer_cot, packed),
        2 * 512 * 512 * 1024,
        scratch=[pltpu.VMEM((512, 512), BF16), pltpu.SemaphoreType.DMA],
        far_out=(1,),
    )


def fine_backward_kernel(
    q_hbm,
    k_hbm,
    v_hbm,
    inner_hbm,
    outer_hbm,
    da_hbm,
    att_hbm,
    w_hbm,
    lse_ref,
    delta_ref,
    cdq_ref,
    gq_out,
    dk_out,
    dv_out,
    mixed_out,
    bias_ref,
    gq_ref,
    dk_ref,
    dv_ref,
    mixed_ref,
    q_ref,
    k_ref,
    v_ref,
    da_ref,
    att_ref,
    w_ref,
    inner_ref,
    outer_ref,
    left_ref,
    right_ref,
    sems,
    load_sems,
    mixed_sem,
):
    pairs = (
        (inner_hbm, inner_ref),
        (outer_hbm, outer_ref),
        (k_hbm, k_ref),
        (q_hbm, q_ref),
        (v_hbm, v_ref),
        (da_hbm, da_ref),
        (att_hbm, att_ref),
        (w_hbm, w_ref),
    )
    loads = [
        pltpu.make_async_copy(far, near, load_sems.at[i]) for i, (far, near) in enumerate(pairs)
    ]
    for load in loads:
        load.start()
    bias_ref[0] = band_bias(0, 0)
    bias_ref[1] = band_bias(1, 0)
    for load in loads[:6]:
        load.wait()
    left_ref[...], right_ref[...] = by_parity(inner_ref[...], outer_ref[...])
    masks = head_masks(1.0)
    scaled = head_masks(SCALE)
    low_lane = iota((128, 128), 1) < HEAD_DIM

    def copies(g, span):
        held_refs = (gq_ref, dk_ref, dv_ref)
        return [
            pltpu.make_async_copy(ref.at[:, span], out.at[:, span], sems.at[i, g])
            for i, (ref, out) in enumerate(zip(held_refs, (gq_out, dk_out, dv_out)))
        ]

    def body(g, groups, span):
        units = [
            (g * len(groups) + p, lanes, half) for p, lanes in enumerate(groups) for half in range(2)
        ]
        held = []
        for pair, lanes, half in units:
            rows = slice(128 * half, 128 * (half + 1))
            near = (left_ref.at[:, lanes], right_ref.at[:, lanes], half)
            keys = window(k_ref.at[:, lanes], *near, 0)
            vals = window(v_ref.at[:, lanes], *near, BLOCK)
            query = two_heads(q_ref[rows, lanes], scaled)
            grad = two_heads(da_ref[rows, lanes], masks)
            scores = mm(keys, query, ((1,), (1,))) + bias_ref[half]
            prob_grad = mm(vals, grad, ((1,), (1,)))
            held.append((keys, query, grad, scores, prob_grad))
        probs = [
            jnp.exp(h[3] - stat_row(lse_ref, u[0], 128 * u[2], 128)) for u, h in zip(units, held)
        ]
        parts = []
        for (pair, lanes, half), (keys, query, grad, _, prob_grad), prob in zip(
            units, held, probs
        ):
            rows = slice(128 * half, 128 * (half + 1))
            delta = stat_row(delta_ref, pair, 128 * half, 128)
            score_grad = (prob * (prob_grad - delta)).astype(BF16)
            dk = mm(score_grad, query, ((1,), (0,)))
            dv = mm(prob.astype(BF16), grad, ((1,), (0,)))
            parts.append((dk, dv))
            dq = pick(mm(score_grad, keys, ((0,), (0,))), low_lane) * SCALE
            for b in range(2):
                block = 2 * half + b
                coarse = (
                    cdq_ref[block : block + 1, lanes]
                    + cdq_ref[4 + half : 5 + half, lanes]
                    + cdq_ref[6:7, lanes]
                )
                gq_ref[BLOCK * block : BLOCK * (block + 1), lanes] = (
                    dq[BLOCK * b : BLOCK * (b + 1), :] + coarse
                ).astype(BF16)
        for p, lanes in enumerate(groups):
            for ref, low, high in zip((dk_ref, dv_ref), parts[2 * p], parts[2 * p + 1]):
                ref[:BLOCK, lanes] = low[BLOCK : 2 * BLOCK, :].astype(BF16)
                middle = low[2 * BLOCK :, :] + high[: 2 * BLOCK, :]
                ref[BLOCK : 3 * BLOCK, lanes] = middle.astype(BF16)
                ref[3 * BLOCK :, lanes] = high[2 * BLOCK : 3 * BLOCK, :].astype(BF16)
        for copy in copies(g, span):
            copy.start()

    over_groups(body, BACKWARD_GROUP)
    for load in loads[6:]:
        load.wait()
    mixed_ref[...] = mm(att_ref[...], w_ref[...], ((1,), (0,))).astype(BF16)
    mixed_copy = pltpu.make_async_copy(mixed_ref, mixed_out, mixed_sem)
    mixed_copy.start()
    width = 128 * BACKWARD_GROUP
    for g in range(PAIRS // BACKWARD_GROUP):
        for copy in copies(g, pl.ds(width * g, width)):
            copy.wait()
    mixed_copy.wait()


def fine_backward(q, k, v, inner, outer, da, att, w, lse, delta, cdq):
    out = ((TOKENS, HIDDEN), BF16)
    return local_call(
        fine_backward_kernel,
        [out, out, out, out],
        (q, k, v, inner, outer, da, att, w, lse, delta, cdq),
        5 * 16 * 2 * 256 * 256 * 128 + 2 * 256 * 1024 * 1024,
        scratch=[pltpu.VMEM((2, 256, 256), F32)]
        + [pltpu.VMEM((TOKENS, HIDDEN), BF16)] * 9
        + [pltpu.VMEM((HIDDEN, HIDDEN), BF16)]
        + [pltpu.VMEM((2 * BLOCK, HIDDEN), BF16)] * 4
        + [
            pltpu.SemaphoreType.DMA((3, PAIRS // BACKWARD_GROUP)),
            pltpu.SemaphoreType.DMA((8,)),
            pltpu.SemaphoreType.DMA,
        ],
        exps=16 * 256 * 256,
        far_in=tuple(range(8)),
        far_out=(0, 1, 2, 3),
    )


def sums_kernel(
    got_ref,
    near_ref,
    own_ref,
    dk_hbm,
    dv_hbm,
    coarse_ref,
    mine_ref,
    to_low_ref,
    to_high_ref,
    to_both_ref,
    dk_ref,
    dv_ref,
    sems,
):
    copies = [
        pltpu.make_async_copy(dk_hbm, dk_ref, sems.at[0]),
        pltpu.make_async_copy(dv_hbm, dv_ref, sems.at[1]),
    ]
    for copy in copies:
        copy.start()
    me = lax.axis_index("seq")
    low, column = me % 2, me // 2
    high = lax.axis_index("dp") // 2
    row = iota((64, 16 * SLOT), 0)
    col = iota((64, 16 * SLOT), 1)
    source = col // SLOT
    at = col % SLOT
    near = source // 2 == column // 2
    mid = jnp.logical_and(source // 8 == column // 8, jnp.logical_not(near))
    far = source // 8 != column // 8
    level_row = row % 8
    side = jnp.where(row < 16, 0, 1)
    term = at - 4 * side - 2 * (row // 8 % 2)
    two = jnp.logical_and(jnp.logical_and(level_row // 2 == 2, term == level_row - 4), mid)
    three = jnp.logical_and(jnp.logical_and(level_row == 6, term == 0), far)
    coarse = jnp.logical_and(jnp.logical_or(two, three), row < 32)
    block = row // 8 - 4
    block_high = jnp.where(block < 2, high, 1 - high)
    block_low = jnp.where(block % 2 == 0, low, 1 - low)
    weight = jnp.logical_and(row >= 32, at == 8 + 16 * block_high + 8 * block_low + level_row)
    chosen = jnp.where(jnp.logical_or(coarse, weight), 1.0, 0.0).astype(BF16)
    sums = mm(chosen, got_ref[...], ((1,), (0,)))
    row = iota((32, 32), 0)
    col = iota((32, 32), 1) % 16
    side = jnp.where(row < 16, 0, 1)
    first = jnp.logical_and(row % 8 < 4, col == 8 * side + 4 * (row // 8 % 2) + row % 8)
    close = jnp.concatenate([near_ref[...], own_ref[...]], axis=0)
    coarse_sums = sums[:32, :] + mm(jnp.where(first, 1.0, 0.0).astype(BF16), close, ((1,), (0,)))
    coarse_ref[...] = coarse_sums[:16, :]
    mine_ref[...] = sums[32:40, :]
    to_low_ref[:16, :] = coarse_sums[16:, :].astype(BF16)
    to_low_ref[16:, :] = sums[40:48, :].astype(BF16)
    to_high_ref[...] = sums[48:56, :].astype(BF16)
    to_both_ref[...] = sums[56:, :].astype(BF16)
    for copy in copies:
        copy.wait()


def all_sums(got, near, own, dk, dv):
    return local_call(
        sums_kernel,
        [
            ((16, HIDDEN), F32),
            ((8, HIDDEN), F32),
            ((24, HIDDEN), BF16),
            ((8, HIDDEN), BF16),
            ((8, HIDDEN), BF16),
            ((TOKENS, HIDDEN), BF16),
            ((TOKENS, HIDDEN), BF16),
        ],
        (got, near, own, dk, dv),
        2 * 64 * 640 * 1024,
        scratch=[pltpu.SemaphoreType.DMA((2,))],
        far_in=(3, 4),
    )


def finish_kernel(
    dk_ref,
    dv_ref,
    inner_ref,
    outer_ref,
    sums_ref,
    low_ref,
    gk_out,
    gv_out,
    gk_ref,
    gv_ref,
    sems,
):
    copies = []
    sums = sums_ref[...] + low_ref[:16, :].astype(F32)
    from_left, from_right = by_parity(inner_ref[...], outer_ref[...])
    for at, own_ref, out_ref, out in ((0, dk_ref, gk_ref, gk_out), (8, dv_ref, gv_ref, gv_out)):
        side = BLOCK * (at // 8)
        for b in range(4):
            rows = slice(BLOCK * b, BLOCK * (b + 1))
            c1, c2, c3 = at + b, at + 4 + b // 2, at + 6
            coarse = (
                sums[c1 : c1 + 1, :] * (1.0 / ROOTS[0])
                + sums[c2 : c2 + 1, :] * (1.0 / ROOTS[1])
                + sums[c3 : c3 + 1, :] * (1.0 / ROOTS[2])
            )
            value = own_ref[rows, :].astype(F32) + coarse
            if b == 0:
                value = value + from_left[side : side + BLOCK, :].astype(F32)
            if b == 3:
                value = value + from_right[side : side + BLOCK, :].astype(F32)
            out_ref[rows, :] = value.astype(BF16)
            span = pl.ds(BLOCK * b, BLOCK)
            copies.append(
                pltpu.make_async_copy(out_ref.at[span], out.at[span], sems.at[at // 8, b])
            )
            copies[-1].start()
    for copy in copies:
        copy.wait()


def finish(dk, dv, inner, outer, sums, low):
    out = ((TOKENS, HIDDEN), BF16)
    return local_call(
        finish_kernel,
        [out, out],
        (dk, dv, inner, outer, sums, low),
        16 * 256 * 1024,
        scratch=[pltpu.VMEM((TOKENS, HIDDEN), BF16)] * 2 + [pltpu.SemaphoreType.DMA((2, 4))],
        far_out=(0, 1),
    )


def swap(x, axis, bit):
    return lax.ppermute(x, axis, [(i, i ^ bit) for i in range(lax.axis_size(axis))])


def swap_inner(x):
    return swap(x, "seq", 1)


def swap_outer(x):
    n = lax.axis_size("seq")
    return lax.ppermute(x, "seq", [(i, i + 1 if i % 2 else i - 1) for i in range(1, n - 1)])


def swap_both(x):
    n = lax.axis_size("seq")
    total = n * lax.axis_size("dp")
    return lax.ppermute(x, ("dp", "seq"), [(i, i ^ (2 * n + 1)) for i in range(total)])


def exchanged(x, rows):
    groups = [[2 * j + low for j in range(16)] for low in range(2)]
    got = lax.all_to_all(
        x.reshape(16, rows, HIDDEN),
        "seq",
        split_axis=0,
        concat_axis=0,
        tiled=True,
        axis_index_groups=groups,
    )
    return got.reshape(16 * rows, HIDDEN)


def body(q, k, v, out_weight, cot):
    levels, cq, inner, outer = pool(q, k, v)
    peer_levels = swap(levels, "seq", 1)
    outer = swap_outer(outer)
    inner = swap_inner(inner)
    send = slots(levels, peer_levels)
    coarse_kv = exchanged(send, 16)
    peer_cot = swap(cot, "dp", 1)
    *inside, d_att = inside_forward(q, k, v, cot, out_weight)
    rim = rim_forward(q, k, v, inner, outer)
    att, lse, delta, cdq, packed, own_rows, near_rows, give, to_inner, to_outer = join(
        cq, coarse_kv, inside, rim, d_att, q, inner, outer
    )
    got = swap(give, "dp", 1)
    from_outer = swap_outer(to_outer)
    from_inner = swap_inner(to_inner)
    send_back, far_att = weight_terms(att, got, cot, peer_cot, packed)
    back = exchanged(send_back, SLOT)
    near_rows = swap(near_rows, "seq", 2)
    gq, dk, dv, mixed = fine_backward(
        q, k, v, inner, outer, d_att, far_att, out_weight, lse, delta, cdq
    )
    sums, mine, to_low, to_high, to_both, dk, dv = all_sums(
        back, near_rows, own_rows, dk, dv
    )
    low = swap(to_low, "seq", 1)
    high = swap(to_high, "dp", 2)
    both = swap_both(to_both)
    gk, gv = finish(dk, dv, from_inner, from_outer, sums, low)
    grad_weight = (mine + low[16:].astype(F32)) + (high.astype(F32) + both.astype(F32))
    return (mixed[None], grad_weight, gq[None], gk[None], gv[None])


def on_device(queries, keys, values, out_weight, cotangent):
    return body(queries[0], keys[0], values[0], out_weight, cotangent[0])


def solution(mesh):
    tokens = P("dp", "seq", None)
    return jax.shard_map(
        on_device,
        mesh=mesh,
        in_specs=(tokens, tokens, tokens, P(), tokens),
        out_specs=(tokens, P(("dp", "seq"), None), tokens, tokens, tokens),
        check_vma=False,
    )
```

```python
import math

import jax
import jax.numpy as jnp
from jax import lax
from jax.experimental import pallas as pl
from jax.experimental.pallas import tpu as pltpu
from jax.sharding import PartitionSpec as P


HEADS = 16
HEAD_DIM = 64
BLOCK = 64
TOKENS = 256
HIDDEN = 1024
PAIRS = HIDDEN // 128
LEVEL_ROWS = 8
MASKED = -1e30
F32 = jnp.float32
BF16 = jnp.bfloat16
SCALE = 1.0 / math.sqrt(HEAD_DIM)
ROOTS = (math.sqrt(64.0), math.sqrt(128.0), math.sqrt(256.0))


def mm(a, b, dims):
    return lax.dot_general(a, b, (dims, ((), ())), preferred_element_type=F32)


def iota(shape, dim):
    return lax.broadcasted_iota(jnp.int32, shape, dim)


def local_call(kernel, outs, args, flops, scratch=(), exps=0, far_in=(), far_out=()):
    near = pl.BlockSpec(memory_space=pltpu.VMEM)
    far = pl.BlockSpec(memory_space=pltpu.HBM)
    held = [
        pltpu.with_memory_space_constraint(x, pltpu.HBM if i in far_in else pltpu.VMEM)
        for i, x in enumerate(args)
    ]
    return pl.pallas_call(
        kernel,
        in_specs=[far if i in far_in else near for i in range(len(args))],
        out_specs=tuple(far if i in far_out else near for i in range(len(outs))),
        out_shape=tuple(
            (pltpu.HBM if i in far_out else pltpu.VMEM)(*out) for i, out in enumerate(outs)
        ),
        scratch_shapes=list(scratch),
        compiler_params=pltpu.CompilerParams(vmem_limit_bytes=24 << 20),
        cost_estimate=pl.CostEstimate(flops=flops, transcendentals=exps, bytes_accessed=1 << 20),
    )(*held)


def pooled_levels(one):
    two = [one[0] + one[1], one[2] + one[3]]
    three = [two[0] + two[1]]
    return [[x / root for x in rows] for rows, root in zip((one, two, three), ROOTS)]


def pool_kernel(k_hbm, v_hbm, levels_ref, inner_ref, outer_ref, k_ref, v_ref, sems):
    me = lax.axis_index("seq")
    copies = [
        pltpu.make_async_copy(k_hbm, k_ref, sems.at[0]),
        pltpu.make_async_copy(v_hbm, v_ref, sems.at[1]),
    ]
    for copy in copies:
        copy.start()
    inner = pl.multiple_of((1 - me % 2) * (TOKENS - BLOCK), BLOCK)
    outer = pl.multiple_of((me % 2) * (TOKENS - BLOCK), BLOCK)

    def sums(i, ref):
        copies[i].wait()
        to = slice(BLOCK * i, BLOCK * (i + 1))
        inner_ref[to, :] = ref[pl.ds(inner, BLOCK), :]
        outer_ref[to, :] = ref[pl.ds(outer, BLOCK), :]
        return [
            jnp.sum(ref[BLOCK * b : BLOCK * (b + 1), :].astype(F32), axis=0, keepdims=True)
            for b in range(4)
        ]

    zero = jnp.zeros((1, HIDDEN), F32)
    k1, k2, k3 = pooled_levels(sums(0, k_ref))
    v1, v2, v3 = pooled_levels(sums(1, v_ref))
    slot1 = jnp.concatenate(k1 + v1, axis=0)
    slot2 = jnp.concatenate(k2 + [zero] * 2 + v2 + [zero] * 2, axis=0)
    slot3 = jnp.concatenate(k3 + [zero] * 3 + v3 + [zero] * 3, axis=0)
    levels_ref[...] = jnp.concatenate([slot1, slot2, slot3], axis=0).astype(BF16)


def pool(k, v):
    slab = ((2 * BLOCK, HIDDEN), BF16)
    return local_call(
        pool_kernel,
        [((24, HIDDEN), BF16), slab, slab],
        (k, v),
        2 * 256 * 1024,
        scratch=[
            pltpu.VMEM((TOKENS, HIDDEN), BF16),
            pltpu.VMEM((TOKENS, HIDDEN), BF16),
            pltpu.SemaphoreType.DMA((2,)),
        ],
        far_in=(0, 1),
    )


def slots_kernel(own_ref, peer_ref, send_out, send_ref, sem):
    column = lax.axis_index("seq") // 2
    own, peer = own_ref[...].astype(F32), peer_ref[...].astype(F32)
    one, two, three = [
        jnp.concatenate([own[8 * i : 8 * (i + 1)], peer[8 * i : 8 * (i + 1)]], axis=0).astype(BF16)
        for i in range(3)
    ]
    for j in range(16):
        slot = jnp.where(column // 2 == j // 2, one, jnp.where(column // 8 == j // 8, two, three))
        send_ref[16 * j : 16 * (j + 1), :] = slot
    copy = pltpu.make_async_copy(send_ref, send_out, sem)
    copy.start()
    copy.wait()


def slots(own, peer):
    return local_call(
        slots_kernel,
        [((256, HIDDEN), BF16)],
        (own, peer),
        256 * 1024,
        scratch=[pltpu.VMEM((256, HIDDEN), BF16), pltpu.SemaphoreType.DMA],
        far_out=(0,),
    )[0]


def window(own, left, right, half, row):
    if half == 0:
        return jnp.concatenate([left[row : row + BLOCK, :], own[: 3 * BLOCK, :]], axis=0)
    return jnp.concatenate([own[BLOCK:, :], right[row : row + BLOCK, :]], axis=0)


def band_bias(half, key_dim):
    me = lax.axis_index("seq")
    key_block = iota((256, 256), key_dim) // BLOCK
    query_block = iota((256, 256), 1 - key_dim) // BLOCK % 2
    gap = key_block - query_block
    keep = jnp.logical_and(gap >= 0, gap <= 2)
    if half == 0:
        keep = jnp.logical_and(keep, key_block >= jnp.where(me > 0, 0, 1))
    else:
        last = lax.axis_size("seq") - 1
        keep = jnp.logical_and(keep, key_block <= jnp.where(me < last, 3, 2))
    return jnp.where(keep, 0.0, MASKED).astype(F32)


def head_masks(scale):
    lane = iota((1, 128), 1)
    low = jnp.where(lane < HEAD_DIM, scale, 0.0).astype(BF16)
    high = jnp.where(lane < HEAD_DIM, 0.0, scale).astype(BF16)
    return low, high


def two_heads(rows, masks):
    return jnp.concatenate([rows * masks[0], rows * masks[1]], axis=0)


def pick(stacked, low_lane):
    return jnp.where(low_lane, stacked[:128, :], stacked[128:, :])


def over_groups(body, count):
    width = 128 * count

    def step(g, carry):
        start = g * width
        lanes = [pl.ds(pl.multiple_of(start + 128 * p, 128), 128) for p in range(count)]
        body(g, lanes, pl.ds(pl.multiple_of(start, 128), width))
        return carry

    if count == PAIRS:
        body(0, [slice(128 * p, 128 * (p + 1)) for p in range(PAIRS)], slice(0, HIDDEN))
    else:
        lax.fori_loop(0, PAIRS // count, step, 0)


def by_parity(inner, outer):
    odd = lax.axis_index("seq") % 2 == 1
    return jnp.where(odd, inner, outer), jnp.where(odd, outer, inner)


FORWARD_GROUP = 2
BACKWARD_GROUP = 2
RIM_GROUP = 4


def soft_rows(scores, vals, low_lane, rows):
    top = jnp.max(scores, axis=1, keepdims=True)
    weight = jnp.exp(scores - top).astype(BF16)
    ones = jnp.ones((vals.shape[0], 128), BF16)
    both = mm(weight, jnp.concatenate([vals, ones], axis=1), ((1,), (0,)))
    total = both[:, 128:]
    part = jnp.where(low_lane, both[:rows, :128], both[rows:, :128])
    share = jnp.where(low_lane, total[:rows], total[rows:])
    return (part / share).astype(BF16), top + jnp.log(total)


def place(ref, span, lse, lane, head, rows):
    ref[span, :] = jnp.where(
        lane == head, lse[:rows, :], jnp.where(lane == head + 1, lse[rows:, :], ref[span, :])
    )


def inside_kernel(
    q_ref,
    k_ref,
    v_ref,
    cot_ref,
    w_hbm,
    a_out,
    lse_out,
    da_out,
    cq_ref,
    a_ref,
    lse_ref,
    w_ref,
    da_ref,
    sems,
    lse_sem,
    w_sems,
    da_sems,
):
    steps = PAIRS // FORWARD_GROUP
    width = 128 * FORWARD_GROUP

    def w_copy(g):
        rows = pl.ds(pl.multiple_of(width * g, width), width)
        return pltpu.make_async_copy(w_hbm.at[rows], w_ref.at[rows], w_sems.at[g])

    def da_copy(g, span):
        return pltpu.make_async_copy(da_ref.at[:, span], da_out.at[:, span], da_sems.at[g])

    def a_copy(g, span):
        return pltpu.make_async_copy(a_ref.at[:, span], a_out.at[:, span], sems.at[g])

    for g in range(steps):
        w_copy(g).start()
    gap = iota((256, 256), 1) // BLOCK - iota((256, 256), 0) // BLOCK % 2
    bias = jnp.where(jnp.logical_and(gap >= 0, gap <= 2), 0.0, MASKED).astype(F32)
    masks = head_masks(SCALE)
    lane = iota((128, 128), 1)
    low_lane = lane < HEAD_DIM
    lse_ref[...] = jnp.zeros((128, 128), F32)

    def body(g, groups, span):
        scores = []
        for lanes in groups:
            query = two_heads(q_ref[BLOCK : 3 * BLOCK, lanes], masks)
            scores.append(mm(query, k_ref[:, lanes], ((1,), (1,))) + bias)
        for p, (lanes, score) in enumerate(zip(groups, scores)):
            a_ref[:, lanes], lse = soft_rows(score, v_ref[:, lanes], low_lane, 128)
            place(lse_ref, slice(0, 128), lse, lane, 2 * (g * len(groups) + p), 128)
        a_copy(g, span).start()
        w_copy(g).wait()
        rows = pl.ds(pl.multiple_of(width * g, width), width)
        da_ref[:, span] = mm(cot_ref[...], w_ref[rows, :], ((1,), (1,))).astype(BF16)
        da_copy(g, span).start()

    over_groups(body, FORWARD_GROUP)
    q1, q2, q3 = pooled_levels(
        [
            jnp.sum(q_ref[BLOCK * b : BLOCK * (b + 1), :].astype(F32), axis=0, keepdims=True)
            for b in range(4)
        ]
    )
    zero = jnp.zeros((1, HIDDEN), F32)
    cq_ref[...] = jnp.concatenate(q1 + q2 + q3 + [zero], axis=0).astype(BF16)
    lse_copy = pltpu.make_async_copy(lse_ref, lse_out, lse_sem)
    lse_copy.start()
    for g in range(steps):
        a_copy(g, pl.ds(width * g, width)).wait()
        da_copy(g, pl.ds(width * g, width)).wait()
    lse_copy.wait()


def inside_forward(q, k, v, cot, w):
    steps = PAIRS // FORWARD_GROUP
    return local_call(
        inside_kernel,
        [
            ((128, HIDDEN), BF16),
            ((128, 128), F32),
            ((TOKENS, HIDDEN), BF16),
            ((LEVEL_ROWS, HIDDEN), BF16),
        ],
        (q, k, v, cot, w),
        3 * 16 * 2 * 128 * 256 * 128 + 2 * 256 * 1024 * 1024,
        scratch=[
            pltpu.VMEM((128, HIDDEN), BF16),
            pltpu.VMEM((128, 128), F32),
            pltpu.VMEM((HIDDEN, HIDDEN), BF16),
            pltpu.VMEM((TOKENS, HIDDEN), BF16),
            pltpu.SemaphoreType.DMA((steps,)),
            pltpu.SemaphoreType.DMA,
            pltpu.SemaphoreType.DMA((steps,)),
            pltpu.SemaphoreType.DMA((steps,)),
        ],
        exps=8 * 256 * 256,
        far_in=(4,),
        far_out=(0, 1, 2),
    )


def rim_kernel(
    q_ref, k_ref, v_ref, inner_ref, outer_ref, a_out, lse_out, left_ref, right_ref, a_ref, lse_ref, sems
):
    left_ref[...], right_ref[...] = by_parity(inner_ref[...], outer_ref[...])
    me = lax.axis_index("seq")
    last = lax.axis_size("seq") - 1
    key_lane = iota((128, 192), 1)
    starts = (
        jnp.where(jnp.logical_and(key_lane < BLOCK, me == 0), MASKED, 0.0).astype(F32),
        jnp.where(jnp.logical_and(key_lane >= 2 * BLOCK, me == last), MASKED, 0.0).astype(F32),
    )
    masks = head_masks(SCALE)
    lane = iota((BLOCK, 128), 1)
    low_lane = lane < HEAD_DIM
    lse_ref[...] = jnp.zeros((128, 128), F32)

    def body(g, groups, span):
        units = [(p, lanes, side) for p, lanes in enumerate(groups) for side in range(2)]
        scores = []
        for p, lanes, side in units:
            at = side * (TOKENS - BLOCK)
            query = two_heads(q_ref[at : at + BLOCK, lanes], masks)
            if side == 0:
                keys = jnp.concatenate([left_ref[:BLOCK, lanes], k_ref[: 2 * BLOCK, lanes]], axis=0)
            else:
                keys = jnp.concatenate([k_ref[2 * BLOCK :, lanes], right_ref[:BLOCK, lanes]], axis=0)
            scores.append(mm(query, keys, ((1,), (1,))) + starts[side])
        for (p, lanes, side), score in zip(units, scores):
            if side == 0:
                vals = jnp.concatenate([left_ref[BLOCK:, lanes], v_ref[: 2 * BLOCK, lanes]], axis=0)
            else:
                vals = jnp.concatenate([v_ref[2 * BLOCK :, lanes], right_ref[BLOCK:, lanes]], axis=0)
            rows = slice(BLOCK * side, BLOCK * (side + 1))
            a_ref[rows, lanes], lse = soft_rows(score, vals, low_lane, BLOCK)
            place(lse_ref, rows, lse, lane, 2 * (g * len(groups) + p), BLOCK)

    over_groups(body, RIM_GROUP)
    copies = [
        pltpu.make_async_copy(a_ref, a_out, sems.at[0]),
        pltpu.make_async_copy(lse_ref, lse_out, sems.at[1]),
    ]
    for copy in copies:
        copy.start()
    for copy in copies:
        copy.wait()


def rim_forward(q, k, v, inner, outer):
    return local_call(
        rim_kernel,
        [((128, HIDDEN), BF16), ((128, 128), F32)],
        (q, k, v, inner, outer),
        3 * 16 * 2 * 128 * 192 * 128,
        scratch=[
            pltpu.VMEM((2 * BLOCK, HIDDEN), BF16),
            pltpu.VMEM((2 * BLOCK, HIDDEN), BF16),
            pltpu.VMEM((128, HIDDEN), BF16),
            pltpu.VMEM((128, 128), F32),
            pltpu.SemaphoreType.DMA((2,)),
        ],
        exps=16 * 128 * 192,
        far_out=(0, 1),
    )


def coarse_keep():
    me = lax.axis_index("seq")
    row = iota((128, 256), 0) % LEVEL_ROWS
    col = iota((128, 256), 1)
    same = me % 2
    dev = 2 * (col // 16) + same + (1 - 2 * same) * (col % 16 // 8)
    term = col % 8
    near = dev // 4 == me // 4
    mid = jnp.logical_and(dev // 16 == me // 16, jnp.logical_not(near))
    far = dev // 16 != me // 16
    apart = jnp.abs(4 * me + row - (4 * dev + term)) > 1
    one = jnp.logical_and(jnp.logical_and(row < 4, term < 4), jnp.logical_and(near, apart))
    two = jnp.logical_and(jnp.logical_and(row // 2 == 2, term < 2), mid)
    three = jnp.logical_and(jnp.logical_and(row == 6, term == 0), far)
    return jnp.logical_or(one, jnp.logical_or(two, three))


def by_head(rows, own):
    return jnp.concatenate([rows] * HEADS, axis=0) * own


def over_heads(stacked, own):
    return jnp.sum((stacked * own).reshape(HEADS, LEVEL_ROWS, HIDDEN), axis=0)


def three_terms(x):
    first = x.astype(BF16)
    rest = x - first.astype(F32)
    second = rest.astype(BF16)
    third = (rest - second.astype(F32)).astype(BF16)
    return jnp.concatenate([first, second, third], axis=1)


def stat_row(ref, pair, start, count):
    half, at = start // 128, start % 128
    row = ref[pair, half : half + 1, :]
    if count == 128:
        return row
    return jnp.concatenate([row[:, at : at + count], row[:, 128 + at : 128 + at + count]], axis=1)


def edge_terms(q_ref, da_ref, lse_ref, delta_ref, left_ref, right_ref, to_left_ref, to_right_ref):
    me = lax.axis_index("seq")
    masks = head_masks(1.0)
    scaled = head_masks(SCALE)
    last = lax.axis_size("seq") - 1
    left_bias = jnp.where(me > 0, 0.0, MASKED).astype(F32)
    right_bias = jnp.where(me < last, 0.0, MASKED).astype(F32)
    units = []
    for pair in range(PAIRS):
        lanes = slice(128 * pair, 128 * (pair + 1))
        units.append((pair, lanes, 0, 0, left_ref, to_left_ref, left_bias))
        units.append((pair, lanes, TOKENS - BLOCK, BLOCK, right_ref, to_right_ref, right_bias))
    held = []
    for pair, lanes, start, at, near_ref, out_ref, bias in units:
        query = two_heads(q_ref[at : at + BLOCK, lanes], scaled)
        grad = two_heads(da_ref[start : start + BLOCK, lanes], masks)
        scores = mm(near_ref[:BLOCK, lanes], query, ((1,), (1,))) + bias
        prob_grad = mm(near_ref[BLOCK:, lanes], grad, ((1,), (1,)))
        held.append((query, grad, scores, prob_grad))
    probs = [jnp.exp(h[2] - stat_row(lse_ref, u[0], u[2], BLOCK)) for u, h in zip(units, held)]
    for (pair, lanes, start, at, near_ref, out_ref, bias), (query, grad, _, prob_grad), prob in zip(
        units, held, probs
    ):
        delta = stat_row(delta_ref, pair, start, BLOCK)
        score_grad = (prob * (prob_grad - delta)).astype(BF16)
        out_ref[:BLOCK, lanes] = mm(score_grad, query, ((1,), (0,))).astype(BF16)
        out_ref[BLOCK:, lanes] = mm(prob.astype(BF16), grad, ((1,), (0,))).astype(BF16)


def join_kernel(
    cq_ref,
    kv_ref,
    a_mid_hbm,
    lse_mid_hbm,
    a_rim_hbm,
    lse_rim_hbm,
    da_hbm,
    q_hbm,
    inner_hbm,
    outer_hbm,
    att_ref,
    lse_ref,
    delta_ref,
    dq_ref,
    packed_ref,
    own_ref,
    near_ref,
    give_ref,
    to_inner_ref,
    to_outer_ref,
    a_ref,
    da_ref,
    lse0_ref,
    m0_ref,
    mc_ref,
    nc_ref,
    g_ref,
    h_ref,
    dkv_ref,
    q_ref,
    inner_ref,
    outer_ref,
    left_ref,
    right_ref,
    to_left_ref,
    to_right_ref,
    sems,
    edge_sems,
):
    loads = [
        pltpu.make_async_copy(da_hbm, da_ref, sems.at[0]),
    ]
    mid = pl.ds(BLOCK, 2 * BLOCK)
    for i, (mid_hbm, rim_hbm, ref) in enumerate(
        ((lse_mid_hbm, lse_rim_hbm, lse0_ref), (a_mid_hbm, a_rim_hbm, a_ref))
    ):
        loads.append(pltpu.make_async_copy(mid_hbm, ref.at[mid], sems.at[2 + 3 * i]))
        for side in range(2):
            to = pl.ds(side * (TOKENS - BLOCK), BLOCK)
            rows = pl.ds(side * BLOCK, BLOCK)
            sem = sems.at[3 + 3 * i + side]
            loads.append(pltpu.make_async_copy(rim_hbm.at[rows], ref.at[to], sem))
    edge_loads = [
        pltpu.make_async_copy(inner_hbm, inner_ref, edge_sems.at[0]),
        pltpu.make_async_copy(outer_hbm, outer_ref, edge_sems.at[1]),
    ]
    for side in range(2):
        rows = pl.ds(side * (TOKENS - BLOCK), BLOCK)
        to = pl.ds(side * BLOCK, BLOCK)
        edge_loads.append(
            pltpu.make_async_copy(q_hbm.at[rows], q_ref.at[to], edge_sems.at[2 + side])
        )
    for load in loads + edge_loads:
        load.start()
    own = jnp.where(
        iota((128, HIDDEN), 0) // LEVEL_ROWS == iota((128, HIDDEN), 1) // HEAD_DIM, 1.0, 0.0
    ).astype(F32)
    keep = coarse_keep()
    kv = kv_ref[...]
    query = by_head(cq_ref[...].astype(F32), own * SCALE).astype(BF16)
    scores = jnp.where(keep, mm(query, kv, ((1,), (1,))), MASKED)
    top = jnp.max(scores, axis=1, keepdims=True)
    weights = jnp.where(keep, jnp.exp(scores - top), 0.0)
    total = jnp.maximum(jnp.sum(weights, axis=1, keepdims=True), 1.0)
    on_values = pltpu.roll(weights, 4, 1).astype(BF16)
    inverse = 1.0 / total
    nc_ref[...] = over_heads(mm(on_values, kv, ((1,), (0,))) * inverse, own)
    mc_ref[...] = over_heads(jnp.broadcast_to(top + jnp.log(total), (128, HIDDEN)), own)
    same_head = jnp.where(
        iota((128, 128), 0) // HEAD_DIM == iota((128, 128), 1) // HEAD_DIM, 1.0, 0.0
    ).astype(BF16)
    spread = jnp.where(
        iota((384, HIDDEN), 0) % 128 == iota((384, HIDDEN), 1) // HEAD_DIM, 1.0, 0.0
    ).astype(BF16)
    for load in loads:
        load.wait()
    m0_ref[...] = mm(three_terms(lse0_ref[...]), spread, ((1,), (0,)))
    zero = jnp.zeros((1, 128), F32)

    def rows_of(parts):
        one, two, three = zip(*parts)
        return jnp.concatenate(
            list(one)
            + [two[0] + two[1], two[2] + two[3]]
            + [(three[0] + three[1]) + (three[2] + three[3]), zero],
            axis=0,
        )

    for p in range(PAIRS):
        lanes = slice(128 * p, 128 * (p + 1))
        g_parts, h_parts, lses, deltas = [], [], [], []
        for b in range(4):
            rows = slice(BLOCK * b, BLOCK * (b + 1))
            level = (b, 4 + b // 2, 6)
            m0 = m0_ref[rows, lanes]
            mc = [mc_ref[c : c + 1, lanes] for c in level]
            top_all = jnp.maximum(m0, jnp.maximum(mc[0], jnp.maximum(mc[1], mc[2])))
            f0 = jnp.exp(m0 - top_all)
            fc = [jnp.exp(x - top_all) for x in mc]
            inv = 1.0 / (f0 + fc[0] + (fc[1] + fc[2]))
            num = a_ref[rows, lanes].astype(F32) * f0
            for c, f in zip(level, fc):
                num = num + nc_ref[c : c + 1, lanes] * f
            att = (num * inv).astype(BF16)
            att_ref[rows, lanes] = att
            lses.append(top_all - jnp.log(inv))
            da = da_ref[rows, lanes].astype(F32)
            product = da * att.astype(F32)
            part = product.astype(BF16)
            rest = (product - part.astype(F32)).astype(BF16)
            delta = mm(part, same_head, ((1,), (0,))) + mm(rest, same_head, ((1,), (0,)))
            deltas.append(delta)
            wc = [f * inv for f in fc]
            g_parts.append([jnp.sum(w * da, axis=0, keepdims=True) for w in wc])
            h_parts.append([jnp.sum(w * delta, axis=0, keepdims=True) for w in wc])
        for parts, ref in ((lses, lse_ref), (deltas, delta_ref)):
            turned = jnp.concatenate(parts, axis=0).T
            for half in range(2):
                span = slice(128 * half, 128 * (half + 1))
                ref[p, half : half + 1, :] = jnp.concatenate(
                    [turned[:1, span], turned[HEAD_DIM : HEAD_DIM + 1, span]], axis=1
                )
        g_ref[:, lanes] = rows_of(g_parts)
        h_ref[:, lanes] = rows_of(h_parts)
    core = lax.axis_index("dp") % 2
    for hi in range(2):
        start = pl.multiple_of((2 * hi + 1 - core) * 256, 256)
        give_ref[:, 256 * hi : 256 * (hi + 1)] = att_ref[:, pl.ds(start, 256)]
    grads = (by_head(g_ref[...], own) * inverse).astype(BF16)
    sums = jnp.sum(by_head(h_ref[...], own), axis=1, keepdims=True) * (inverse * (1.0 / HEAD_DIM))
    on_keys = pltpu.roll(mm(grads, kv, ((1,), (1,))), 252, 1)
    score_grad = (weights * (on_keys - sums)).astype(BF16)
    row = iota((LEVEL_ROWS, 1), 0)
    share = jnp.where(row < 4, 1.0 / ROOTS[0], jnp.where(row < 6, 1.0 / ROOTS[1], 1.0 / ROOTS[2]))
    dq_ref[...] = over_heads(mm(score_grad, kv, ((1,), (0,))), own) * (share.astype(F32) * SCALE)
    for load in edge_loads:
        load.wait()
    left_ref[...], right_ref[...] = by_parity(inner_ref[...], outer_ref[...])
    edge_terms(q_ref, da_ref, lse_ref, delta_ref, left_ref, right_ref, to_left_ref, to_right_ref)
    to_inner_ref[...], to_outer_ref[...] = by_parity(to_left_ref[...], to_right_ref[...])
    left = jnp.concatenate([score_grad, on_values], axis=0)
    right = jnp.concatenate([query, grads], axis=0)
    dkv = mm(left, right, ((0,), (0,))).astype(BF16)
    dkv_ref[...] = dkv
    row, col = iota((128, 256), 0), iota((128, 256), 1)
    taken = 16 * (row // 8) + 8 * (row % 8 // 4) + 4 * (row % 4 // 2) + row % 2
    pick_rows = jnp.where(col == taken, 1.0, 0.0).astype(BF16)
    packed_ref[...] = mm(pick_rows, dkv, ((1,), (0,))).astype(BF16)
    column = lax.axis_index("seq") // 2
    other = column + 1 - 2 * (column % 2)
    own_ref[...] = dkv_ref[pl.ds(pl.multiple_of(16 * column, 16), 16), :]
    near_ref[...] = dkv_ref[pl.ds(pl.multiple_of(16 * other, 16), 16), :]


def join(cq, kv, inside, rim, da, q, inner, outer):
    stat = ((PAIRS, 2, 256), F32)
    level = pltpu.VMEM((LEVEL_ROWS, HIDDEN), F32)
    slab = ((2 * BLOCK, HIDDEN), BF16)
    return local_call(
        join_kernel,
        [
            ((TOKENS, HIDDEN), BF16),
            stat,
            stat,
            ((LEVEL_ROWS, HIDDEN), F32),
            ((128, HIDDEN), BF16),
            ((16, HIDDEN), BF16),
            ((16, HIDDEN), BF16),
            ((TOKENS, 512), BF16),
            slab,
            slab,
        ],
        (cq, kv, *inside, *rim, da, q, inner, outer),
        5 * 2 * 128 * 256 * 1024,
        scratch=[
            pltpu.VMEM((TOKENS, HIDDEN), BF16),
            pltpu.VMEM((TOKENS, HIDDEN), BF16),
            pltpu.VMEM((TOKENS, 128), F32),
            pltpu.VMEM((TOKENS, HIDDEN), F32),
            level,
            level,
            level,
            level,
            pltpu.VMEM((256, HIDDEN), BF16),
            *[pltpu.VMEM(*slab)] * 7,
            pltpu.SemaphoreType.DMA((8,)),
            pltpu.SemaphoreType.DMA((4,)),
        ],
        exps=6 * 256 * 1024,
        far_in=(2, 3, 4, 5, 6, 7, 8, 9),
    )


SLOT = 40


def weight_kernel(
    att_ref, got_ref, cot_ref, peer_cot_ref, packed_ref, send_ref, att_out, lhs_ref, att_sem
):
    att_copy = pltpu.make_async_copy(att_ref, att_out, att_sem)
    att_copy.start()
    core = lax.axis_index("dp") % 2
    for hi in range(2):
        start = pl.multiple_of((2 * hi + core) * 256, 256)
        rows = slice(256 * hi, 256 * (hi + 1))
        lhs_ref[rows, :TOKENS] = att_ref[:, pl.ds(start, 256)].T
        lhs_ref[rows, TOKENS:] = got_ref[:, rows].T
    width = 256
    for j in range(HIDDEN // width):
        cols = slice(width * j, width * (j + 1))
        cot = jnp.concatenate([cot_ref[:, cols], peer_cot_ref[:, cols]], axis=0)
        terms = mm(lhs_ref[...], cot, ((1,), (0,))).reshape(2, 16, 16, width)
        coarse = packed_ref[:, cols].astype(F32).reshape(16, 8, width)
        slots = jnp.concatenate([coarse, terms[0], terms[1]], axis=1)
        send_ref[:, cols] = slots.reshape(16 * SLOT, width).astype(BF16)
    att_copy.wait()


def weight_terms(att, got, cot, peer_cot, packed):
    return local_call(
        weight_kernel,
        [((16 * SLOT, HIDDEN), BF16), ((TOKENS, HIDDEN), BF16)],
        (att, got, cot, peer_cot, packed),
        2 * 512 * 512 * 1024,
        scratch=[pltpu.VMEM((512, 512), BF16), pltpu.SemaphoreType.DMA],
        far_out=(1,),
    )


def fine_backward_kernel(
    q_hbm,
    k_hbm,
    v_hbm,
    inner_hbm,
    outer_hbm,
    da_hbm,
    att_hbm,
    w_hbm,
    lse_ref,
    delta_ref,
    cdq_ref,
    gq_out,
    dk_out,
    dv_out,
    mixed_out,
    bias_ref,
    gq_ref,
    dk_ref,
    dv_ref,
    mixed_ref,
    q_ref,
    k_ref,
    v_ref,
    da_ref,
    att_ref,
    w_ref,
    inner_ref,
    outer_ref,
    left_ref,
    right_ref,
    sems,
    load_sems,
    mixed_sem,
):
    pairs = (
        (inner_hbm, inner_ref),
        (outer_hbm, outer_ref),
        (k_hbm, k_ref),
        (q_hbm, q_ref),
        (v_hbm, v_ref),
        (da_hbm, da_ref),
        (att_hbm, att_ref),
        (w_hbm, w_ref),
    )
    loads = [
        pltpu.make_async_copy(far, near, load_sems.at[i]) for i, (far, near) in enumerate(pairs)
    ]
    for load in loads:
        load.start()
    bias_ref[0] = band_bias(0, 0)
    bias_ref[1] = band_bias(1, 0)
    for load in loads[:6]:
        load.wait()
    left_ref[...], right_ref[...] = by_parity(inner_ref[...], outer_ref[...])
    masks = head_masks(1.0)
    scaled = head_masks(SCALE)
    low_lane = iota((128, 128), 1) < HEAD_DIM

    def copies(g, span):
        held_refs = (gq_ref, dk_ref, dv_ref)
        return [
            pltpu.make_async_copy(ref.at[:, span], out.at[:, span], sems.at[i, g])
            for i, (ref, out) in enumerate(zip(held_refs, (gq_out, dk_out, dv_out)))
        ]

    def body(g, groups, span):
        units = [
            (g * len(groups) + p, lanes, half) for p, lanes in enumerate(groups) for half in range(2)
        ]
        held = []
        for pair, lanes, half in units:
            rows = slice(128 * half, 128 * (half + 1))
            near = (left_ref.at[:, lanes], right_ref.at[:, lanes], half)
            keys = window(k_ref.at[:, lanes], *near, 0)
            vals = window(v_ref.at[:, lanes], *near, BLOCK)
            query = two_heads(q_ref[rows, lanes], scaled)
            grad = two_heads(da_ref[rows, lanes], masks)
            scores = mm(keys, query, ((1,), (1,))) + bias_ref[half]
            prob_grad = mm(vals, grad, ((1,), (1,)))
            held.append((keys, query, grad, scores, prob_grad))
        probs = [
            jnp.exp(h[3] - stat_row(lse_ref, u[0], 128 * u[2], 128)) for u, h in zip(units, held)
        ]
        parts = []
        for (pair, lanes, half), (keys, query, grad, _, prob_grad), prob in zip(
            units, held, probs
        ):
            rows = slice(128 * half, 128 * (half + 1))
            delta = stat_row(delta_ref, pair, 128 * half, 128)
            score_grad = (prob * (prob_grad - delta)).astype(BF16)
            dk = mm(score_grad, query, ((1,), (0,)))
            dv = mm(prob.astype(BF16), grad, ((1,), (0,)))
            parts.append((dk, dv))
            dq = pick(mm(score_grad, keys, ((0,), (0,))), low_lane) * SCALE
            for b in range(2):
                block = 2 * half + b
                coarse = (
                    cdq_ref[block : block + 1, lanes]
                    + cdq_ref[4 + half : 5 + half, lanes]
                    + cdq_ref[6:7, lanes]
                )
                gq_ref[BLOCK * block : BLOCK * (block + 1), lanes] = (
                    dq[BLOCK * b : BLOCK * (b + 1), :] + coarse
                ).astype(BF16)
        for p, lanes in enumerate(groups):
            for ref, low, high in zip((dk_ref, dv_ref), parts[2 * p], parts[2 * p + 1]):
                ref[:BLOCK, lanes] = low[BLOCK : 2 * BLOCK, :].astype(BF16)
                middle = low[2 * BLOCK :, :] + high[: 2 * BLOCK, :]
                ref[BLOCK : 3 * BLOCK, lanes] = middle.astype(BF16)
                ref[3 * BLOCK :, lanes] = high[2 * BLOCK : 3 * BLOCK, :].astype(BF16)
        for copy in copies(g, span):
            copy.start()

    over_groups(body, BACKWARD_GROUP)
    for load in loads[6:]:
        load.wait()
    mixed_ref[...] = mm(att_ref[...], w_ref[...], ((1,), (0,))).astype(BF16)
    mixed_copy = pltpu.make_async_copy(mixed_ref, mixed_out, mixed_sem)
    mixed_copy.start()
    width = 128 * BACKWARD_GROUP
    for g in range(PAIRS // BACKWARD_GROUP):
        for copy in copies(g, pl.ds(width * g, width)):
            copy.wait()
    mixed_copy.wait()


def fine_backward(q, k, v, inner, outer, da, att, w, lse, delta, cdq):
    out = ((TOKENS, HIDDEN), BF16)
    return local_call(
        fine_backward_kernel,
        [out, out, out, out],
        (q, k, v, inner, outer, da, att, w, lse, delta, cdq),
        5 * 16 * 2 * 256 * 256 * 128 + 2 * 256 * 1024 * 1024,
        scratch=[pltpu.VMEM((2, 256, 256), F32)]
        + [pltpu.VMEM((TOKENS, HIDDEN), BF16)] * 9
        + [pltpu.VMEM((HIDDEN, HIDDEN), BF16)]
        + [pltpu.VMEM((2 * BLOCK, HIDDEN), BF16)] * 4
        + [
            pltpu.SemaphoreType.DMA((3, PAIRS // BACKWARD_GROUP)),
            pltpu.SemaphoreType.DMA((8,)),
            pltpu.SemaphoreType.DMA,
        ],
        exps=16 * 256 * 256,
        far_in=tuple(range(8)),
        far_out=(0, 1, 2, 3),
    )


def sums_kernel(
    got_ref,
    near_ref,
    own_ref,
    dk_hbm,
    dv_hbm,
    coarse_ref,
    mine_ref,
    to_low_ref,
    to_high_ref,
    to_both_ref,
    dk_ref,
    dv_ref,
    sems,
):
    copies = [
        pltpu.make_async_copy(dk_hbm, dk_ref, sems.at[0]),
        pltpu.make_async_copy(dv_hbm, dv_ref, sems.at[1]),
    ]
    for copy in copies:
        copy.start()
    me = lax.axis_index("seq")
    low, column = me % 2, me // 2
    high = lax.axis_index("dp") // 2
    row = iota((64, 16 * SLOT), 0)
    col = iota((64, 16 * SLOT), 1)
    source = col // SLOT
    at = col % SLOT
    near = source // 2 == column // 2
    mid = jnp.logical_and(source // 8 == column // 8, jnp.logical_not(near))
    far = source // 8 != column // 8
    level_row = row % 8
    side = jnp.where(row < 16, 0, 1)
    term = at - 4 * side - 2 * (row // 8 % 2)
    two = jnp.logical_and(jnp.logical_and(level_row // 2 == 2, term == level_row - 4), mid)
    three = jnp.logical_and(jnp.logical_and(level_row == 6, term == 0), far)
    coarse = jnp.logical_and(jnp.logical_or(two, three), row < 32)
    block = row // 8 - 4
    block_high = jnp.where(block < 2, high, 1 - high)
    block_low = jnp.where(block % 2 == 0, low, 1 - low)
    weight = jnp.logical_and(row >= 32, at == 8 + 16 * block_high + 8 * block_low + level_row)
    chosen = jnp.where(jnp.logical_or(coarse, weight), 1.0, 0.0).astype(BF16)
    sums = mm(chosen, got_ref[...], ((1,), (0,)))
    row = iota((32, 32), 0)
    col = iota((32, 32), 1) % 16
    side = jnp.where(row < 16, 0, 1)
    first = jnp.logical_and(row % 8 < 4, col == 8 * side + 4 * (row // 8 % 2) + row % 8)
    close = jnp.concatenate([near_ref[...], own_ref[...]], axis=0)
    coarse_sums = sums[:32, :] + mm(jnp.where(first, 1.0, 0.0).astype(BF16), close, ((1,), (0,)))
    coarse_ref[...] = coarse_sums[:16, :]
    mine_ref[...] = sums[32:40, :]
    to_low_ref[:16, :] = coarse_sums[16:, :].astype(BF16)
    to_low_ref[16:, :] = sums[40:48, :].astype(BF16)
    to_high_ref[...] = sums[48:56, :].astype(BF16)
    to_both_ref[...] = sums[56:, :].astype(BF16)
    for copy in copies:
        copy.wait()


def all_sums(got, near, own, dk, dv):
    return local_call(
        sums_kernel,
        [
            ((16, HIDDEN), F32),
            ((8, HIDDEN), F32),
            ((24, HIDDEN), BF16),
            ((8, HIDDEN), BF16),
            ((8, HIDDEN), BF16),
            ((TOKENS, HIDDEN), BF16),
            ((TOKENS, HIDDEN), BF16),
        ],
        (got, near, own, dk, dv),
        2 * 64 * 640 * 1024,
        scratch=[pltpu.SemaphoreType.DMA((2,))],
        far_in=(3, 4),
    )


def finish_kernel(
    dk_ref,
    dv_ref,
    inner_ref,
    outer_ref,
    sums_ref,
    low_ref,
    gk_out,
    gv_out,
    gk_ref,
    gv_ref,
    sems,
):
    copies = []
    sums = sums_ref[...] + low_ref[:16, :].astype(F32)
    from_left, from_right = by_parity(inner_ref[...], outer_ref[...])
    for at, own_ref, out_ref, out in ((0, dk_ref, gk_ref, gk_out), (8, dv_ref, gv_ref, gv_out)):
        side = BLOCK * (at // 8)
        for b in range(4):
            rows = slice(BLOCK * b, BLOCK * (b + 1))
            c1, c2, c3 = at + b, at + 4 + b // 2, at + 6
            coarse = (
                sums[c1 : c1 + 1, :] * (1.0 / ROOTS[0])
                + sums[c2 : c2 + 1, :] * (1.0 / ROOTS[1])
                + sums[c3 : c3 + 1, :] * (1.0 / ROOTS[2])
            )
            value = own_ref[rows, :].astype(F32) + coarse
            if b == 0:
                value = value + from_left[side : side + BLOCK, :].astype(F32)
            if b == 3:
                value = value + from_right[side : side + BLOCK, :].astype(F32)
            out_ref[rows, :] = value.astype(BF16)
            span = pl.ds(BLOCK * b, BLOCK)
            copies.append(
                pltpu.make_async_copy(out_ref.at[span], out.at[span], sems.at[at // 8, b])
            )
            copies[-1].start()
    for copy in copies:
        copy.wait()


def finish(dk, dv, inner, outer, sums, low):
    out = ((TOKENS, HIDDEN), BF16)
    return local_call(
        finish_kernel,
        [out, out],
        (dk, dv, inner, outer, sums, low),
        16 * 256 * 1024,
        scratch=[pltpu.VMEM((TOKENS, HIDDEN), BF16)] * 2 + [pltpu.SemaphoreType.DMA((2, 4))],
        far_out=(0, 1),
    )


def swap(x, axis, bit):
    return lax.ppermute(x, axis, [(i, i ^ bit) for i in range(lax.axis_size(axis))])


def swap_inner(x):
    return swap(x, "seq", 1)


def swap_outer(x):
    n = lax.axis_size("seq")
    return lax.ppermute(x, "seq", [(i, i + 1 if i % 2 else i - 1) for i in range(1, n - 1)])


def swap_both(x):
    n = lax.axis_size("seq")
    total = n * lax.axis_size("dp")
    return lax.ppermute(x, ("dp", "seq"), [(i, i ^ (2 * n + 1)) for i in range(total)])


def exchanged(x, rows):
    groups = [[2 * j + low for j in range(16)] for low in range(2)]
    got = lax.all_to_all(
        x.reshape(16, rows, HIDDEN),
        "seq",
        split_axis=0,
        concat_axis=0,
        tiled=True,
        axis_index_groups=groups,
    )
    return got.reshape(16 * rows, HIDDEN)


def body(q, k, v, out_weight, cot):
    levels, inner, outer = pool(k, v)
    peer_levels = swap(levels, "seq", 1)
    outer = swap_outer(outer)
    inner = swap_inner(inner)
    send = slots(levels, peer_levels)
    coarse_kv = exchanged(send, 16)
    peer_cot = swap(cot, "dp", 1)
    *inside, d_att, cq = inside_forward(q, k, v, cot, out_weight)
    rim = rim_forward(q, k, v, inner, outer)
    att, lse, delta, cdq, packed, own_rows, near_rows, give, to_inner, to_outer = join(
        cq, coarse_kv, inside, rim, d_att, q, inner, outer
    )
    got = swap(give, "dp", 1)
    from_outer = swap_outer(to_outer)
    from_inner = swap_inner(to_inner)
    send_back, far_att = weight_terms(att, got, cot, peer_cot, packed)
    back = exchanged(send_back, SLOT)
    near_rows = swap(near_rows, "seq", 2)
    gq, dk, dv, mixed = fine_backward(
        q, k, v, inner, outer, d_att, far_att, out_weight, lse, delta, cdq
    )
    sums, mine, to_low, to_high, to_both, dk, dv = all_sums(
        back, near_rows, own_rows, dk, dv
    )
    low = swap(to_low, "seq", 1)
    high = swap(to_high, "dp", 2)
    both = swap_both(to_both)
    gk, gv = finish(dk, dv, from_inner, from_outer, sums, low)
    grad_weight = (mine + low[16:].astype(F32)) + (high.astype(F32) + both.astype(F32))
    return (mixed[None], grad_weight, gq[None], gk[None], gv[None])


def on_device(queries, keys, values, out_weight, cotangent):
    return body(queries[0], keys[0], values[0], out_weight, cotangent[0])


def solution(mesh):
    tokens = P("dp", "seq", None)
    return jax.shard_map(
        on_device,
        mesh=mesh,
        in_specs=(tokens, tokens, tokens, P(), tokens),
        out_specs=(tokens, P(("dp", "seq"), None), tokens, tokens, tokens),
        check_vma=False,
    )
```
